256 devices in a mesh: gx: 8 (over y, x_lo), gy: 16 (over z, core), gz: 2 (over x_hi).
Axes of the slice: x: 4 (x_hi: 2, x_lo: 2; x = x_hi * 2 + x_lo), y: 4, z: 8, core: 2. Of those that a mesh axis runs over, the one named last changes fastest.
Arguments:
- starting_kelvin: float32 [16, 128, 4096], P(None, 'gx', ('gy', 'gz')), may hold values from -6 to 6
- substance_label: int32 [16, 128, 4096], P(None, 'gx', ('gy', 'gz')), may hold values from 0 to 3
- voxel_source_patch: int32 [16, 128, 4096], P(None, 'gx', ('gy', 'gz')), may hold values from 0 to 15
- substance_traits: float32 [4, 4], replicated, may hold values from 0.5 to 2
- patch_source_intensity: float32 [16], replicated, may hold values from 0 to 8
Outputs:
- warmed_result: float32 [16, 128, 4096], P(None, 'gx', ('gy', 'gz'))
- solution: float32 [3, 16, 128, 4096], P(None, 'gz', 'gx', 'gy')
- residual: float32 [3, 16, 128, 4096], P(None, 'gz', 'gx', 'gy')
The draws below stay inside these ranges and needn't reach their ends.
All inputs are finite; a program needn't handle non-finite values.
Results may differ from the reference program's by a relative error of at most 0.0029.
Values sent between devices are 32-bit elements; how exact they have to be, the bound alone decides.
A program may use at most 64 MiB of HBM per device.

```python
import math
import jax
import jax.numpy as jnp

HEIGHT_VOXELS = 16
MATS = 4
TILES = 16
HEAT_STEPS = 2
ITERS = 3
LATERAL_DEPTH = 128
LATERAL_WIDTH = 4096


def with_ends(entries, own_key, low, high):
    longest = entries.shape.index(max(entries.shape))
    spots = []
    for shift in (0, 1):
        where = [jax.random.randint(jax.random.fold_in(own_key, axis), (), 0, length) for axis, length in enumerate(entries.shape)]
        where[longest] = (where[longest] + shift) % entries.shape[longest]
        spots.append(tuple(where))
    return entries.at[spots[0]].set(low).at[spots[1]].set(high)


def shard_levels(key, shape, shards, least, top_value):
    def one(dim, shards_of):
        steps = jax.random.uniform(jax.random.fold_in(jax.random.fold_in(key, 6), dim), (shards_of,), jnp.float32, least / len(shards), top_value / len(shards))
        return jnp.repeat(jnp.exp(steps), shape[dim] // shards_of).reshape((-1,) + (1,) * (len(shape) - dim - 1))

    gain = one(*shards[0])
    for cut in shards[1:]:
        gain = gain * one(*cut)
    return gain


def scatter_about(stream_key, extent, spread, limit, cuts=(), held_as=jnp.bfloat16):
    entries = spread * jax.random.normal(stream_key, extent, jnp.float32)
    if cuts:
        entries = entries * shard_levels(stream_key, extent, cuts, -0.22, 0.18)
    return jnp.clip(entries, -limit, limit).astype(held_as)


def setup_inputs(seed: int = 0) -> dict:
    arg_keys = jax.random.split(jax.random.key(seed), 6)
    return {
        "starting_kelvin": scatter_about(arg_keys[0], (HEIGHT_VOXELS, LATERAL_DEPTH, LATERAL_WIDTH), 1.0, 6.0, ((1, 8), (2, 32)), jnp.float32),
        "substance_label": with_ends(jax.random.randint(arg_keys[1], (HEIGHT_VOXELS, LATERAL_DEPTH, LATERAL_WIDTH), 0, MATS), jax.random.fold_in(arg_keys[1], 1), 0, MATS - 1).astype(jnp.int32),
        "voxel_source_patch": with_ends(jax.random.randint(arg_keys[2], (HEIGHT_VOXELS, LATERAL_DEPTH, LATERAL_WIDTH), 0, TILES), jax.random.fold_in(arg_keys[2], 1), 0, TILES - 1).astype(jnp.int32),
        "substance_traits": jnp.clip(jnp.exp(jax.random.uniform(arg_keys[3], (4, MATS), jnp.float32, math.log(0.5), math.log(2.0))), 0.5, 2.0),
        "patch_source_intensity": jnp.clip(jax.random.uniform(arg_keys[4], (TILES,), jnp.float32, 0.0, 8.0), 0.0, 8.0),
    }


time_step = 0.03
anchor_scale = 0.5
strain_gain = 2.0


def lookup(identity, table, count):
    summed = jnp.zeros(identity.shape, jnp.float32)
    for number in range(count):
        summed = summed + jnp.where(identity == number, table[number], jnp.float32(0.0))
    return summed


def conduct(own, other):
    return 2.0 * own * other / jnp.maximum(own + other, 0.25)


def heat_step(padded_temp, padded_cond, power, inverse_cap):
    centre = padded_temp[:, 1:-1, 1:-1]
    own = padded_cond[:, 1:-1, 1:-1]
    layers, rows, columns = centre.shape
    heat_flux = jnp.zeros_like(centre)
    for row_offset, column_offset in ((0, 1), (2, 1), (1, 0), (1, 2)):
        neighbour = padded_temp[:, row_offset:row_offset + rows, column_offset:column_offset + columns]
        other = padded_cond[:, row_offset:row_offset + rows, column_offset:column_offset + columns]
        heat_flux = heat_flux + conduct(own, other) * (neighbour - centre)
    vertical_temp = jnp.pad(centre, ((1, 1), (0, 0), (0, 0)))
    vertical_cond = jnp.pad(own, ((1, 1), (0, 0), (0, 0)))
    for layer_offset in (0, 2):
        other = vertical_cond[layer_offset:layer_offset + layers]
        neighbour = vertical_temp[layer_offset:layer_offset + layers]
        heat_flux = heat_flux + conduct(own, other) * (neighbour - centre)
    return centre + time_step * inverse_cap * (heat_flux + power)


def neighbour_offsets():
    listed = []
    for along_z in (-1, 0, 1):
        for along_x in (-1, 0, 1):
            for along_y in (-1, 0, 1):
                if along_z != 0 or along_x != 0 or along_y != 0:
                    listed.append((along_z, along_x, along_y))
    return listed


def apply_operator(field, padded_field, modulus, padded_modulus):
    layers, rows, columns = modulus.shape
    parts = [anchor_scale * modulus * field[0], anchor_scale * modulus * field[1], anchor_scale * modulus * field[2]]
    for along_z, along_x, along_y in neighbour_offsets():
        length_sq = along_z * along_z + along_x * along_x + along_y * along_y
        window = (slice(1 + along_z, 1 + along_z + layers), slice(1 + along_x, 1 + along_x + rows), slice(1 + along_y, 1 + along_y + columns))
        weight = (0.5 / length_sq) * (modulus + padded_modulus[window])
        change = [field[index_c] - padded_field[index_c][window] for index_c in range(3)]
        projected = (along_z * change[0] + along_x * change[1] + along_y * change[2]) / length_sq
        for index_c, direction_part in enumerate((along_z, along_x, along_y)):
            parts[index_c] = parts[index_c] + weight * (0.5 * change[index_c] + direction_part * projected)
    return jnp.stack(parts)


def thermal_load(modulus, padded_modulus, strain, padded_strain):
    layers, rows, columns = modulus.shape
    parts = [jnp.zeros_like(modulus), jnp.zeros_like(modulus), jnp.zeros_like(modulus)]
    for along_z, along_x, along_y in neighbour_offsets():
        length_sq = along_z * along_z + along_x * along_x + along_y * along_y
        window = (slice(1 + along_z, 1 + along_z + layers), slice(1 + along_x, 1 + along_x + rows), slice(1 + along_y, 1 + along_y + columns))
        weight = (0.5 / length_sq) * (modulus + padded_modulus[window])
        pushing = weight * (0.5 * (strain + padded_strain[window]))
        for index_c, direction_part in enumerate((along_z, along_x, along_y)):
            if direction_part != 0:
                parts[index_c] = parts[index_c] - strain_gain * direction_part * pushing
    return jnp.stack(parts)


def reference(starting_kelvin, substance_label, voxel_source_patch, substance_traits, patch_source_intensity):
    diffusive_coefficient = lookup(substance_label, substance_traits[0], MATS)
    inverse_cap = 1.0 / lookup(substance_label, substance_traits[1], MATS)
    power = lookup(voxel_source_patch, patch_source_intensity, TILES)
    cycle = ((0, 0), (1, 1), (1, 1))
    padded_cond = jnp.pad(diffusive_coefficient, cycle)
    warmed_result = starting_kelvin
    for number in range(HEAT_STEPS):
        warmed_result = heat_step(jnp.pad(warmed_result, cycle), padded_cond, power, inverse_cap)
    modulus = lookup(substance_label, substance_traits[2], MATS)
    strain = lookup(substance_label, substance_traits[3], MATS) * warmed_result
    padded_modulus = jnp.pad(modulus, 1)
    load = thermal_load(modulus, padded_modulus, strain, jnp.pad(strain, 1))
    solution = jnp.zeros_like(load)
    residual = load
    direction = load
    norm_now = jnp.sum(residual * residual)
    shell = ((0, 0), (1, 1), (1, 1), (1, 1))
    for number in range(ITERS):
        image = apply_operator(direction, jnp.pad(direction, shell), modulus, padded_modulus)
        alpha = norm_now / jnp.sum(direction * image)
        solution = solution + alpha * direction
        residual = residual - alpha * image
        norm_next = jnp.sum(residual * residual)
        direction = residual + (norm_next / norm_now) * direction
        norm_now = norm_next
    return warmed_result, solution, residual
```

```python
import jax
import jax.numpy as jnp
from jax import lax
from jax.experimental import pallas as pl
from jax.experimental.pallas import tpu as pltpu
from jax.sharding import PartitionSpec as P

MESH = pl.DeviceIdType.MESH
F32 = jnp.float32
TIME_STEP = 0.03
TAU = 4.0 / 3.0
SPAN = 6.0
DIAGONAL = 0.5 + 2.5 + 2.5 + 10.0 / 9.0


def plus(value, axis):
    return pltpu.roll(value, value.shape[axis] - 1, axis)


def minus(value, axis):
    return pltpu.roll(value, 1, axis)


def tree(bits, entries):
    while len(entries) > 1:
        mask, bits = bits[0], bits[1:]
        entries = [jnp.where(mask, entries[i + 1], entries[i]) for i in range(0, len(entries), 2)]
    return entries[0]


def lookup(identity, entries):
    bits, width = [], 1
    while width < len(entries):
        bits.append((identity & width) != 0)
        width *= 2
    return tree(bits, entries)


def conduct(own, other):
    return 2.0 * own * other / jnp.maximum(own + other, 0.25)


def stencil(get):
    def both(comp, kind):
        up, down = get(comp, kind, 1), get(comp, kind, -1)
        return up + down, up - down

    z, x, y = 0, 1, 2
    e, p, q = 0, 1, 2
    pz_ez, qz_ez = both(z, e)
    pz_pz, qz_pz = both(z, p)
    pz_ex, qz_ex = both(x, e)
    pz_px, qz_px = both(x, p)
    pz_qx = get(x, q, 1) + get(x, q, -1)
    pz_qy, qz_qy = both(y, q)
    qz_qz = get(z, q, 1) - get(z, q, -1)
    e_z, p_z = get(z, e, 0), get(z, p, 0)
    e_x, p_x = get(x, e, 0), get(x, p, 0)
    p_y = get(y, p, 0)
    eighth, corner, mixed = 0.125, 5.0 / 36.0, 1.0 / 18.0
    parts = []
    parts.append((
        0.25 * (p_z + pz_pz) + 0.75 * pz_ez + eighth * qz_qy,
        0.25 * (e_z + pz_ez) + eighth * p_z + corner * pz_pz + mixed * qz_qy,
        eighth * qz_ex + mixed * qz_px,
    ))
    shared = 0.25 * (p_x + pz_ex)
    parts.append((
        shared + eighth * pz_px,
        0.75 * e_x + shared + corner * pz_px,
        eighth * (get(y, q, 0) + qz_ez) + mixed * (pz_qy + qz_pz),
    ))
    pz_ey = get(y, e, 1) + get(y, e, -1)
    pz_py = get(y, p, 1) + get(y, p, -1)
    parts.append((
        0.75 * p_y + 0.25 * (pz_ey + pz_py) + eighth * qz_qz,
        0.25 * (get(y, e, 0) + p_y) + eighth * pz_ey + corner * pz_py + mixed * qz_qz,
        eighth * get(x, q, 0) + mixed * pz_qx,
    ))
    return [c + plus(a + b, 0) + minus(a - b, 0) for c, a, b in parts]


def scalar_stencils(get):
    e, p, q = 0, 1, 2
    pz_e, qz_e = get(e, 1) + get(e, -1), get(e, 1) - get(e, -1)
    pz_p, qz_p = get(p, 1) + get(p, -1), get(p, 1) - get(p, -1)
    pz_q, qz_q = get(q, 1) + get(q, -1), get(q, 1) - get(q, -1)
    e0, p0, q0 = get(e, 0), get(p, 0), get(q, 0)
    eighth, corner, mixed = 0.125, 5.0 / 36.0, 1.0 / 18.0

    def even(c, a):
        return c + plus(a, 0) + minus(a, 0)

    def odd(b):
        return plus(b, 0) - minus(b, 0)

    return [
        even(0.25 * (p0 + pz_p) + 0.75 * pz_e, 0.25 * (e0 + pz_e) + eighth * p0 + corner * pz_p),
        even(0.25 * (p0 + pz_e) + eighth * pz_p, 0.75 * e0 + 0.25 * (p0 + pz_e) + corner * pz_p),
        even(0.75 * p0 + 0.25 * (pz_e + pz_p), 0.25 * (e0 + p0) + eighth * pz_e + corner * pz_p),
        odd(eighth * qz_e + mixed * qz_p),
        even(eighth * qz_q, mixed * qz_q),
        odd(eighth * q0 + mixed * pz_q),
    ]


def gradient(get):
    e, p, q = 0, 1, 2
    qz_e, qz_p = get(e, 1) - get(e, -1), get(p, 1) - get(p, -1)
    pz_e, pz_p = get(e, 1) + get(e, -1), get(p, 1) + get(p, -1)
    q0, pz_q = get(q, 0), get(q, 1) + get(q, -1)
    sixth = 1.0 / 6.0
    a_z = 0.25 * qz_e + sixth * qz_p
    b_x = 0.5 * get(e, 0) + 0.25 * (get(p, 0) + pz_e) + sixth * pz_p
    a_y = 0.25 * q0 + sixth * pz_q
    return [
        0.5 * qz_e + 0.25 * qz_p + plus(a_z, 0) + minus(a_z, 0),
        plus(b_x, 0) - minus(b_x, 0),
        0.5 * q0 + 0.25 * pz_q + plus(a_y, 0) + minus(a_y, 0),
    ]


def poly_dot(first, second, moments):
    total = None
    for i, a in enumerate(first):
        for j, b in enumerate(second):
            term = a * b * moments[i + j]
            total = term if total is None else total + term
    return total


def shifted(poly):
    out = [TAU * c for c in poly] + [jnp.zeros_like(poly[0])]
    for k, c in enumerate(poly):
        out[k + 1] = out[k + 1] + c
    return out


def added(first, second):
    if len(first) < len(second):
        first, second = second, first
    return [a + second[i] if i < len(second) else a for i, a in enumerate(first)]


def iterate_coefficients(moments):
    one = jnp.ones_like(moments[0])
    residual, direction, solution = [one], [one], []
    norm = moments[0]
    for number in range(3):
        image = shifted(direction)
        alpha = norm / poly_dot(direction, image, moments)
        solution = added(solution, [alpha * c for c in direction])
        residual = added([-alpha * c for c in image], residual)
        if number < 2:
            following = poly_dot(residual, residual, moments)
            ratio = following / norm
            direction = added(residual, [ratio * c for c in direction])
            norm = following
    return solution, residual


def make_kernel(sizes):
    nx, ny = sizes["gx"], sizes["gy"]
    group_a, group_b = nx * 2, ny

    def kernel(
        kelvin_in, label_in, patch_in, traits, intensity,
        warmed_out, solution_out, residual_out,
        temp, label, patch, cond, rate, power, g_row, g_col, g_up, temp_one,
        packs, strips, packed_strain, strain_strips, label_strips,
        strain, e_label, e_strain, base, field, lanes, stiff,
        sums, sums_a, sums_b, total_a,
        local_sem, send, recv,
    ):
        gx, gy, gz = lax.axis_index("gx"), lax.axis_index("gy"), lax.axis_index("gz")
        other = 1 - gz
        nexts = {-1: lax.rem(gx + nx - 1, nx), 0: gx, 1: lax.rem(gx + 1, nx)}
        gy_up, gy_down = lax.rem(gy + 1, ny), lax.rem(gy + ny - 1, ny)
        own_lanes = pl.ds(pl.multiple_of(gz * 128, 128), 128)

        loads = [
            pltpu.make_async_copy(kelvin_in, temp.at[:, 0:16, 0:128], local_sem.at[0]),
            pltpu.make_async_copy(label_in, label.at[:, 0:16, 0:128], local_sem.at[1]),
            pltpu.make_async_copy(patch_in, patch.at[:, 0:16, 0:128], local_sem.at[2]),
            pltpu.make_async_copy(
                label_in.at[pl.ds(4 * gz, 12)], e_label.at[:, 0:16, own_lanes], local_sem.at[3]
            ),
        ]
        for copy in loads:
            copy.start()
        temp[:, 16:24, 0:128] = jnp.zeros((16, 8, 128), F32)
        label[:, 16:24, 0:128] = jnp.zeros((16, 8, 128), jnp.int32)
        patch[:, 16:24, 0:128] = jnp.zeros((16, 8, 128), jnp.int32)

        barrier = pltpu.get_barrier_semaphore()
        peers = [
            (nexts[dx], dy, dz)
            for dx in (-1, 0, 1)
            for dy in (gy, gy_up, gy_down)
            for dz in (gz, other)
            if not (dx == 0 and dy is gy and dz is gz)
        ]
        number_a = gx * 2 + gz
        ring_a = []
        for step in range(1, group_a):
            there = lax.rem(number_a + step, group_a)
            ring_a.append((there // 2, gy, lax.rem(there, 2)))
        ring_b = [(gx, lax.rem(gy + step, ny), gz) for step in range(1, group_b)]
        everyone = peers + ring_a + ring_b
        for peer in everyone:
            pl.semaphore_signal(barrier, inc=1, device_id=peer, device_id_type=MESH)
        for copy in loads:
            copy.wait()

        lane = lax.broadcasted_iota(jnp.int32, (8, 128), 1)
        sub = lax.broadcasted_iota(jnp.int32, (8, 128), 0)

        def pack(read, width, sides):
            def body(layer, acc):
                acc = list(acc)
                for half in range(2):
                    slot = layer * 2 + half
                    mask = (lane >> 2) == slot
                    for k in range(width):
                        value = read(k, layer, half)
                        for n, start in enumerate(sides):
                            moved = pltpu.roll(value, lax.rem(slot * 4 + 128 - start, 128), 1)
                            acc[k * len(sides) + n] = jnp.where(mask, moved, acc[k * len(sides) + n])
                return tuple(acc)

            return lax.fori_loop(0, 16, body, tuple(jnp.zeros((8, 128), F32) for _ in range(width * len(sides))))

        def read_inputs(k, layer, half):
            ref = (temp, label, patch)[k]
            return ref[layer, 8 * half : 8 * half + 8, 0:128].astype(F32)

        packed = pack(read_inputs, 3, (0, 124))
        for k in range(3):
            for side in range(2):
                packs[side, k] = packed[k * 2 + side]

        pl.semaphore_wait(barrier, len(everyone))

        count = [0]

        def remote(src, dst, peer):
            n = count[0]
            count[0] += 1
            copy = pltpu.make_async_remote_copy(
                src_ref=src, dst_ref=dst, send_sem=send.at[n], recv_sem=recv.at[n],
                device_id=peer, device_id_type=MESH,
            )
            copy.start()
            return copy

        heat = []
        for ref in (temp, label, patch):
            heat.append(remote(ref.at[:, 0:2, 0:128], ref.at[:, 16:18, 0:128], (nexts[-1], gy, gz)))
            heat.append(remote(ref.at[:, 14:16, 0:128], ref.at[:, 22:24, 0:128], (nexts[1], gy, gz)))
        right_gy = jnp.where(gz == 0, gy, gy_up)
        left_gy = jnp.where(gz == 0, gy_down, gy)
        for dx in (0, -1, 1):
            heat.append(remote(packs.at[0], strips.at[0, 1 - dx], (nexts[dx], left_gy, other)))
            heat.append(remote(packs.at[1], strips.at[1, 1 - dx], (nexts[dx], right_gy, other)))

        side_gy = jnp.where(gz == 0, gy_down, gy_up)

        def elastic_sends(src, src_layers, dst, pack_src, pack_dst):
            out = [remote(src.at[pl.ds(src_layers(other), 12), 0:16, 0:128], dst.at[:, 0:16, own_lanes], (gx, gy, other))]
            for dz in (gz, other):
                layers = pl.ds(src_layers(dz), 12)
                out.append(remote(src.at[layers, 0:4, 0:128], dst.at[:, 16:20, own_lanes], (nexts[-1], gy, dz)))
                out.append(remote(src.at[layers, 12:16, 0:128], dst.at[:, 20:24, own_lanes], (nexts[1], gy, dz)))
                for dx in (0, -1, 1):
                    out.append(remote(pack_src, pack_dst.at[gz, 1 - dx], (nexts[dx], side_gy, dz)))
            return out

        labels = elastic_sends(label, lambda dz: 4 * dz, e_label, packs.at[gz, 1], label_strips)

        for copy in heat:
            copy.wait_recv()

        def halo_blocks(blocks):
            right = [blocks(0, d) for d in (-1, 0, 1)]
            left = [blocks(1, d) for d in (-1, 0, 1)]

            def corner(three):
                return jnp.where(sub < 4, three[2], pltpu.roll(three[0], 124, 1))

            right_corner, left_corner = corner(right), corner(left)

            def at(layer):
                def one(r, l, slot):
                    r = pltpu.roll(r, lax.rem(128 - slot * 4, 128), 1)
                    l = pltpu.roll(l, lax.rem(252 - slot * 4, 128), 1)
                    return jnp.where(lane < 64, r, l)

                return jnp.concatenate([
                    one(right[1], left[1], layer * 2),
                    one(right[1], left[1], layer * 2 + 1),
                    one(right_corner, left_corner, layer * 2),
                ], axis=0)

            return at

        temp_halo, label_halo, patch_halo = [
            halo_blocks(lambda side, d, k=k: strips[side, d + 1, k]) for k in range(3)
        ]

        row = lax.broadcasted_iota(jnp.int32, (24, 128), 0)
        wide_lane = lax.broadcasted_iota(jnp.int32, (24, 128), 1)
        low_row = jnp.where(gx == nx - 1, 16, 24)
        high_row = jnp.where(gx == 0, 20, 32)
        rows_ok = ((row < 16) | ((row >= 16) & (row < 20) & (row < low_row)) | ((row >= 20) & (row < high_row) & (gx > 0)))
        first_tile, last_tile = (gy == 0) & (gz == 0), (gy == ny - 1) & (gz == 1)
        right_limit = jnp.where(last_tile, 0, 64)
        left_limit = jnp.where(first_tile, 128, 64)
        cols_ok = (wide_lane < right_limit) | (wide_lane >= left_limit)
        grid_ok = [rows_ok, rows_ok & cols_ok]
        e_right_limit = jnp.where(gy == ny - 1, 0, 64)
        e_left_limit = jnp.where(gy == 0, 128, 64)
        e_cols_ok = (wide_lane < e_right_limit) | (wide_lane >= e_left_limit)
        e_ok = [rows_ok, rows_ok, rows_ok & e_cols_ok]

        materials = range(4)
        conductivity = [traits[0, m] for m in materials]
        capacity = [traits[1, m] for m in materials]
        modulus = [traits[2, m] for m in materials]
        expansion = [traits[3, m] for m in materials]
        tiles = [intensity[t] for t in range(16)]

        def heat_fields(layer, carry):
            temp[layer, :, 128:256] = temp_halo(layer)
            ids = [label[layer, :, 0:128], label_halo(layer).astype(jnp.int32)]
            tile_ids = [patch[layer, :, 0:128], patch_halo(layer).astype(jnp.int32)]
            for n in range(2):
                cut = slice(128 * n, 128 * n + 128)
                cond[layer, :, cut] = jnp.where(grid_ok[n], lookup(ids[n], conductivity), 0.0)
                rate[layer, :, cut] = TIME_STEP / lookup(ids[n], capacity)
                power[layer, :, cut] = lookup(tile_ids[n], tiles)
            return carry

        lax.fori_loop(0, 16, heat_fields, 0)
        cond[16] = jnp.zeros((24, 256), F32)

        def conductances(layer, carry):
            own = cond[layer]
            g_row[layer] = conduct(own, plus(own, 0))
            g_col[layer] = conduct(own, plus(own, 1))
            g_up[layer + 1] = conduct(own, cond[layer + 1])
            return carry

        g_up[0] = jnp.zeros((24, 256), F32)
        lax.fori_loop(0, 16, conductances, 0)

        def heat_step(source, layer):
            own = source[layer]
            above, below = source[jnp.minimum(layer + 1, 15)], source[jnp.maximum(layer - 1, 0)]
            row_flux = g_row[layer] * (plus(own, 0) - own)
            col_flux = g_col[layer] * (plus(own, 1) - own)
            flux = row_flux - minus(row_flux, 0) + col_flux - minus(col_flux, 1)
            flux = flux + g_up[layer + 1] * (above - own) + g_up[layer] * (below - own)
            return own + rate[layer] * (flux + power[layer])

        def heat_one(layer, carry):
            temp_one[layer] = heat_step(temp, layer)
            return carry

        lax.fori_loop(0, 16, heat_one, 0)

        def heat_two(layer, carry):
            warm = heat_step(temp_one, layer)[0:16, 0:128]
            warmed_out[layer] = warm
            strain[layer] = lookup(label[layer, 0:16, 0:128], expansion) * warm
            return carry

        lax.fori_loop(0, 16, heat_two, 0)

        start = jnp.where(gz == 0, 0, 124)

        def pack_strain(layer, acc):
            for half in range(2):
                slot = layer * 2 + half
                moved = pltpu.roll(strain[layer, 8 * half : 8 * half + 8], lax.rem(slot * 4 + 128 - start, 128), 1)
                acc = jnp.where((lane >> 2) == slot, moved, acc)
            return acc

        packed_strain[...] = lax.fori_loop(0, 16, pack_strain, jnp.zeros((8, 128), F32))
        strains = elastic_sends(strain, lambda dz: 4 * dz, e_strain, packed_strain, strain_strips)

        def own_strain(layer, carry):
            e_strain[layer, 0:16, own_lanes] = strain[layer + 4 * gz]
            return carry

        lax.fori_loop(0, 12, own_strain, 0)

        for ref in (base, field, lanes):
            for n in range(ref.shape[0]):
                for m in range(ref.shape[1]):
                    ref[n, m, 0] = jnp.zeros((24, 384), F32)

        largest = jnp.maximum(jnp.maximum(modulus[0], modulus[1]), jnp.maximum(modulus[2], modulus[3]))
        scale = SPAN * largest
        inverse = 1.0 / jnp.full((1, 128), scale, F32)
        scaled = [m * inverse for m in modulus]

        for copy in labels:
            copy.wait_recv()
        for copy in strains:
            copy.wait_recv()

        e_label_halo = halo_blocks(lambda side, d: label_strips[side, d + 1])
        e_strain_halo = halo_blocks(lambda side, d: strain_strips[side, d + 1])

        def stacked(layer):
            return jnp.where(gz == 0, layer, 11 - layer)

        def spread(ref, n, layer, value):
            ahead, behind = plus(value, 1), minus(value, 1)
            ref[n, 0, layer + 1] = value
            ref[n, 1, layer + 1] = ahead + behind
            ref[n, 2, layer + 1] = ahead - behind

        def base_fields(layer, carry):
            raw = stacked(layer)
            ids = [e_label[raw, :, 0:128], e_label[raw, :, 128:256]]
            hot = [e_strain[raw, :, 0:128], e_strain[raw, :, 128:256]]
            whole = raw + 4 * gz
            ids.append(e_label_halo(whole).astype(jnp.int32))
            hot.append(e_strain_halo(whole))
            stiffness = [jnp.where(e_ok[n], lookup(ids[n], scaled), 0.0) for n in range(3)]
            hot = [jnp.where(e_ok[n], hot[n], 0.0) for n in range(3)]
            e = jnp.concatenate(stiffness, axis=1)
            s = jnp.concatenate(hot, axis=1)
            spread(base, 0, layer, e)
            spread(base, 1, layer, s)
            spread(base, 2, layer, e * s)
            return carry

        lax.fori_loop(0, 12, base_fields, 0)

        cuts = [slice(128 * n, 128 * n + 128) for n in range(3)]

        def put(step, layer, chunks):
            e = base[0, 0, layer + 1]
            for comp in range(3):
                value = jnp.concatenate(chunks[comp], axis=1)
                field[step, comp, layer + 1] = value
                if step < 3:
                    ahead, behind = plus(value, 1), minus(value, 1)
                    slot = (step % 2) * 5
                    lanes[slot, comp, layer + 1] = ahead + behind
                    lanes[slot + 1, comp, layer + 1] = ahead - behind
                    value = e * value
                    ahead, behind = plus(value, 1), minus(value, 1)
                    lanes[slot + 2, comp, layer + 1] = value
                    lanes[slot + 3, comp, layer + 1] = ahead + behind
                    lanes[slot + 4, comp, layer + 1] = ahead - behind

        def first_vector(layer, carry):
            chunks = [[], [], []]
            for cut in cuts:
                def get(n):
                    return lambda kind, dz: base[n, kind, layer + 1 + dz, :, cut]

                e, s = base[0, 0, layer + 1, :, cut], base[1, 0, layer + 1, :, cut]
                inside = e > 0.0
                de, ds, des = gradient(get(0)), gradient(get(1)), gradient(get(2))
                for comp in range(3):
                    load = -(e * ds[comp] + s * de[comp] + des[comp])
                    chunks[comp].append(jnp.where(inside, load, 0.0))
                for n, value in enumerate(scalar_stencils(get(0))):
                    stiff[n, layer, :, cut] = value
            put(0, layer, chunks)
            return carry

        lax.fori_loop(0, 11, first_vector, 0)

        def next_vector(step, layer):
            chunks = [[], [], []]
            slot = (step % 2) * 5
            for cut in cuts:
                def plain(comp, kind, dz):
                    if kind == 0:
                        return field[step, comp, layer + 1 + dz, :, cut]
                    return lanes[slot + kind - 1, comp, layer + 1 + dz, :, cut]

                def weighted(comp, kind, dz):
                    return lanes[slot + 2 + kind, comp, layer + 1 + dz, :, cut]

                ku, kw = stencil(plain), stencil(weighted)
                e = base[0, 0, layer + 1, :, cut]
                inside = e > 0.0
                zz, xx, yy, zx, zy, xy = [stiff[n, layer, :, cut] for n in range(6)]
                u = [plain(comp, 0, 0) for comp in range(3)]
                gu = [
                    zz * u[0] + zx * u[1] + zy * u[2],
                    zx * u[0] + xx * u[1] + xy * u[2],
                    zy * u[0] + xy * u[1] + yy * u[2],
                ]
                for comp in range(3):
                    value = e * (DIAGONAL * u[comp] - ku[comp]) + gu[comp] - kw[comp] - TAU * u[comp]
                    chunks[comp].append(jnp.where(inside, value, 0.0))
            put(step + 1, layer, chunks)

        for step in range(3):
            def body(layer, carry, step=step):
                next_vector(step, layer)
                return carry

            lax.fori_loop(0, 10 - step, body, 0)

        def products(layer, acc):
            acc = list(acc)
            for comp in range(3):
                for half in range(2):
                    for n in range(2):
                        v = [
                            field[step, comp, layer + 1, 8 * half : 8 * half + 8, 128 * n : 128 * n + 128]
                            for step in range(4)
                        ]
                        for k in range(6):
                            acc[k] = acc[k] + v[k // 2] * v[k - k // 2]
            return tuple(acc)

        acc = lax.fori_loop(0, 8, products, tuple(jnp.zeros((8, 128), F32) for _ in range(6)))
        mine = jnp.zeros((8, 128), F32)
        for k in range(6):
            mine = jnp.where(sub == k, jnp.sum(acc[k], axis=0, keepdims=True), mine)
        sums[...] = mine

        def reduce_over(ring, src, dst):
            copies = [remote(src, dst.at[n], peer) for n, peer in enumerate(ring)]
            for copy in copies:
                copy.wait_recv()
            value = src[...]
            for n in range(len(ring)):
                value = value + dst[n]
            return copies, value

        first, value = reduce_over(ring_a, sums, sums_a)
        total_a[...] = value
        second, value = reduce_over(ring_b, total_a, sums_b)

        total = jnp.sum(value, axis=1, keepdims=True)
        moments = [total[k : k + 1] for k in range(6)]
        x_of, r_of = iterate_coefficients(moments)
        x_of = [jnp.broadcast_to(c, (16, 256)) for c in x_of]
        r_of = [jnp.broadcast_to(c * scale, (16, 256)) for c in r_of]
        sign = jnp.where(gz == 0, 1.0, -1.0)

        def outputs(layer, carry):
            place = jnp.where(gz == 0, layer, 7 - layer)
            for comp in range(3):
                v = [field[step, comp, layer + 1, 0:16, 0:256] for step in range(4)]
                x = x_of[0] * v[0] + x_of[1] * v[1] + x_of[2] * v[2]
                r = r_of[0] * v[0] + r_of[1] * v[1] + r_of[2] * v[2] + r_of[3] * v[3]
                solution_out[comp, place] = x * sign if comp == 0 else x
                residual_out[comp, place] = r * sign if comp == 0 else r
            return carry

        lax.fori_loop(0, 8, outputs, 0)

        for copy in heat + labels + strains + first + second:
            copy.wait_send()

    return kernel


def solution(mesh):
    sizes = dict(mesh.shape)
    copies = 12 + 11 + 11 + (2 * sizes["gx"] - 1) + (sizes["gy"] - 1)

    def per_device(kelvin, label, patch, traits, intensity):
        hbm = pl.BlockSpec(memory_space=pltpu.HBM)
        smem = pl.BlockSpec(memory_space=pltpu.SMEM)
        vmem = pl.BlockSpec(memory_space=pltpu.VMEM)
        heat = lambda layers=16, kind=F32: pltpu.VMEM((layers, 24, 256), kind)
        block = lambda *lead: pltpu.VMEM((*lead, 8, 128), F32)
        wide = lambda *lead: pltpu.VMEM((*lead, 24, 384), F32)
        return pl.pallas_call(
            make_kernel(sizes),
            out_shape=(
                jax.ShapeDtypeStruct((16, 16, 128), F32),
                jax.ShapeDtypeStruct((3, 8, 16, 256), F32),
                jax.ShapeDtypeStruct((3, 8, 16, 256), F32),
            ),
            in_specs=[hbm, hbm, hbm, smem, smem],
            out_specs=(vmem, vmem, vmem),
            scratch_shapes=[
                heat(), heat(kind=jnp.int32), heat(kind=jnp.int32),
                heat(17), heat(), heat(), heat(), heat(), heat(17), heat(),
                block(2, 3), block(2, 3, 3), block(), block(2, 3), block(2, 3),
                pltpu.VMEM((16, 16, 128), F32),
                pltpu.VMEM((12, 24, 384), jnp.int32), wide(12),
                wide(3, 3, 13), wide(4, 3, 13), wide(10, 3, 13), wide(6, 11),
                block(), block(2 * sizes["gx"] - 1), block(sizes["gy"] - 1), block(),
                pltpu.SemaphoreType.DMA((4,)),
                pltpu.SemaphoreType.DMA((copies,)),
                pltpu.SemaphoreType.DMA((copies,)),
            ],
            compiler_params=pltpu.CompilerParams(
                collective_id=0, has_side_effects=True, vmem_limit_bytes=60 * 1024 * 1024
            ),
        )(kelvin, label, patch, traits, intensity)

    columns = P(None, "gx", ("gy", "gz"))
    return jax.shard_map(
        per_device,
        mesh=mesh,
        in_specs=(columns, columns, columns, P(), P()),
        out_specs=(columns, P(None, "gz", "gx", "gy"), P(None, "gz", "gx", "gy")),
        check_vma=False,
    )
```

```python
import jax
import jax.numpy as jnp
from jax import lax
from jax.experimental import pallas as pl
from jax.experimental.pallas import tpu as pltpu
from jax.sharding import PartitionSpec as P

MESH = pl.DeviceIdType.MESH
F32 = jnp.float32
TIME_STEP = 0.03
TAU = 4.0 / 3.0
SPAN = 6.0
DIAGONAL = 0.5 + 2.5 + 2.5 + 10.0 / 9.0


def plus(value, axis):
    return pltpu.roll(value, value.shape[axis] - 1, axis)


def minus(value, axis):
    return pltpu.roll(value, 1, axis)


def tree(bits, entries):
    while len(entries) > 1:
        mask, bits = bits[0], bits[1:]
        entries = [jnp.where(mask, entries[i + 1], entries[i]) for i in range(0, len(entries), 2)]
    return entries[0]


def lookup(identity, entries):
    bits, width = [], 1
    while width < len(entries):
        bits.append((identity & width) != 0)
        width *= 2
    return tree(bits, entries)


def conduct(own, other):
    return 2.0 * own * other / jnp.maximum(own + other, 0.25)


def stencil(get):
    def both(comp, kind):
        up, down = get(comp, kind, 1), get(comp, kind, -1)
        return up + down, up - down

    z, x, y = 0, 1, 2
    e, p, q = 0, 1, 2
    pz_ez, qz_ez = both(z, e)
    pz_pz, qz_pz = both(z, p)
    pz_ex, qz_ex = both(x, e)
    pz_px, qz_px = both(x, p)
    pz_qx = get(x, q, 1) + get(x, q, -1)
    pz_qy, qz_qy = both(y, q)
    qz_qz = get(z, q, 1) - get(z, q, -1)
    e_z, p_z = get(z, e, 0), get(z, p, 0)
    e_x, p_x = get(x, e, 0), get(x, p, 0)
    p_y = get(y, p, 0)
    eighth, corner, mixed = 0.125, 5.0 / 36.0, 1.0 / 18.0
    parts = []
    parts.append((
        0.25 * (p_z + pz_pz) + 0.75 * pz_ez + eighth * qz_qy,
        0.25 * (e_z + pz_ez) + eighth * p_z + corner * pz_pz + mixed * qz_qy,
        eighth * qz_ex + mixed * qz_px,
    ))
    shared = 0.25 * (p_x + pz_ex)
    parts.append((
        shared + eighth * pz_px,
        0.75 * e_x + shared + corner * pz_px,
        eighth * (get(y, q, 0) + qz_ez) + mixed * (pz_qy + qz_pz),
    ))
    pz_ey = get(y, e, 1) + get(y, e, -1)
    pz_py = get(y, p, 1) + get(y, p, -1)
    parts.append((
        0.75 * p_y + 0.25 * (pz_ey + pz_py) + eighth * qz_qz,
        0.25 * (get(y, e, 0) + p_y) + eighth * pz_ey + corner * pz_py + mixed * qz_qz,
        eighth * get(x, q, 0) + mixed * pz_qx,
    ))
    return [c + plus(a + b, 0) + minus(a - b, 0) for c, a, b in parts]


def scalar_stencils(get):
    e, p, q = 0, 1, 2
    pz_e, qz_e = get(e, 1) + get(e, -1), get(e, 1) - get(e, -1)
    pz_p, qz_p = get(p, 1) + get(p, -1), get(p, 1) - get(p, -1)
    pz_q, qz_q = get(q, 1) + get(q, -1), get(q, 1) - get(q, -1)
    e0, p0, q0 = get(e, 0), get(p, 0), get(q, 0)
    eighth, corner, mixed = 0.125, 5.0 / 36.0, 1.0 / 18.0

    def even(c, a):
        return c + plus(a, 0) + minus(a, 0)

    def odd(b):
        return plus(b, 0) - minus(b, 0)

    return [
        even(0.25 * (p0 + pz_p) + 0.75 * pz_e, 0.25 * (e0 + pz_e) + eighth * p0 + corner * pz_p),
        even(0.25 * (p0 + pz_e) + eighth * pz_p, 0.75 * e0 + 0.25 * (p0 + pz_e) + corner * pz_p),
        even(0.75 * p0 + 0.25 * (pz_e + pz_p), 0.25 * (e0 + p0) + eighth * pz_e + corner * pz_p),
        odd(eighth * qz_e + mixed * qz_p),
        even(eighth * qz_q, mixed * qz_q),
        odd(eighth * q0 + mixed * pz_q),
    ]


def gradient(get):
    e, p, q = 0, 1, 2
    qz_e, qz_p = get(e, 1) - get(e, -1), get(p, 1) - get(p, -1)
    pz_e, pz_p = get(e, 1) + get(e, -1), get(p, 1) + get(p, -1)
    q0, pz_q = get(q, 0), get(q, 1) + get(q, -1)
    sixth = 1.0 / 6.0
    a_z = 0.25 * qz_e + sixth * qz_p
    b_x = 0.5 * get(e, 0) + 0.25 * (get(p, 0) + pz_e) + sixth * pz_p
    a_y = 0.25 * q0 + sixth * pz_q
    return [
        0.5 * qz_e + 0.25 * qz_p + plus(a_z, 0) + minus(a_z, 0),
        plus(b_x, 0) - minus(b_x, 0),
        0.5 * q0 + 0.25 * pz_q + plus(a_y, 0) + minus(a_y, 0),
    ]


def poly_dot(first, second, moments):
    total = None
    for i, a in enumerate(first):
        for j, b in enumerate(second):
            term = a * b * moments[i + j]
            total = term if total is None else total + term
    return total


def shifted(poly):
    out = [TAU * c for c in poly] + [jnp.zeros_like(poly[0])]
    for k, c in enumerate(poly):
        out[k + 1] = out[k + 1] + c
    return out


def added(first, second):
    if len(first) < len(second):
        first, second = second, first
    return [a + second[i] if i < len(second) else a for i, a in enumerate(first)]


def iterate_coefficients(moments):
    one = jnp.ones_like(moments[0])
    residual, direction, solution = [one], [one], []
    norm = moments[0]
    for number in range(3):
        image = shifted(direction)
        alpha = norm / poly_dot(direction, image, moments)
        solution = added(solution, [alpha * c for c in direction])
        residual = added([-alpha * c for c in image], residual)
        if number < 2:
            following = poly_dot(residual, residual, moments)
            ratio = following / norm
            direction = added(residual, [ratio * c for c in direction])
            norm = following
    return solution, residual


def grouped(total, size, body, init):
    def trip(number, carry):
        for k in range(size):
            carry = body(number * size + k, carry)
        return carry

    return lax.fori_loop(0, total // size, trip, init)


def make_kernel(sizes):
    nx, ny = sizes["gx"], sizes["gy"]
    group_a, group_b = nx * 2, ny

    def kernel(
        kelvin_in, label_in, patch_in, traits, intensity,
        warmed_out, solution_out, residual_out,
        temp, label, patch, cond, rate, power, g_row, g_row_back, g_col, g_col_back, g_up, temp_one,
        packs, strips, packed_strain, strain_strips, label_strips,
        strain, e_label, e_strain, base, field, lanes, stiff,
        sums, sums_a, sums_b, total_a,
        local_sem, send, recv,
    ):
        gx, gy, gz = lax.axis_index("gx"), lax.axis_index("gy"), lax.axis_index("gz")
        other = 1 - gz
        nexts = {-1: lax.rem(gx + nx - 1, nx), 0: gx, 1: lax.rem(gx + 1, nx)}
        gy_up, gy_down = lax.rem(gy + 1, ny), lax.rem(gy + ny - 1, ny)
        own_lanes = pl.ds(pl.multiple_of(gz * 128, 128), 128)

        loads = [
            pltpu.make_async_copy(kelvin_in, temp.at[:, 0:16, 0:128], local_sem.at[0]),
            pltpu.make_async_copy(label_in, label.at[:, 0:16, 0:128], local_sem.at[1]),
            pltpu.make_async_copy(patch_in, patch.at[:, 0:16, 0:128], local_sem.at[2]),
            pltpu.make_async_copy(
                label_in.at[pl.ds(4 * gz, 12)], e_label.at[:, 0:16, own_lanes], local_sem.at[3]
            ),
        ]
        for copy in loads:
            copy.start()
        temp[:, 16:24, 0:128] = jnp.zeros((16, 8, 128), F32)
        label[:, 16:24, 0:128] = jnp.zeros((16, 8, 128), jnp.int32)
        patch[:, 16:24, 0:128] = jnp.zeros((16, 8, 128), jnp.int32)
        for side in range(2):
            for d in (0, 2):
                strips[side, d] = jnp.zeros((2, 8, 128), F32)

        barrier = pltpu.get_barrier_semaphore()
        peers = [
            (nexts[dx], dy, dz)
            for dx in (-1, 0, 1)
            for dy in (gy, gy_up, gy_down)
            for dz in (gz, other)
            if not (dx == 0 and dy is gy and dz is gz)
        ]
        number_a = gx * 2 + gz
        ring_a = []
        for step in range(1, group_a):
            there = lax.rem(number_a + step, group_a)
            ring_a.append((there // 2, gy, lax.rem(there, 2)))
        ring_b = [(gx, lax.rem(gy + step, ny), gz) for step in range(1, group_b)]
        everyone = peers + ring_a[2:-2] + ring_b[1:-1] if nx > 2 and ny > 2 else peers + ring_a + ring_b
        for peer in everyone:
            pl.semaphore_signal(barrier, inc=1, device_id=peer, device_id_type=MESH)
        for copy in loads:
            copy.wait()

        lane = lax.broadcasted_iota(jnp.int32, (8, 128), 1)
        sub = lax.broadcasted_iota(jnp.int32, (8, 128), 0)

        def pack_inputs(layer, acc):
            acc = list(acc)
            for half in range(2):
                slot = layer * 2 + half
                rows = slice(8 * half, 8 * half + 8)
                place = lane - slot * 4
                ids = label[layer, rows, 0:128].astype(F32)
                kelvin = temp[layer, rows, 0:128]
                tile_ids = patch[layer, rows, 0:128].astype(F32)
                for side, (four, two) in enumerate(((0, 0), (124, 126))):
                    moved = pltpu.roll(ids, lax.rem(slot * 4 + 128 - four, 128), 1)
                    acc[2 * side] = jnp.where((lane >> 2) == slot, moved, acc[2 * side])
                    moved = pltpu.roll(kelvin, lax.rem(slot * 4 + 128 - two, 128), 1)
                    acc[2 * side + 1] = jnp.where((place >= 0) & (place < 2), moved, acc[2 * side + 1])
                    moved = pltpu.roll(tile_ids, lax.rem(slot * 4 + 130 - two, 128), 1)
                    acc[2 * side + 1] = jnp.where((place >= 2) & (place < 4), moved, acc[2 * side + 1])
            return tuple(acc)

        packed = grouped(16, 8, pack_inputs, tuple(jnp.zeros((8, 128), F32) for _ in range(4)))
        for k in range(4):
            packs[k // 2, k % 2] = packed[k]

        pl.semaphore_wait(barrier, len(everyone))

        count = [0]

        def remote(src, dst, peer):
            n = count[0]
            count[0] += 1
            copy = pltpu.make_async_remote_copy(
                src_ref=src, dst_ref=dst, send_sem=send.at[n], recv_sem=recv.at[n],
                device_id=peer, device_id_type=MESH,
            )
            copy.start()
            return copy

        heat = []
        for ref, deep in ((temp, 2), (label, 2), (patch, 1)):
            up, down = slice(16 - deep, 16), slice(24 - deep, 24)
            heat.append(remote(ref.at[:, 0:deep, 0:128], ref.at[:, 16 : 16 + deep, 0:128], (nexts[-1], gy, gz)))
            heat.append(remote(ref.at[:, up, 0:128], ref.at[:, down, 0:128], (nexts[1], gy, gz)))
        right_gy = jnp.where(gz == 0, gy, gy_up)
        left_gy = jnp.where(gz == 0, gy_down, gy)
        for dx in (0, -1, 1):
            rows = {0: slice(0, 8), -1: slice(0, 2), 1: slice(6, 8)}[dx]
            for side, there in ((0, left_gy), (1, right_gy)):
                heat.append(remote(packs.at[side, :, rows], strips.at[side, 1 - dx, :, rows], (nexts[dx], there, other)))

        side_gy = jnp.where(gz == 0, gy_down, gy_up)

        def elastic_sends(src, src_layers, dst, pack_src, pack_dst):
            out = [remote(src.at[pl.ds(src_layers(other), 12), 0:16, 0:128], dst.at[:, 0:16, own_lanes], (gx, gy, other))]
            for dz in (gz, other):
                layers = pl.ds(src_layers(dz), 12)
                out.append(remote(src.at[layers, 0:4, 0:128], dst.at[:, 16:20, own_lanes], (nexts[-1], gy, dz)))
                out.append(remote(src.at[layers, 12:16, 0:128], dst.at[:, 20:24, own_lanes], (nexts[1], gy, dz)))
                for dx in (0, -1, 1):
                    out.append(remote(pack_src, pack_dst.at[gz, 1 - dx], (nexts[dx], side_gy, dz)))
            return out

        for copy in heat:
            copy.wait_recv()

        labels = elastic_sends(label, lambda dz: 4 * dz, e_label, packs.at[gz, 0], label_strips)

        def halo_blocks(blocks, inset=0, last=252):
            right = [blocks(0, d) for d in (-1, 0, 1)]
            left = [blocks(1, d) for d in (-1, 0, 1)]

            def corner(three):
                return jnp.where(sub < 4, three[2], pltpu.roll(three[0], 124, 1))

            right_corner, left_corner = corner(right), corner(left)

            def at(layer):
                def one(r, l, slot):
                    r = pltpu.roll(r, lax.rem(256 - inset - slot * 4, 128), 1)
                    l = pltpu.roll(l, lax.rem(last - inset - slot * 4, 128), 1)
                    return jnp.where(lane < 64, r, l)

                return jnp.concatenate([
                    one(right[1], left[1], layer * 2),
                    one(right[1], left[1], layer * 2 + 1),
                    one(right_corner, left_corner, layer * 2),
                ], axis=0)

            return at

        label_halo = halo_blocks(lambda side, d: strips[side, d + 1, 0])
        temp_halo = halo_blocks(lambda side, d: strips[side, d + 1, 1], 0, 254)
        patch_halo = halo_blocks(lambda side, d: strips[side, d + 1, 1], 2, 254)

        row = lax.broadcasted_iota(jnp.int32, (24, 128), 0)
        wide_lane = lax.broadcasted_iota(jnp.int32, (24, 128), 1)
        low_row = jnp.where(gx == nx - 1, 16, 24)
        high_row = jnp.where(gx == 0, 20, 32)
        rows_ok = ((row < 16) | ((row >= 16) & (row < 20) & (row < low_row)) | ((row >= 20) & (row < high_row) & (gx > 0)))
        first_tile, last_tile = (gy == 0) & (gz == 0), (gy == ny - 1) & (gz == 1)
        right_limit = jnp.where(last_tile, 0, 64)
        left_limit = jnp.where(first_tile, 128, 64)
        cols_ok = (wide_lane < right_limit) | (wide_lane >= left_limit)
        grid_ok = [rows_ok, rows_ok & cols_ok]
        e_right_limit = jnp.where(gy == ny - 1, 0, 64)
        e_left_limit = jnp.where(gy == 0, 128, 64)
        e_cols_ok = (wide_lane < e_right_limit) | (wide_lane >= e_left_limit)
        e_ok = [rows_ok, rows_ok, rows_ok & e_cols_ok]

        materials = range(4)
        conductivity = [traits[0, m] for m in materials]
        capacity = [traits[1, m] for m in materials]
        modulus = [traits[2, m] for m in materials]
        expansion = [traits[3, m] for m in materials]
        tiles = [intensity[t] for t in range(16)]

        def heat_fields(layer, carry):
            temp[layer, :, 128:256] = temp_halo(layer)
            ids = [label[layer, :, 0:128], label_halo(layer).astype(jnp.int32)]
            tile_ids = [patch[layer, :, 0:128], patch_halo(layer).astype(jnp.int32)]
            for n in range(2):
                cut = slice(128 * n, 128 * n + 128)
                cond[layer, :, cut] = jnp.where(grid_ok[n], lookup(ids[n], conductivity), 0.0)
                rate[layer, :, cut] = TIME_STEP / lookup(ids[n], capacity)
                power[layer, :, cut] = lookup(tile_ids[n], tiles)
            return carry

        grouped(16, 4, heat_fields, 0)
        cond[16] = jnp.zeros((24, 256), F32)

        def conductances(layer, carry):
            own = cond[layer]
            row_g, col_g = conduct(own, plus(own, 0)), conduct(own, plus(own, 1))
            g_row[layer], g_col[layer] = row_g, col_g
            g_row_back[layer], g_col_back[layer] = minus(row_g, 0), minus(col_g, 1)
            g_up[layer + 1] = conduct(own, cond[layer + 1])
            return carry

        g_up[0] = jnp.zeros((24, 256), F32)
        grouped(16, 4, conductances, 0)

        def heat_step(source, layer):
            own = source[layer]
            above, below = source[jnp.minimum(layer + 1, 15)], source[jnp.maximum(layer - 1, 0)]
            flux = g_row[layer] * (plus(own, 0) - own) + g_row_back[layer] * (minus(own, 0) - own)
            flux = flux + g_col[layer] * (plus(own, 1) - own) + g_col_back[layer] * (minus(own, 1) - own)
            flux = flux + g_up[layer + 1] * (above - own) + g_up[layer] * (below - own)
            return own + rate[layer] * (flux + power[layer])

        def heat_one(layer, carry):
            temp_one[layer] = heat_step(temp, layer)
            return carry

        grouped(16, 4, heat_one, 0)

        start = jnp.where(gz == 0, 0, 124)

        def heat_two(layer, acc):
            warm = heat_step(temp_one, layer)[0:16, 0:128]
            warmed_out[layer] = warm
            value = lookup(label[layer, 0:16, 0:128], expansion) * warm
            strain[layer] = value
            for half in range(2):
                slot = layer * 2 + half
                moved = pltpu.roll(value[8 * half : 8 * half + 8], lax.rem(slot * 4 + 128 - start, 128), 1)
                acc = jnp.where((lane >> 2) == slot, moved, acc)
            return acc

        packed_strain[...] = grouped(16, 4, heat_two, jnp.zeros((8, 128), F32))
        strains = elastic_sends(strain, lambda dz: 4 * dz, e_strain, packed_strain, strain_strips)

        def own_strain(layer, carry):
            e_strain[layer, 0:16, own_lanes] = strain[layer + 4 * gz]
            return carry

        lax.fori_loop(0, 12, own_strain, 0)

        for ref in (base, field, lanes):
            for n in range(ref.shape[0]):
                for m in range(ref.shape[1]):
                    ref[n, m, 0] = jnp.zeros((24, 384), F32)

        largest = jnp.maximum(jnp.maximum(modulus[0], modulus[1]), jnp.maximum(modulus[2], modulus[3]))
        scale = SPAN * largest
        inverse = 1.0 / jnp.full((1, 128), scale, F32)
        scaled = [m * inverse for m in modulus]

        for copy in labels:
            copy.wait_recv()
        for copy in strains:
            copy.wait_recv()

        e_label_halo = halo_blocks(lambda side, d: label_strips[side, d + 1])
        e_strain_halo = halo_blocks(lambda side, d: strain_strips[side, d + 1])

        def stacked(layer):
            return jnp.where(gz == 0, layer, 11 - layer)

        def spread(ref, n, layer, value):
            ahead, behind = plus(value, 1), minus(value, 1)
            ref[n, 0, layer + 1] = value
            ref[n, 1, layer + 1] = ahead + behind
            ref[n, 2, layer + 1] = ahead - behind

        def base_fields(layer, carry):
            raw = stacked(layer)
            ids = [e_label[raw, :, 0:128], e_label[raw, :, 128:256]]
            hot = [e_strain[raw, :, 0:128], e_strain[raw, :, 128:256]]
            whole = raw + 4 * gz
            ids.append(e_label_halo(whole).astype(jnp.int32))
            hot.append(e_strain_halo(whole))
            stiffness = [jnp.where(e_ok[n], lookup(ids[n], scaled), 0.0) for n in range(3)]
            hot = [jnp.where(e_ok[n], hot[n], 0.0) for n in range(3)]
            e = jnp.concatenate(stiffness, axis=1)
            s = jnp.concatenate(hot, axis=1)
            spread(base, 0, layer, e)
            spread(base, 1, layer, s)
            spread(base, 2, layer, e * s)
            return carry

        grouped(12, 2, base_fields, 0)

        cuts = [slice(128 * n, 128 * n + 128) for n in range(3)]

        def put(step, layer, chunks):
            e = base[0, 0, layer + 1]
            for comp in range(3):
                value = jnp.concatenate(chunks[comp], axis=1)
                if step == 3:
                    field[step, comp, layer + 1, 0:16, 0:256] = value[0:16]
                else:
                    field[step, comp, layer + 1] = value
                    ahead, behind = plus(value, 1), minus(value, 1)
                    slot = (step % 2) * 5
                    lanes[slot, comp, layer + 1] = ahead + behind
                    lanes[slot + 1, comp, layer + 1] = ahead - behind
                    value = e * value
                    ahead, behind = plus(value, 1), minus(value, 1)
                    lanes[slot + 2, comp, layer + 1] = value
                    lanes[slot + 3, comp, layer + 1] = ahead + behind
                    lanes[slot + 4, comp, layer + 1] = ahead - behind

        def first_vector(layer, carry):
            chunks = [[], [], []]
            for cut in cuts:
                def get(n):
                    return lambda kind, dz: base[n, kind, layer + 1 + dz, :, cut]

                e, s = base[0, 0, layer + 1, :, cut], base[1, 0, layer + 1, :, cut]
                inside = e > 0.0
                de, ds, des = gradient(get(0)), gradient(get(1)), gradient(get(2))
                for comp in range(3):
                    load = -(e * ds[comp] + s * de[comp] + des[comp])
                    chunks[comp].append(jnp.where(inside, load, 0.0))
                for n, value in enumerate(scalar_stencils(get(0))):
                    stiff[n, layer, :, cut] = value
            put(0, layer, chunks)
            return carry

        lax.fori_loop(0, 11, first_vector, 0)

        def next_vector(step, layer):
            chunks = [[], [], []]
            slot = (step % 2) * 5
            for cut in cuts if step < 2 else cuts[:2]:
                def plain(comp, kind, dz):
                    if kind == 0:
                        return field[step, comp, layer + 1 + dz, :, cut]
                    return lanes[slot + kind - 1, comp, layer + 1 + dz, :, cut]

                def weighted(comp, kind, dz):
                    return lanes[slot + 2 + kind, comp, layer + 1 + dz, :, cut]

                ku, kw = stencil(plain), stencil(weighted)
                e = base[0, 0, layer + 1, :, cut]
                inside = e > 0.0
                zz, xx, yy, zx, zy, xy = [stiff[n, layer, :, cut] for n in range(6)]
                u = [plain(comp, 0, 0) for comp in range(3)]
                gu = [
                    zz * u[0] + zx * u[1] + zy * u[2],
                    zx * u[0] + xx * u[1] + xy * u[2],
                    zy * u[0] + xy * u[1] + yy * u[2],
                ]
                for comp in range(3):
                    value = e * (DIAGONAL * u[comp] - ku[comp]) + gu[comp] - kw[comp] - TAU * u[comp]
                    chunks[comp].append(jnp.where(inside, value, 0.0))
            put(step + 1, layer, chunks)

        for step in range(3):
            def body(layer, carry, step=step):
                next_vector(step, layer)
                return carry

            lax.fori_loop(0, 10 - step, body, 0)

        def products(layer, acc):
            acc = list(acc)
            for comp in range(3):
                for half in range(2):
                    for n in range(2):
                        v = [
                            field[step, comp, layer + 1, 8 * half : 8 * half + 8, 128 * n : 128 * n + 128]
                            for step in range(4)
                        ]
                        for k in range(6):
                            acc[k] = acc[k] + v[k // 2] * v[k - k // 2]
            return tuple(acc)

        acc = lax.fori_loop(0, 8, products, tuple(jnp.zeros((8, 128), F32) for _ in range(6)))
        mine = jnp.zeros((8, 128), F32)
        for k in range(6):
            mine = jnp.where(sub == k, jnp.sum(acc[k], axis=0, keepdims=True), mine)
        mine = jnp.sum(mine, axis=1, keepdims=True)
        sums[...] = jnp.sum(jnp.where(lane == sub, mine, 0.0), axis=0, keepdims=True)

        def reduce_over(ring, src, dst):
            copies = [remote(src, dst.at[n], peer) for n, peer in enumerate(ring)]
            for copy in copies:
                copy.wait_recv()
            value = src[...]
            for n in range(len(ring)):
                value = value + dst[n]
            return copies, value

        first, value = reduce_over(ring_a, sums, sums_a)
        total_a[...] = value
        second, value = reduce_over(ring_b, total_a, sums_b)

        moments = [value[:, k : k + 1] for k in range(6)]
        x_of, r_of = iterate_coefficients(moments)
        x_of = [jnp.broadcast_to(c, (16, 256)) for c in x_of]
        r_of = [jnp.broadcast_to(c * scale, (16, 256)) for c in r_of]
        sign = jnp.where(gz == 0, 1.0, -1.0)

        def outputs(layer, carry):
            place = jnp.where(gz == 0, layer, 7 - layer)
            for comp in range(3):
                v = [field[step, comp, layer + 1, 0:16, 0:256] for step in range(4)]
                x = x_of[0] * v[0] + x_of[1] * v[1] + x_of[2] * v[2]
                r = r_of[0] * v[0] + r_of[1] * v[1] + r_of[2] * v[2] + r_of[3] * v[3]
                solution_out[comp, place] = x * sign if comp == 0 else x
                residual_out[comp, place] = r * sign if comp == 0 else r
            return carry

        lax.fori_loop(0, 8, outputs, 0)

        for copy in heat + labels + strains + first + second:
            copy.wait_send()

    return kernel


def copy_out(*refs):
    sems = refs[-1]
    copies = [pltpu.make_async_copy(refs[n], refs[n + 3], sems.at[n]) for n in range(3)]
    for copy in copies:
        copy.start()
    for copy in copies:
        copy.wait()


def solution(mesh):
    sizes = dict(mesh.shape)
    hbm = pl.BlockSpec(memory_space=pltpu.HBM)
    smem = pl.BlockSpec(memory_space=pltpu.SMEM)
    vmem = pl.BlockSpec(memory_space=pltpu.VMEM)
    copies = 12 + 11 + 11 + (2 * sizes["gx"] - 1) + (sizes["gy"] - 1)

    def per_device(kelvin, label, patch, traits, intensity):
        heat = lambda layers=16, kind=F32: pltpu.VMEM((layers, 24, 256), kind)
        block = lambda *lead: pltpu.VMEM((*lead, 8, 128), F32)
        wide = lambda *lead: pltpu.VMEM((*lead, 24, 384), F32)
        row = lambda *lead: pltpu.VMEM((*lead, 1, 128), F32)
        shapes = (
            jax.ShapeDtypeStruct((16, 16, 128), F32),
            jax.ShapeDtypeStruct((3, 8, 16, 256), F32),
            jax.ShapeDtypeStruct((3, 8, 16, 256), F32),
        )
        results = pl.pallas_call(
            make_kernel(sizes),
            out_shape=shapes,
            in_specs=[hbm, hbm, hbm, smem, smem],
            out_specs=(vmem, vmem, vmem),
            scratch_shapes=[
                heat(), heat(kind=jnp.int32), heat(kind=jnp.int32),
                heat(17), heat(), heat(), heat(), heat(), heat(), heat(), heat(17), heat(),
                block(2, 2), block(2, 3, 2), block(), block(2, 3), block(2, 3),
                pltpu.VMEM((16, 16, 128), F32),
                pltpu.VMEM((12, 24, 384), jnp.int32), wide(12),
                wide(3, 3, 13), wide(4, 3, 13), wide(10, 3, 13), wide(6, 11),
                row(), row(2 * sizes["gx"] - 1), row(sizes["gy"] - 1), row(),
                pltpu.SemaphoreType.DMA((4,)),
                pltpu.SemaphoreType.DMA((copies,)),
                pltpu.SemaphoreType.DMA((copies,)),
            ],
            compiler_params=pltpu.CompilerParams(
                collective_id=0, has_side_effects=True, vmem_limit_bytes=60 * 1024 * 1024
            ),
        )(kelvin, label, patch, traits, intensity)
        return pl.pallas_call(
            copy_out,
            out_shape=shapes,
            in_specs=[vmem, vmem, vmem],
            out_specs=(hbm, hbm, hbm),
            scratch_shapes=[pltpu.SemaphoreType.DMA((3,))],
        )(*results)

    columns = P(None, "gx", ("gy", "gz"))
    return jax.shard_map(
        per_device,
        mesh=mesh,
        in_specs=(columns, columns, columns, P(), P()),
        out_specs=(columns, P(None, "gz", "gx", "gy"), P(None, "gz", "gx", "gy")),
        check_vma=False,
    )
```

```python
import jax
import jax.numpy as jnp
from jax import lax
from jax.experimental import pallas as pl
from jax.experimental.pallas import tpu as pltpu
from jax.sharding import PartitionSpec as P

MESH = pl.DeviceIdType.MESH
F32 = jnp.float32
TIME_STEP = 0.03
TAU = 4.0 / 3.0
SPAN = 6.0
DIAGONAL = 0.5 + 2.5 + 2.5 + 10.0 / 9.0


def plus(value, axis):
    return pltpu.roll(value, value.shape[axis] - 1, axis)


def minus(value, axis):
    return pltpu.roll(value, 1, axis)


def tree(bits, entries):
    while len(entries) > 1:
        mask, bits = bits[0], bits[1:]
        entries = [jnp.where(mask, entries[i + 1], entries[i]) for i in range(0, len(entries), 2)]
    return entries[0]


def lookup(identity, entries):
    bits, width = [], 1
    while width < len(entries):
        bits.append((identity & width) != 0)
        width *= 2
    return tree(bits, entries)


def conduct(own, other):
    return 2.0 * own * other / jnp.maximum(own + other, 0.25)


CORNER, MIXED = 10.0 / 9.0, 4.0 / 9.0
Z, X, Y = 0, 1, 2
KEPT, SUM, DIFF = 0, 1, 2


def even(get, *which):
    return get(*which, 1) + get(*which, -1)


def odd(get, *which):
    return get(*which, 1) - get(*which, -1)


def stencil(get, comp):
    if comp == Z:
        e, p = get(Z, KEPT, 0), get(Z, SUM, 0)
        pe, pp, qq = even(get, Z, KEPT), even(get, Z, SUM), odd(get, Y, DIFF)
        return (
            2.0 * (p + pp) + 6.0 * pe + qq,
            2.0 * (e + pe) + p + CORNER * pp + MIXED * qq,
            odd(get, X, KEPT) + MIXED * odd(get, X, SUM),
        )
    if comp == X:
        shared = 2.0 * (get(X, SUM, 0) + even(get, X, KEPT))
        pp = even(get, X, SUM)
        return (
            shared + pp,
            6.0 * get(X, KEPT, 0) + shared + CORNER * pp,
            get(Y, DIFF, 0) + odd(get, Z, KEPT) + MIXED * (even(get, Y, DIFF) + odd(get, Z, SUM)),
        )
    p, pe, pp, qq = get(Y, SUM, 0), even(get, Y, KEPT), even(get, Y, SUM), odd(get, Z, DIFF)
    return (
        6.0 * p + 2.0 * (pe + pp) + qq,
        2.0 * (get(Y, KEPT, 0) + p) + pe + CORNER * pp + MIXED * qq,
        get(X, DIFF, 0) + MIXED * even(get, X, DIFF),
    )


def scalar_stencils(get):
    e, p, q = get(KEPT, 0), get(SUM, 0), get(DIFF, 0)
    pe, pp, qe, qp = even(get, KEPT), even(get, SUM), odd(get, KEPT), odd(get, SUM)
    pq, qq = even(get, DIFF), odd(get, DIFF)

    def evenly(c, a):
        return c + plus(a, 0) + minus(a, 0)

    def oddly(b):
        return plus(b, 0) - minus(b, 0)

    shared = 2.0 * (p + pe)
    yield evenly(2.0 * (p + pp) + 6.0 * pe, 2.0 * (e + pe) + p + CORNER * pp)
    yield evenly(shared + pp, 6.0 * e + shared + CORNER * pp)
    yield evenly(6.0 * p + 2.0 * (pe + pp), 2.0 * (e + p) + pe + CORNER * pp)
    yield oddly(qe + MIXED * qp)
    yield evenly(qq, MIXED * qq)
    yield oddly(q + MIXED * pq)


def gradient(get, comp):
    if comp == Z:
        qe, qp = odd(get, KEPT), odd(get, SUM)
        a = 2.0 * qe + 4.0 / 3.0 * qp
        return 4.0 * qe + 2.0 * qp + plus(a, 0) + minus(a, 0)
    if comp == X:
        b = 4.0 * get(KEPT, 0) + 2.0 * (get(SUM, 0) + even(get, KEPT)) + 4.0 / 3.0 * even(get, SUM)
        return plus(b, 0) - minus(b, 0)
    q, pq = get(DIFF, 0), even(get, DIFF)
    a = 2.0 * q + 4.0 / 3.0 * pq
    return 4.0 * q + 2.0 * pq + plus(a, 0) + minus(a, 0)


def poly_dot(first, second, moments):
    total = None
    for i, a in enumerate(first):
        for j, b in enumerate(second):
            term = a * b * moments[i + j]
            total = term if total is None else total + term
    return total


def shifted(poly):
    out = [TAU * c for c in poly] + [jnp.zeros_like(poly[0])]
    for k, c in enumerate(poly):
        out[k + 1] = out[k + 1] + c
    return out


def added(first, second):
    if len(first) < len(second):
        first, second = second, first
    return [a + second[i] if i < len(second) else a for i, a in enumerate(first)]


def iterate_coefficients(moments):
    one = jnp.ones_like(moments[0])
    residual, direction, solution = [one], [one], []
    norm = moments[0]
    for number in range(3):
        image = shifted(direction)
        alpha = norm / poly_dot(direction, image, moments)
        solution = added(solution, [alpha * c for c in direction])
        residual = added([-alpha * c for c in image], residual)
        if number < 2:
            following = poly_dot(residual, residual, moments)
            ratio = following / norm
            direction = added(residual, [ratio * c for c in direction])
            norm = following
    return solution, residual


def grouped(total, size, body, init):
    def trip(number, carry):
        for k in range(size):
            carry = body(number * size + k, carry)
        return carry

    return lax.fori_loop(0, total // size, trip, init)


def make_kernel(sizes):
    nx, ny = sizes["gx"], sizes["gy"]
    group_a, group_b = nx * 2, ny

    def kernel(
        kelvin_in, label_in, patch_in, traits, intensity,
        warmed_hbm, solution_hbm, residual_hbm,
        warmed_out, solution_out, residual_out,
        temp, label, patch, cond, rate, power, g_row, g_row_back, g_col, g_col_back, g_up, temp_one,
        packs, strips, packed_strain, strain_strips, label_strips,
        strain, e_label, e_strain, base, beside, field, lanes, stiff,
        sums, sums_a, sums_b, total_a,
        local_sem, out_sem, send, recv,
    ):
        gx, gy, gz = lax.axis_index("gx"), lax.axis_index("gy"), lax.axis_index("gz")
        other = 1 - gz
        nexts = {-1: lax.rem(gx + nx - 1, nx), 0: gx, 1: lax.rem(gx + 1, nx)}
        gy_up, gy_down = lax.rem(gy + 1, ny), lax.rem(gy + ny - 1, ny)
        own_lanes = pl.ds(pl.multiple_of(gz * 128, 128), 128)

        loads = [
            pltpu.make_async_copy(kelvin_in, temp.at[:, 0:16, 0:128], local_sem.at[0]),
            pltpu.make_async_copy(label_in, label.at[:, 0:16, 0:128], local_sem.at[1]),
            pltpu.make_async_copy(patch_in, patch.at[:, 0:16, 0:128], local_sem.at[2]),
            pltpu.make_async_copy(
                label_in.at[pl.ds(4 * gz, 12)], e_label.at[:, 0:16, own_lanes], local_sem.at[3]
            ),
        ]
        for copy in loads:
            copy.start()
        temp[:, 16:24, 0:128] = jnp.zeros((16, 8, 128), F32)
        label[:, 16:24, 0:128] = jnp.zeros((16, 8, 128), jnp.int32)
        patch[:, 16:24, 0:128] = jnp.zeros((16, 8, 128), jnp.int32)
        for side in range(2):
            for d in (0, 2):
                strips[side, d] = jnp.zeros((2, 8, 128), F32)

        barrier = pltpu.get_barrier_semaphore()
        peers = [
            (nexts[dx], dy, dz)
            for dx in (-1, 0, 1)
            for dy in (gy, gy_up, gy_down)
            for dz in (gz, other)
            if not (dx == 0 and dy is gy and dz is gz)
        ]
        number_a = gx * 2 + gz
        ring_a = []
        for step in range(1, group_a):
            there = lax.rem(number_a + step, group_a)
            ring_a.append((there // 2, gy, lax.rem(there, 2)))
        ring_b = [(gx, lax.rem(gy + step, ny), gz) for step in range(1, group_b)]
        everyone = peers + ring_a[2:-2] + ring_b[1:-1] if nx > 2 and ny > 2 else peers + ring_a + ring_b
        for peer in everyone:
            pl.semaphore_signal(barrier, inc=1, device_id=peer, device_id_type=MESH)
        for copy in loads:
            copy.wait()

        lane = lax.broadcasted_iota(jnp.int32, (8, 128), 1)
        sub = lax.broadcasted_iota(jnp.int32, (8, 128), 0)

        def pack_inputs(layer, acc):
            acc = list(acc)
            for half in range(2):
                slot = layer * 2 + half
                rows = slice(8 * half, 8 * half + 8)
                place = lane - slot * 4
                ids = label[layer, rows, 0:128].astype(F32)
                kelvin = temp[layer, rows, 0:128]
                tile_ids = patch[layer, rows, 0:128].astype(F32)
                for side, (four, two) in enumerate(((0, 0), (124, 126))):
                    moved = pltpu.roll(ids, lax.rem(slot * 4 + 128 - four, 128), 1)
                    acc[2 * side] = jnp.where((lane >> 2) == slot, moved, acc[2 * side])
                    moved = pltpu.roll(kelvin, lax.rem(slot * 4 + 128 - two, 128), 1)
                    acc[2 * side + 1] = jnp.where((place >= 0) & (place < 2), moved, acc[2 * side + 1])
                    moved = pltpu.roll(tile_ids, lax.rem(slot * 4 + 130 - two, 128), 1)
                    acc[2 * side + 1] = jnp.where((place >= 2) & (place < 4), moved, acc[2 * side + 1])
            return tuple(acc)

        packed = grouped(16, 8, pack_inputs, tuple(jnp.zeros((8, 128), F32) for _ in range(4)))
        for k in range(4):
            packs[k // 2, k % 2] = packed[k]

        pl.semaphore_wait(barrier, len(everyone))

        count = [0]

        def remote(src, dst, peer):
            n = count[0]
            count[0] += 1
            copy = pltpu.make_async_remote_copy(
                src_ref=src, dst_ref=dst, send_sem=send.at[n], recv_sem=recv.at[n],
                device_id=peer, device_id_type=MESH,
            )
            copy.start()
            return copy

        heat = []
        for ref, deep in ((temp, 2), (label, 2), (patch, 1)):
            up, down = slice(16 - deep, 16), slice(24 - deep, 24)
            heat.append(remote(ref.at[:, 0:deep, 0:128], ref.at[:, 16 : 16 + deep, 0:128], (nexts[-1], gy, gz)))
            heat.append(remote(ref.at[:, up, 0:128], ref.at[:, down, 0:128], (nexts[1], gy, gz)))
        right_gy = jnp.where(gz == 0, gy, gy_up)
        left_gy = jnp.where(gz == 0, gy_down, gy)
        for dx in (0, -1, 1):
            rows = {0: slice(0, 8), -1: slice(0, 2), 1: slice(6, 8)}[dx]
            for side, there in ((0, left_gy), (1, right_gy)):
                heat.append(remote(packs.at[side, :, rows], strips.at[side, 1 - dx, :, rows], (nexts[dx], there, other)))

        side_gy = jnp.where(gz == 0, gy_down, gy_up)

        def elastic_sends(src, src_layers, dst, pack_src, pack_dst):
            out = [remote(src.at[pl.ds(src_layers(other), 12), 0:16, 0:128], dst.at[:, 0:16, own_lanes], (gx, gy, other))]
            for dz in (gz, other):
                layers = pl.ds(src_layers(dz), 12)
                out.append(remote(src.at[layers, 0:4, 0:128], dst.at[:, 16:20, own_lanes], (nexts[-1], gy, dz)))
                out.append(remote(src.at[layers, 12:16, 0:128], dst.at[:, 20:24, own_lanes], (nexts[1], gy, dz)))
                for dx in (0, -1, 1):
                    out.append(remote(pack_src, pack_dst.at[gz, 1 - dx], (nexts[dx], side_gy, dz)))
            return out

        for copy in heat:
            copy.wait_recv()

        labels = elastic_sends(label, lambda dz: 4 * dz, e_label, packs.at[gz, 0], label_strips)

        def halo_blocks(blocks, inset=0, last=252):
            right = [blocks(0, d) for d in (-1, 0, 1)]
            left = [blocks(1, d) for d in (-1, 0, 1)]

            def corner(three):
                return jnp.where(sub < 4, three[2], pltpu.roll(three[0], 124, 1))

            right_corner, left_corner = corner(right), corner(left)

            def at(layer):
                def one(r, l, slot):
                    r = pltpu.roll(r, lax.rem(256 - inset - slot * 4, 128), 1)
                    l = pltpu.roll(l, lax.rem(last - inset - slot * 4, 128), 1)
                    return jnp.where(lane < 64, r, l)

                return jnp.concatenate([
                    one(right[1], left[1], layer * 2),
                    one(right[1], left[1], layer * 2 + 1),
                    one(right_corner, left_corner, layer * 2),
                ], axis=0)

            return at

        label_halo = halo_blocks(lambda side, d: strips[side, d + 1, 0])
        temp_halo = halo_blocks(lambda side, d: strips[side, d + 1, 1], 0, 254)
        patch_halo = halo_blocks(lambda side, d: strips[side, d + 1, 1], 2, 254)

        row = lax.broadcasted_iota(jnp.int32, (24, 128), 0)
        wide_lane = lax.broadcasted_iota(jnp.int32, (24, 128), 1)
        low_row = jnp.where(gx == nx - 1, 16, 24)
        high_row = jnp.where(gx == 0, 20, 32)
        rows_ok = ((row < 16) | ((row >= 16) & (row < 20) & (row < low_row)) | ((row >= 20) & (row < high_row) & (gx > 0)))
        first_tile, last_tile = (gy == 0) & (gz == 0), (gy == ny - 1) & (gz == 1)
        right_limit = jnp.where(last_tile, 0, 64)
        left_limit = jnp.where(first_tile, 128, 64)
        cols_ok = (wide_lane < right_limit) | (wide_lane >= left_limit)
        grid_ok = [rows_ok, rows_ok & cols_ok]
        e_right_limit = jnp.where(gy == ny - 1, 0, 64)
        e_left_limit = jnp.where(gy == 0, 128, 64)
        e_cols_ok = (wide_lane < e_right_limit) | (wide_lane >= e_left_limit)
        e_ok = [rows_ok, rows_ok, rows_ok & e_cols_ok]

        materials = range(4)
        conductivity = [traits[0, m] for m in materials]
        capacity = [traits[1, m] for m in materials]
        modulus = [traits[2, m] for m in materials]
        expansion = [traits[3, m] for m in materials]
        tiles = [intensity[t] for t in range(16)]

        def heat_fields(layer, carry):
            temp[layer, :, 128:256] = temp_halo(layer)
            ids = [label[layer, :, 0:128], label_halo(layer).astype(jnp.int32)]
            tile_ids = [patch[layer, :, 0:128], patch_halo(layer).astype(jnp.int32)]
            for n in range(2):
                cut = slice(128 * n, 128 * n + 128)
                cond[layer, :, cut] = jnp.where(grid_ok[n], lookup(ids[n], conductivity), 0.0)
                rate[layer, :, cut] = TIME_STEP / lookup(ids[n], capacity)
                power[layer, :, cut] = lookup(tile_ids[n], tiles)
            return carry

        grouped(16, 4, heat_fields, 0)
        cond[16] = jnp.zeros((24, 256), F32)

        def conductances(layer, carry):
            own = cond[layer]
            row_g, col_g = conduct(own, plus(own, 0)), conduct(own, plus(own, 1))
            g_row[layer], g_col[layer] = row_g, col_g
            g_row_back[layer], g_col_back[layer] = minus(row_g, 0), minus(col_g, 1)
            g_up[layer + 1] = conduct(own, cond[layer + 1])
            return carry

        g_up[0] = jnp.zeros((24, 256), F32)
        grouped(16, 4, conductances, 0)

        def heat_step(source, layer):
            own = source[layer]
            above, below = source[jnp.minimum(layer + 1, 15)], source[jnp.maximum(layer - 1, 0)]
            flux = g_row[layer] * (plus(own, 0) - own) + g_row_back[layer] * (minus(own, 0) - own)
            flux = flux + g_col[layer] * (plus(own, 1) - own) + g_col_back[layer] * (minus(own, 1) - own)
            flux = flux + g_up[layer + 1] * (above - own) + g_up[layer] * (below - own)
            return own + rate[layer] * (flux + power[layer])

        def heat_one(layer, carry):
            temp_one[layer] = heat_step(temp, layer)
            return carry

        grouped(16, 4, heat_one, 0)

        start = jnp.where(gz == 0, 0, 124)

        def heat_two(layer, acc):
            warm = heat_step(temp_one, layer)[0:16, 0:128]
            warmed_out[layer] = warm
            value = lookup(label[layer, 0:16, 0:128], expansion) * warm
            strain[layer] = value
            for half in range(2):
                slot = layer * 2 + half
                moved = pltpu.roll(value[8 * half : 8 * half + 8], lax.rem(slot * 4 + 128 - start, 128), 1)
                acc = jnp.where((lane >> 2) == slot, moved, acc)
            return acc

        packed_strain[...] = grouped(16, 4, heat_two, jnp.zeros((8, 128), F32))
        stores = [pltpu.make_async_copy(warmed_out, warmed_hbm, out_sem.at[0])]
        stores[0].start()
        strains = elastic_sends(strain, lambda dz: 4 * dz, e_strain, packed_strain, strain_strips)

        def own_strain(layer, carry):
            e_strain[layer, 0:16, own_lanes] = strain[layer + 4 * gz]
            return carry

        lax.fori_loop(0, 12, own_strain, 0)

        for ref in (base, field, lanes):
            for n in range(ref.shape[0]):
                for m in range(ref.shape[1]):
                    ref[n, m, 0] = jnp.zeros((24, 384), F32)

        largest = jnp.maximum(jnp.maximum(modulus[0], modulus[1]), jnp.maximum(modulus[2], modulus[3]))
        scale = SPAN * largest
        inverse = 0.125 / jnp.full((1, 128), scale, F32)
        scaled = [m * inverse for m in modulus]

        for copy in labels:
            copy.wait_recv()
        for copy in strains:
            copy.wait_recv()

        e_label_halo = halo_blocks(lambda side, d: label_strips[side, d + 1])
        e_strain_halo = halo_blocks(lambda side, d: strain_strips[side, d + 1])

        def stacked(layer):
            return jnp.where(gz == 0, layer, 11 - layer)

        def spread(ref, n, layer, value):
            ahead, behind = plus(value, 1), minus(value, 1)
            ref[n, 0, layer + 1] = value
            ref[n, 1, layer + 1] = ahead + behind
            ref[n, 2, layer + 1] = ahead - behind

        def base_fields(layer, carry):
            raw = stacked(layer)
            ids = [e_label[raw, :, 0:128], e_label[raw, :, 128:256]]
            hot = [e_strain[raw, :, 0:128], e_strain[raw, :, 128:256]]
            whole = raw + 4 * gz
            ids.append(e_label_halo(whole).astype(jnp.int32))
            hot.append(e_strain_halo(whole))
            stiffness = [jnp.where(e_ok[n], lookup(ids[n], scaled), 0.0) for n in range(3)]
            hot = [jnp.where(e_ok[n], hot[n], 0.0) for n in range(3)]
            e = jnp.concatenate(stiffness, axis=1)
            s = jnp.concatenate(hot, axis=1)
            spread(base, 0, layer, e)
            spread(base, 1, layer, s)
            spread(base, 2, layer, e * s)
            beside[0, layer], beside[1, layer] = minus(e, 0), plus(e, 0)
            return carry

        grouped(12, 2, base_fields, 0)

        cuts = [slice(128 * n, 128 * n + 128) for n in range(3)]

        def put(step, layer):
            e = base[0, 0, layer + 1]
            slot = (step % 2) * 5
            for comp in range(3):
                value = field[step, comp, layer + 1]
                ahead, behind = plus(value, 1), minus(value, 1)
                lanes[slot, comp, layer + 1] = ahead + behind
                lanes[slot + 1, comp, layer + 1] = ahead - behind
                value = e * value
                ahead, behind = plus(value, 1), minus(value, 1)
                lanes[slot + 2, comp, layer + 1] = value
                lanes[slot + 3, comp, layer + 1] = ahead + behind
                lanes[slot + 4, comp, layer + 1] = ahead - behind

        def first_vector(layer, carry):
            for cut in cuts:
                def get(n):
                    return lambda kind, dz: base[n, kind, layer + 1 + dz, :, cut]

                e, s = base[0, 0, layer + 1, :, cut], base[1, 0, layer + 1, :, cut]
                for comp in range(3):
                    load = -(e * gradient(get(1), comp) + s * gradient(get(0), comp) + gradient(get(2), comp))
                    field[0, comp, layer + 1, :, cut] = jnp.where(e > 0.0, load, 0.0)
                for n, value in enumerate(scalar_stencils(get(0))):
                    stiff[n, layer, :, cut] = value + (8.0 * DIAGONAL * e - TAU) if n < 3 else value
            put(0, layer)
            return carry

        lax.fori_loop(0, 11, first_vector, 0)

        places = ((0, 3, 4), (3, 1, 5), (4, 5, 2))

        def next_vector(step, layer):
            slot = (step % 2) * 5
            for cut in cuts if step < 2 else cuts[:2]:
                def plain(comp, kind, dz):
                    if kind == 0:
                        return field[step, comp, layer + 1 + dz, :, cut]
                    return lanes[slot + kind - 1, comp, layer + 1 + dz, :, cut]

                def weighted(comp, kind, dz):
                    return lanes[slot + 2 + kind, comp, layer + 1 + dz, :, cut]

                for comp in range(3):
                    c, a, b = stencil(plain, comp)
                    c_w, a_w, b_w = stencil(weighted, comp)
                    e = base[0, 0, layer + 1, :, cut]
                    value = -(e * c + c_w)
                    for n in range(3):
                        value = value + stiff[places[comp][n], layer, :, cut] * field[step, n, layer + 1, :, cut]
                    value = value - plus(beside[0, layer, :, cut] * (a + b) + (a_w + b_w), 0)
                    value = value - minus(beside[1, layer, :, cut] * (a - b) + (a_w - b_w), 0)
                    value = jnp.where(e > 0.0, value, 0.0)
                    if step < 2:
                        field[step + 1, comp, layer + 1, :, cut] = value
                    else:
                        field[step + 1, comp, layer + 1, 0:16, cut] = value[0:16]
            if step < 2:
                put(step + 1, layer)

        for step in range(3):
            def body(layer, carry, step=step):
                next_vector(step, layer)
                return carry

            lax.fori_loop(0, 10 - step, body, 0)

        def products(layer, acc):
            acc = list(acc)
            for comp in range(3):
                for half in range(2):
                    for n in range(2):
                        v = [
                            field[step, comp, layer + 1, 8 * half : 8 * half + 8, 128 * n : 128 * n + 128]
                            for step in range(4)
                        ]
                        for k in range(6):
                            acc[k] = acc[k] + v[k // 2] * v[k - k // 2]
            return tuple(acc)

        acc = lax.fori_loop(0, 8, products, tuple(jnp.zeros((8, 128), F32) for _ in range(6)))
        mine = jnp.zeros((8, 128), F32)
        for k in range(6):
            mine = jnp.where(sub == k, jnp.sum(acc[k], axis=0, keepdims=True), mine)
        mine = jnp.sum(mine, axis=1, keepdims=True)
        sums[...] = jnp.sum(jnp.where(lane == sub, mine, 0.0), axis=0, keepdims=True)

        def reduce_over(ring, src, dst):
            copies = [remote(src, dst.at[n], peer) for n, peer in enumerate(ring)]
            for copy in copies:
                copy.wait_recv()
            value = src[...]
            for n in range(len(ring)):
                value = value + dst[n]
            return copies, value

        first, value = reduce_over(ring_a, sums, sums_a)
        total_a[...] = value
        second, value = reduce_over(ring_b, total_a, sums_b)

        moments = [value[:, k : k + 1] for k in range(6)]
        x_of, r_of = iterate_coefficients(moments)
        x_of = [jnp.broadcast_to(c, (16, 256)) for c in x_of]
        r_of = [jnp.broadcast_to(c * scale, (16, 256)) for c in r_of]
        sign = jnp.where(gz == 0, 1.0, -1.0)

        def outputs(layer, carry):
            place = jnp.where(gz == 0, layer, 7 - layer)
            for comp in range(3):
                v = [field[step, comp, layer + 1, 0:16, 0:256] for step in range(4)]
                x = x_of[0] * v[0] + x_of[1] * v[1] + x_of[2] * v[2]
                r = r_of[0] * v[0] + r_of[1] * v[1] + r_of[2] * v[2] + r_of[3] * v[3]
                solution_out[comp, place] = x * sign if comp == 0 else x
                residual_out[comp, place] = r * sign if comp == 0 else r
            return carry

        lax.fori_loop(0, 8, outputs, 0)
        stores.append(pltpu.make_async_copy(solution_out, solution_hbm, out_sem.at[1]))
        stores.append(pltpu.make_async_copy(residual_out, residual_hbm, out_sem.at[2]))
        for copy in stores[1:]:
            copy.start()
        for copy in stores:
            copy.wait()

        for copy in heat + labels + strains + first + second:
            copy.wait_send()

    return kernel


def copy_out(*refs):
    sources, targets, held, (arrived, left) = refs[:3], refs[3:6], refs[6:9], refs[9:]
    pieces = [(n, n_piece) for n in (1, 2) for n_piece in range(3)] + [(0, slice(0, 16))]
    loads = [pltpu.make_async_copy(sources[n].at[k], held[n].at[k], arrived.at[i]) for i, (n, k) in enumerate(pieces)]
    stores = [pltpu.make_async_copy(held[n].at[k], targets[n].at[k], left.at[i]) for i, (n, k) in enumerate(pieces)]
    for copy in loads:
        copy.start()
    for load, store in zip(loads, stores):
        load.wait()
        store.start()
    for copy in stores:
        copy.wait()


def solution(mesh):
    sizes = dict(mesh.shape)
    hbm = pl.BlockSpec(memory_space=pltpu.HBM)
    smem = pl.BlockSpec(memory_space=pltpu.SMEM)
    copies = 12 + 11 + 11 + (2 * sizes["gx"] - 1) + (sizes["gy"] - 1)

    def per_device(kelvin, label, patch, traits, intensity):
        heat = lambda layers=16, kind=F32: pltpu.VMEM((layers, 24, 256), kind)
        block = lambda *lead: pltpu.VMEM((*lead, 8, 128), F32)
        wide = lambda *lead: pltpu.VMEM((*lead, 24, 384), F32)
        row = lambda *lead: pltpu.VMEM((*lead, 1, 128), F32)
        shapes = (
            jax.ShapeDtypeStruct((16, 16, 128), F32),
            jax.ShapeDtypeStruct((3, 8, 16, 256), F32),
            jax.ShapeDtypeStruct((3, 8, 16, 256), F32),
        )
        results = pl.pallas_call(
            make_kernel(sizes),
            out_shape=shapes,
            in_specs=[hbm, hbm, hbm, smem, smem],
            out_specs=(hbm, hbm, hbm),
            scratch_shapes=[
                *(pltpu.VMEM(shape.shape, F32) for shape in shapes),
                heat(), heat(kind=jnp.int32), heat(kind=jnp.int32),
                heat(17), heat(), heat(), heat(), heat(), heat(), heat(), heat(17), heat(),
                block(2, 2), block(2, 3, 2), block(), block(2, 3), block(2, 3),
                pltpu.VMEM((16, 16, 128), F32),
                pltpu.VMEM((12, 24, 384), jnp.int32), wide(12),
                wide(3, 3, 13), wide(2, 12), wide(4, 3, 13), wide(10, 3, 13), wide(6, 11),
                row(), row(2 * sizes["gx"] - 1), row(sizes["gy"] - 1), row(),
                pltpu.SemaphoreType.DMA((4,)),
                pltpu.SemaphoreType.DMA((3,)),
                pltpu.SemaphoreType.DMA((copies,)),
                pltpu.SemaphoreType.DMA((copies,)),
            ],
            compiler_params=pltpu.CompilerParams(
                collective_id=0, has_side_effects=True, vmem_limit_bytes=60 * 1024 * 1024
            ),
        )(kelvin, label, patch, traits, intensity)
        return pl.pallas_call(
            copy_out,
            out_shape=shapes,
            in_specs=[hbm, hbm, hbm],
            out_specs=(hbm, hbm, hbm),
            scratch_shapes=[
                *(pltpu.VMEM(shape.shape, F32) for shape in shapes),
                pltpu.SemaphoreType.DMA((7,)),
                pltpu.SemaphoreType.DMA((7,)),
            ],
            compiler_params=pltpu.CompilerParams(vmem_limit_bytes=60 * 1024 * 1024),
        )(*results)

    columns = P(None, "gx", ("gy", "gz"))
    return jax.shard_map(
        per_device,
        mesh=mesh,
        in_specs=(columns, columns, columns, P(), P()),
        out_specs=(columns, P(None, "gz", "gx", "gy"), P(None, "gz", "gx", "gy")),
        check_vma=False,
    )
```

```python
import jax
import jax.numpy as jnp
from jax import lax
from jax.experimental import pallas as pl
from jax.experimental.pallas import tpu as pltpu
from jax.sharding import PartitionSpec as P

MESH = pl.DeviceIdType.MESH
F32 = jnp.float32
TIME_STEP = 0.03
TAU = 4.0 / 3.0
SPAN = 6.0
DIAGONAL = 0.5 + 2.5 + 2.5 + 10.0 / 9.0


def plus(value, axis):
    return pltpu.roll(value, value.shape[axis] - 1, axis)


def minus(value, axis):
    return pltpu.roll(value, 1, axis)


def tree(bits, entries):
    while len(entries) > 1:
        mask, bits = bits[0], bits[1:]
        entries = [jnp.where(mask, entries[i + 1], entries[i]) for i in range(0, len(entries), 2)]
    return entries[0]


def lookup(identity, entries):
    bits, width = [], 1
    while width < len(entries):
        bits.append((identity & width) != 0)
        width *= 2
    return tree(bits, entries)


def conduct(own, other):
    return 2.0 * own * other / jnp.maximum(own + other, 0.25)


CORNER, MIXED = 10.0 / 9.0, 4.0 / 9.0
Z, X, Y = 0, 1, 2
KEPT, SUM, DIFF = 0, 1, 2


def even(get, *which):
    return get(*which, 1) + get(*which, -1)


def odd(get, *which):
    return get(*which, 1) - get(*which, -1)


def stencil(get, comp):
    if comp == Z:
        e, p = get(Z, KEPT, 0), get(Z, SUM, 0)
        pe, pp, qq = even(get, Z, KEPT), even(get, Z, SUM), odd(get, Y, DIFF)
        return (
            2.0 * (p + pp) + 6.0 * pe + qq,
            2.0 * (e + pe) + p + CORNER * pp + MIXED * qq,
            odd(get, X, KEPT) + MIXED * odd(get, X, SUM),
        )
    if comp == X:
        shared = 2.0 * (get(X, SUM, 0) + even(get, X, KEPT))
        pp = even(get, X, SUM)
        return (
            shared + pp,
            6.0 * get(X, KEPT, 0) + shared + CORNER * pp,
            get(Y, DIFF, 0) + odd(get, Z, KEPT) + MIXED * (even(get, Y, DIFF) + odd(get, Z, SUM)),
        )
    p, pe, pp, qq = get(Y, SUM, 0), even(get, Y, KEPT), even(get, Y, SUM), odd(get, Z, DIFF)
    return (
        6.0 * p + 2.0 * (pe + pp) + qq,
        2.0 * (get(Y, KEPT, 0) + p) + pe + CORNER * pp + MIXED * qq,
        get(X, DIFF, 0) + MIXED * even(get, X, DIFF),
    )


def scalar_stencils(get):
    e, p, q = get(KEPT, 0), get(SUM, 0), get(DIFF, 0)
    pe, pp, qe, qp = even(get, KEPT), even(get, SUM), odd(get, KEPT), odd(get, SUM)
    pq, qq = even(get, DIFF), odd(get, DIFF)

    def evenly(c, a):
        return c + plus(a, 0) + minus(a, 0)

    def oddly(b):
        return plus(b, 0) - minus(b, 0)

    shared = 2.0 * (p + pe)
    yield evenly(2.0 * (p + pp) + 6.0 * pe, 2.0 * (e + pe) + p + CORNER * pp)
    yield evenly(shared + pp, 6.0 * e + shared + CORNER * pp)
    yield evenly(6.0 * p + 2.0 * (pe + pp), 2.0 * (e + p) + pe + CORNER * pp)
    yield oddly(qe + MIXED * qp)
    yield evenly(qq, MIXED * qq)
    yield oddly(q + MIXED * pq)


def gradient(get, comp):
    if comp == Z:
        qe, qp = odd(get, KEPT), odd(get, SUM)
        a = 2.0 * qe + 4.0 / 3.0 * qp
        return 4.0 * qe + 2.0 * qp + plus(a, 0) + minus(a, 0)
    if comp == X:
        b = 4.0 * get(KEPT, 0) + 2.0 * (get(SUM, 0) + even(get, KEPT)) + 4.0 / 3.0 * even(get, SUM)
        return plus(b, 0) - minus(b, 0)
    q, pq = get(DIFF, 0), even(get, DIFF)
    a = 2.0 * q + 4.0 / 3.0 * pq
    return 4.0 * q + 2.0 * pq + plus(a, 0) + minus(a, 0)


def poly_dot(first, second, moments):
    total = None
    for i, a in enumerate(first):
        for j, b in enumerate(second):
            term = a * b * moments[i + j]
            total = term if total is None else total + term
    return total


def shifted(poly):
    out = [TAU * c for c in poly] + [jnp.zeros_like(poly[0])]
    for k, c in enumerate(poly):
        out[k + 1] = out[k + 1] + c
    return out


def added(first, second):
    if len(first) < len(second):
        first, second = second, first
    return [a + second[i] if i < len(second) else a for i, a in enumerate(first)]


def iterate_coefficients(moments):
    one = jnp.ones_like(moments[0])
    residual, direction, solution = [one], [one], []
    norm = moments[0]
    for number in range(3):
        image = shifted(direction)
        alpha = norm / poly_dot(direction, image, moments)
        solution = added(solution, [alpha * c for c in direction])
        residual = added([-alpha * c for c in image], residual)
        if number < 2:
            following = poly_dot(residual, residual, moments)
            ratio = following / norm
            direction = added(residual, [ratio * c for c in direction])
            norm = following
    return solution, residual


def grouped(total, size, body, init):
    def trip(number, carry):
        for k in range(size):
            carry = body(number * size + k, carry)
        return carry

    return lax.fori_loop(0, total // size, trip, init)


def make_kernel(sizes):
    nx, ny = sizes["gx"], sizes["gy"]
    group_a, group_b = nx * 2, ny

    def kernel(
        kelvin_in, label_in, patch_in, traits, intensity,
        warmed_hbm, solution_hbm, residual_hbm,
        warmed_out, solution_out, residual_out,
        temp, label, patch, cond, rate, power, g_row, g_row_back, g_col, g_col_back, g_up, temp_one,
        packs, strips, packed_strain, strain_strips, label_strips,
        strain, e_label, e_strain, base, beside, field, lanes_even, lanes_odd, stiff,
        sums, sums_a, sums_b, total_a,
        local_sem, out_sem, send, recv,
    ):
        gx, gy, gz = lax.axis_index("gx"), lax.axis_index("gy"), lax.axis_index("gz")
        other = 1 - gz
        nexts = {-1: lax.rem(gx + nx - 1, nx), 0: gx, 1: lax.rem(gx + 1, nx)}
        gy_up, gy_down = lax.rem(gy + 1, ny), lax.rem(gy + ny - 1, ny)
        own_lanes = pl.ds(pl.multiple_of(gz * 128, 128), 128)

        loads = [
            pltpu.make_async_copy(kelvin_in, temp.at[:, 0:16, 0:128], local_sem.at[0]),
            pltpu.make_async_copy(label_in, label.at[:, 0:16, 0:128], local_sem.at[1]),
            pltpu.make_async_copy(patch_in, patch.at[:, 0:16, 0:128], local_sem.at[2]),
            pltpu.make_async_copy(
                label_in.at[pl.ds(4 * gz, 12)], e_label.at[:, 0:16, own_lanes], local_sem.at[3]
            ),
        ]
        for copy in loads:
            copy.start()
        temp[:, 16:24, 0:128] = jnp.zeros((16, 8, 128), F32)
        label[:, 16:24, 0:128] = jnp.zeros((16, 8, 128), jnp.int32)
        patch[:, 16:24, 0:128] = jnp.zeros((16, 8, 128), jnp.int32)
        for side in range(2):
            for d in (0, 2):
                strips[side, d] = jnp.zeros((2, 8, 128), F32)

        barrier = pltpu.get_barrier_semaphore()
        peers = [
            (nexts[dx], dy, dz)
            for dx in (-1, 0, 1)
            for dy in (gy, gy_up, gy_down)
            for dz in (gz, other)
            if not (dx == 0 and dy is gy and dz is gz)
        ]
        number_a = gx * 2 + gz
        ring_a = []
        for step in range(1, group_a):
            there = lax.rem(number_a + step, group_a)
            ring_a.append((there // 2, gy, lax.rem(there, 2)))
        ring_b = [(gx, lax.rem(gy + step, ny), gz) for step in range(1, group_b)]
        everyone = peers + ring_a[2:-2] + ring_b[1:-1] if nx > 2 and ny > 2 else peers + ring_a + ring_b
        for peer in everyone:
            pl.semaphore_signal(barrier, inc=1, device_id=peer, device_id_type=MESH)
        for copy in loads:
            copy.wait()

        lane = lax.broadcasted_iota(jnp.int32, (8, 128), 1)
        sub = lax.broadcasted_iota(jnp.int32, (8, 128), 0)

        def pack_inputs(layer, acc):
            acc = list(acc)
            for half in range(2):
                slot = layer * 2 + half
                rows = slice(8 * half, 8 * half + 8)
                place = lane - slot * 4
                ids = label[layer, rows, 0:128].astype(F32)
                kelvin = temp[layer, rows, 0:128]
                tile_ids = patch[layer, rows, 0:128].astype(F32)
                for side, (four, two) in enumerate(((0, 0), (124, 126))):
                    moved = pltpu.roll(ids, lax.rem(slot * 4 + 128 - four, 128), 1)
                    acc[2 * side] = jnp.where((lane >> 2) == slot, moved, acc[2 * side])
                    moved = pltpu.roll(kelvin, lax.rem(slot * 4 + 128 - two, 128), 1)
                    acc[2 * side + 1] = jnp.where((place >= 0) & (place < 2), moved, acc[2 * side + 1])
                    moved = pltpu.roll(tile_ids, lax.rem(slot * 4 + 130 - two, 128), 1)
                    acc[2 * side + 1] = jnp.where((place >= 2) & (place < 4), moved, acc[2 * side + 1])
            return tuple(acc)

        packed = grouped(16, 8, pack_inputs, tuple(jnp.zeros((8, 128), F32) for _ in range(4)))
        for k in range(4):
            packs[k // 2, k % 2] = packed[k]

        pl.semaphore_wait(barrier, len(everyone))

        count = [0]

        def remote(src, dst, peer):
            n = count[0]
            count[0] += 1
            copy = pltpu.make_async_remote_copy(
                src_ref=src, dst_ref=dst, send_sem=send.at[n], recv_sem=recv.at[n],
                device_id=peer, device_id_type=MESH,
            )
            copy.start()
            return copy

        heat = []
        for ref, deep in ((temp, 2), (label, 2), (patch, 1)):
            up, down = slice(16 - deep, 16), slice(24 - deep, 24)
            heat.append(remote(ref.at[:, 0:deep, 0:128], ref.at[:, 16 : 16 + deep, 0:128], (nexts[-1], gy, gz)))
            heat.append(remote(ref.at[:, up, 0:128], ref.at[:, down, 0:128], (nexts[1], gy, gz)))
        right_gy = jnp.where(gz == 0, gy, gy_up)
        left_gy = jnp.where(gz == 0, gy_down, gy)
        for dx in (0, -1, 1):
            rows = {0: slice(0, 8), -1: slice(0, 2), 1: slice(6, 8)}[dx]
            for side, there in ((0, left_gy), (1, right_gy)):
                heat.append(remote(packs.at[side, :, rows], strips.at[side, 1 - dx, :, rows], (nexts[dx], there, other)))

        side_gy = jnp.where(gz == 0, gy_down, gy_up)

        def elastic_sends(src, src_layers, dst, pack_src, pack_dst):
            out = [remote(src.at[pl.ds(src_layers(other), 12), 0:16, 0:128], dst.at[:, 0:16, own_lanes], (gx, gy, other))]
            for dz in (gz, other):
                layers = pl.ds(src_layers(dz), 12)
                out.append(remote(src.at[layers, 0:4, 0:128], dst.at[:, 16:20, own_lanes], (nexts[-1], gy, dz)))
                out.append(remote(src.at[layers, 12:16, 0:128], dst.at[:, 20:24, own_lanes], (nexts[1], gy, dz)))
                for dx in (0, -1, 1):
                    out.append(remote(pack_src, pack_dst.at[gz, 1 - dx], (nexts[dx], side_gy, dz)))
            return out

        for copy in heat:
            copy.wait_recv()

        labels = elastic_sends(label, lambda dz: 4 * dz, e_label, packs.at[gz, 0], label_strips)

        def halo_blocks(blocks, inset=0, last=252):
            right = [blocks(0, d) for d in (-1, 0, 1)]
            left = [blocks(1, d) for d in (-1, 0, 1)]

            def corner(three):
                return jnp.where(sub < 4, three[2], pltpu.roll(three[0], 124, 1))

            right_corner, left_corner = corner(right), corner(left)

            def at(layer):
                def one(r, l, slot):
                    r = pltpu.roll(r, lax.rem(256 - inset - slot * 4, 128), 1)
                    l = pltpu.roll(l, lax.rem(last - inset - slot * 4, 128), 1)
                    return jnp.where(lane < 64, r, l)

                return jnp.concatenate([
                    one(right[1], left[1], layer * 2),
                    one(right[1], left[1], layer * 2 + 1),
                    one(right_corner, left_corner, layer * 2),
                ], axis=0)

            return at

        label_halo = halo_blocks(lambda side, d: strips[side, d + 1, 0])
        temp_halo = halo_blocks(lambda side, d: strips[side, d + 1, 1], 0, 254)
        patch_halo = halo_blocks(lambda side, d: strips[side, d + 1, 1], 2, 254)

        row = lax.broadcasted_iota(jnp.int32, (24, 128), 0)
        wide_lane = lax.broadcasted_iota(jnp.int32, (24, 128), 1)
        low_row = jnp.where(gx == nx - 1, 16, 24)
        high_row = jnp.where(gx == 0, 20, 32)
        rows_ok = ((row < 16) | ((row >= 16) & (row < 20) & (row < low_row)) | ((row >= 20) & (row < high_row) & (gx > 0)))
        first_tile, last_tile = (gy == 0) & (gz == 0), (gy == ny - 1) & (gz == 1)
        right_limit = jnp.where(last_tile, 0, 64)
        left_limit = jnp.where(first_tile, 128, 64)
        cols_ok = (wide_lane < right_limit) | (wide_lane >= left_limit)
        grid_ok = [rows_ok, rows_ok & cols_ok]
        e_right_limit = jnp.where(gy == ny - 1, 0, 64)
        e_left_limit = jnp.where(gy == 0, 128, 64)
        e_cols_ok = (wide_lane < e_right_limit) | (wide_lane >= e_left_limit)
        e_ok = [rows_ok, rows_ok, rows_ok & e_cols_ok]

        materials = range(4)
        conductivity = [traits[0, m] for m in materials]
        capacity = [traits[1, m] for m in materials]
        modulus = [traits[2, m] for m in materials]
        expansion = [traits[3, m] for m in materials]
        tiles = [intensity[t] for t in range(16)]

        def heat_fields(layer, carry):
            temp[layer, :, 128:256] = temp_halo(layer)
            ids = [label[layer, :, 0:128], label_halo(layer).astype(jnp.int32)]
            tile_ids = [patch[layer, :, 0:128], patch_halo(layer).astype(jnp.int32)]
            for n in range(2):
                cut = slice(128 * n, 128 * n + 128)
                cond[layer, :, cut] = jnp.where(grid_ok[n], lookup(ids[n], conductivity), 0.0)
                rate[layer, :, cut] = TIME_STEP / lookup(ids[n], capacity)
                power[layer, :, cut] = lookup(tile_ids[n], tiles)
            return carry

        grouped(16, 8, heat_fields, 0)
        cond[16] = jnp.zeros((24, 256), F32)

        def conductances(layer, carry):
            own = cond[layer]
            row_g, col_g = conduct(own, plus(own, 0)), conduct(own, plus(own, 1))
            g_row[layer], g_col[layer] = row_g, col_g
            g_row_back[layer], g_col_back[layer] = minus(row_g, 0), minus(col_g, 1)
            g_up[layer + 1] = conduct(own, cond[layer + 1])
            return carry

        g_up[0] = jnp.zeros((24, 256), F32)
        grouped(16, 8, conductances, 0)

        def heat_step(source, layer):
            own = source[layer]
            above, below = source[jnp.minimum(layer + 1, 15)], source[jnp.maximum(layer - 1, 0)]
            flux = g_row[layer] * (plus(own, 0) - own) + g_row_back[layer] * (minus(own, 0) - own)
            flux = flux + g_col[layer] * (plus(own, 1) - own) + g_col_back[layer] * (minus(own, 1) - own)
            flux = flux + g_up[layer + 1] * (above - own) + g_up[layer] * (below - own)
            return own + rate[layer] * (flux + power[layer])

        def heat_one(layer, carry):
            temp_one[layer] = heat_step(temp, layer)
            return carry

        grouped(16, 8, heat_one, 0)

        start = jnp.where(gz == 0, 0, 124)

        def heat_two(layer, acc):
            warm = heat_step(temp_one, layer)[0:16, 0:128]
            warmed_out[layer] = warm
            value = lookup(label[layer, 0:16, 0:128], expansion) * warm
            strain[layer] = value
            for half in range(2):
                slot = layer * 2 + half
                moved = pltpu.roll(value[8 * half : 8 * half + 8], lax.rem(slot * 4 + 128 - start, 128), 1)
                acc = jnp.where((lane >> 2) == slot, moved, acc)
            return acc

        packed_strain[...] = grouped(16, 8, heat_two, jnp.zeros((8, 128), F32))
        stores = [pltpu.make_async_copy(warmed_out, warmed_hbm, out_sem.at[0])]
        stores[0].start()
        strains = elastic_sends(strain, lambda dz: 4 * dz, e_strain, packed_strain, strain_strips)

        def own_strain(layer, carry):
            e_strain[layer, 0:16, own_lanes] = strain[layer + 4 * gz]
            return carry

        lax.fori_loop(0, 12, own_strain, 0)

        lanes = (lanes_even, lanes_odd)
        for n in range(4):
            beside[n, 0] = jnp.zeros((24, 384), F32)
        for ref in (base, field, *lanes):
            for n in range(ref.shape[0]):
                for m in range(ref.shape[1]):
                    ref[n, m, 0] = jnp.zeros((24, 384), F32)

        largest = jnp.maximum(jnp.maximum(modulus[0], modulus[1]), jnp.maximum(modulus[2], modulus[3]))
        scale = SPAN * largest
        inverse = 0.125 / jnp.full((1, 128), scale, F32)
        scaled = [m * inverse for m in modulus]

        for copy in labels:
            copy.wait_recv()
        for copy in strains:
            copy.wait_recv()

        e_label_halo = halo_blocks(lambda side, d: label_strips[side, d + 1])
        e_strain_halo = halo_blocks(lambda side, d: strain_strips[side, d + 1])

        def stacked(layer):
            return jnp.where(gz == 0, layer, 11 - layer)

        def base_fields(layer, carry):
            raw = stacked(layer)
            ids = [e_label[raw, :, 0:128], e_label[raw, :, 128:256]]
            hot = [e_strain[raw, :, 0:128], e_strain[raw, :, 128:256]]
            whole = raw + 4 * gz
            ids.append(e_label_halo(whole).astype(jnp.int32))
            hot.append(e_strain_halo(whole))
            stiffness = [jnp.where(e_ok[n], lookup(ids[n], scaled), 0.0) for n in range(3)]
            hot = [jnp.where(e_ok[n], hot[n], 0.0) for n in range(3)]
            e = jnp.concatenate(stiffness, axis=1)
            s = jnp.concatenate(hot, axis=1)
            base[0, KEPT, layer + 1], base[1, KEPT, layer + 1] = e, s
            return carry

        grouped(12, 4, base_fields, 0)

        cuts = [slice(128 * n, 128 * n + 128) for n in range(3)]

        def put(step, layer, comps=range(3)):
            e = base[0, 0, layer + 1]
            to = lanes[step % 2]
            for comp in comps:
                value = field[step, comp, layer + 1]
                ahead, behind = plus(value, 1), minus(value, 1)
                to[0, comp, layer + 1] = ahead + behind
                to[1, comp, layer + 1] = ahead - behind
                ahead, behind = beside[2, layer + 1] * ahead, beside[3, layer + 1] * behind
                to[2, comp, layer + 1] = e * value
                to[3, comp, layer + 1] = ahead + behind
                to[4, comp, layer + 1] = ahead - behind

        def spread(layer):
            e, s = base[0, KEPT, layer + 1], base[1, KEPT, layer + 1]
            beside[0, layer + 1], beside[1, layer + 1] = minus(e, 0), plus(e, 0)
            e_ahead, e_behind, s_ahead, s_behind = plus(e, 1), minus(e, 1), plus(s, 1), minus(s, 1)
            beside[2, layer + 1], beside[3, layer + 1] = e_ahead, e_behind
            base[2, KEPT, layer + 1] = e * s
            pairs = ((e_ahead, e_behind), (s_ahead, s_behind), (e_ahead * s_ahead, e_behind * s_behind))
            for n, (ahead, behind) in enumerate(pairs):
                base[n, SUM, layer + 1], base[n, DIFF, layer + 1] = ahead + behind, ahead - behind

        def first_vector(layer, carry):
            spread(layer + 2)
            put(0, layer - 1, [2])

            def get(n, cut):
                return lambda kind, dz: base[n, kind, layer + 1 + dz, :, cut]

            for comp in range(3):
                for cut in cuts:
                    e, s = base[0, 0, layer + 1, :, cut], base[1, 0, layer + 1, :, cut]
                    load = e * gradient(get(1, cut), comp) + s * gradient(get(0, cut), comp) + gradient(get(2, cut), comp)
                    field[0, comp, layer + 1, :, cut] = jnp.where(e > 0.0, -load, 0.0)
                if comp < 2:
                    put(0, layer, [comp])
                cut = cuts[comp]
                e = base[0, 0, layer + 1, :, cut]
                for n, value in enumerate(scalar_stencils(get(0, cut))):
                    stiff[n, layer, :, cut] = value + (8.0 * DIAGONAL * e - TAU) if n < 3 else value
            return carry

        base[0, KEPT, 13] = base[1, KEPT, 13] = jnp.zeros((24, 384), F32)
        spread(0)
        spread(1)
        lax.fori_loop(0, 11, first_vector, 0)
        put(0, 10, [2])

        places = ((0, 3, 4), (3, 1, 5), (4, 5, 2))

        def next_vector(step, layer):
            held = lanes[step % 2]
            if step < 2:
                put(step + 1, layer - 1, [2])
            for comp in range(3):
                for cut in cuts if step < 2 else cuts[:2]:
                    def plain(comp, kind, dz):
                        if kind == 0:
                            return field[step, comp, layer + 1 + dz, :, cut]
                        return held[kind - 1, comp, layer + 1 + dz, :, cut]

                    def weighted(comp, kind, dz):
                        return held[2 + kind, comp, layer + 1 + dz, :, cut]

                    c, a, b = stencil(plain, comp)
                    c_w, a_w, b_w = stencil(weighted, comp)
                    e = base[0, 0, layer + 1, :, cut]
                    value = -(e * c + c_w)
                    for n in range(3):
                        value = value + stiff[places[comp][n], layer, :, cut] * field[step, n, layer + 1, :, cut]
                    value = value - plus(beside[0, layer + 1, :, cut] * (a + b) + (a_w + b_w), 0)
                    value = value - minus(beside[1, layer + 1, :, cut] * (a - b) + (a_w - b_w), 0)
                    value = jnp.where(e > 0.0, value, 0.0)
                    if step < 2:
                        field[step + 1, comp, layer + 1, :, cut] = value
                    else:
                        field[step + 1, comp, layer + 1, 0:16, cut] = value[0:16]
                if step < 2 and comp < 2:
                    put(step + 1, layer, [comp])

        for step in range(3):
            def body(layer, carry, step=step):
                next_vector(step, layer)
                return carry

            lax.fori_loop(0, 10 - step, body, 0)
            if step < 2:
                put(step + 1, 9 - step, [2])

        def products(layer, acc):
            acc = list(acc)
            for comp in range(3):
                for half in range(2):
                    for n in range(2):
                        v = [
                            field[step, comp, layer + 1, 8 * half : 8 * half + 8, 128 * n : 128 * n + 128]
                            for step in range(4)
                        ]
                        for k in range(6):
                            acc[k] = acc[k] + v[k // 2] * v[k - k // 2]
            return tuple(acc)

        acc = lax.fori_loop(0, 8, products, tuple(jnp.zeros((8, 128), F32) for _ in range(6)))
        mine = jnp.zeros((8, 128), F32)
        for k in range(6):
            mine = jnp.where(sub == k, jnp.sum(acc[k], axis=0, keepdims=True), mine)
        mine = jnp.sum(mine, axis=1, keepdims=True)
        sums[...] = jnp.sum(jnp.where(lane == sub, mine, 0.0), axis=0, keepdims=True)

        def reduce_over(ring, src, dst):
            copies = [remote(src, dst.at[n], peer) for n, peer in enumerate(ring)]
            for copy in copies:
                copy.wait_recv()
            value = src[...]
            for n in range(len(ring)):
                value = value + dst[n]
            return copies, value

        first, value = reduce_over(ring_a, sums, sums_a)
        total_a[...] = value
        second, value = reduce_over(ring_b, total_a, sums_b)

        moments = [value[:, k : k + 1] for k in range(6)]
        x_of, r_of = iterate_coefficients(moments)
        x_of = [jnp.broadcast_to(c, (16, 256)) for c in x_of]
        r_of = [jnp.broadcast_to(c * scale, (16, 256)) for c in r_of]
        sign = jnp.where(gz == 0, 1.0, -1.0)

        def outputs(layer, carry):
            place = jnp.where(gz == 0, layer, 7 - layer)
            for comp in range(3):
                v = [field[step, comp, layer + 1, 0:16, 0:256] for step in range(4)]
                x = x_of[0] * v[0] + x_of[1] * v[1] + x_of[2] * v[2]
                r = r_of[0] * v[0] + r_of[1] * v[1] + r_of[2] * v[2] + r_of[3] * v[3]
                solution_out[comp, place] = x * sign if comp == 0 else x
                residual_out[comp, place] = r * sign if comp == 0 else r
            return carry

        lax.fori_loop(0, 8, outputs, 0)
        stores.append(pltpu.make_async_copy(solution_out, solution_hbm, out_sem.at[1]))
        stores.append(pltpu.make_async_copy(residual_out, residual_hbm, out_sem.at[2]))
        for copy in stores[1:]:
            copy.start()
        for copy in stores:
            copy.wait()

        for copy in heat + labels + strains + first + second:
            copy.wait_send()

    return kernel


def copy_out(*refs):
    sources, targets, held, (arrived, left) = refs[:3], refs[3:6], refs[6:9], refs[9:]
    pieces = [(n, n_piece) for n in (1, 2) for n_piece in range(3)] + [(0, slice(0, 16))]
    loads = [pltpu.make_async_copy(sources[n].at[k], held[n].at[k], arrived.at[i]) for i, (n, k) in enumerate(pieces)]
    stores = [pltpu.make_async_copy(held[n].at[k], targets[n].at[k], left.at[i]) for i, (n, k) in enumerate(pieces)]
    for copy in loads:
        copy.start()
    for load, store in zip(loads, stores):
        load.wait()
        store.start()
    for copy in stores:
        copy.wait()


def solution(mesh):
    sizes = dict(mesh.shape)
    hbm = pl.BlockSpec(memory_space=pltpu.HBM)
    smem = pl.BlockSpec(memory_space=pltpu.SMEM)
    copies = 12 + 11 + 11 + (2 * sizes["gx"] - 1) + (sizes["gy"] - 1)

    def per_device(kelvin, label, patch, traits, intensity):
        heat = lambda layers=16, kind=F32: pltpu.VMEM((layers, 24, 256), kind)
        block = lambda *lead: pltpu.VMEM((*lead, 8, 128), F32)
        wide = lambda *lead: pltpu.VMEM((*lead, 24, 384), F32)
        row = lambda *lead: pltpu.VMEM((*lead, 1, 128), F32)
        shapes = (
            jax.ShapeDtypeStruct((16, 16, 128), F32),
            jax.ShapeDtypeStruct((3, 8, 16, 256), F32),
            jax.ShapeDtypeStruct((3, 8, 16, 256), F32),
        )
        results = pl.pallas_call(
            make_kernel(sizes),
            out_shape=shapes,
            in_specs=[hbm, hbm, hbm, smem, smem],
            out_specs=(hbm, hbm, hbm),
            scratch_shapes=[
                *(pltpu.VMEM(shape.shape, F32) for shape in shapes),
                heat(), heat(kind=jnp.int32), heat(kind=jnp.int32),
                heat(17), heat(), heat(), heat(), heat(), heat(), heat(), heat(17), heat(),
                block(2, 2), block(2, 3, 2), block(), block(2, 3), block(2, 3),
                pltpu.VMEM((16, 16, 128), F32),
                pltpu.VMEM((12, 24, 384), jnp.int32), wide(12),
                wide(3, 3, 14), wide(4, 14), wide(4, 3, 13), wide(5, 3, 13), wide(5, 3, 13), wide(6, 11),
                row(), row(2 * sizes["gx"] - 1), row(sizes["gy"] - 1), row(),
                pltpu.SemaphoreType.DMA((4,)),
                pltpu.SemaphoreType.DMA((3,)),
                pltpu.SemaphoreType.DMA((copies,)),
                pltpu.SemaphoreType.DMA((copies,)),
            ],
            compiler_params=pltpu.CompilerParams(
                collective_id=0, has_side_effects=True, vmem_limit_bytes=60 * 1024 * 1024
            ),
        )(kelvin, label, patch, traits, intensity)
        return pl.pallas_call(
            copy_out,
            out_shape=shapes,
            in_specs=[hbm, hbm, hbm],
            out_specs=(hbm, hbm, hbm),
            scratch_shapes=[
                *(pltpu.VMEM(shape.shape, F32) for shape in shapes),
                pltpu.SemaphoreType.DMA((7,)),
                pltpu.SemaphoreType.DMA((7,)),
            ],
            compiler_params=pltpu.CompilerParams(vmem_limit_bytes=60 * 1024 * 1024),
        )(*results)

    columns = P(None, "gx", ("gy", "gz"))
    return jax.shard_map(
        per_device,
        mesh=mesh,
        in_specs=(columns, columns, columns, P(), P()),
        out_specs=(columns, P(None, "gz", "gx", "gy"), P(None, "gz", "gx", "gy")),
        check_vma=False,
    )
```

```python
import jax
import jax.numpy as jnp
from jax import lax
from jax.experimental import pallas as pl
from jax.experimental.pallas import tpu as pltpu
from jax.sharding import PartitionSpec as P

MESH = pl.DeviceIdType.MESH
F32 = jnp.float32
TIME_STEP = 0.03
TAU = 4.0 / 3.0
SPAN = 6.0
DIAGONAL = 0.5 + 2.5 + 2.5 + 10.0 / 9.0


def plus(value, axis):
    return pltpu.roll(value, value.shape[axis] - 1, axis)


def minus(value, axis):
    return pltpu.roll(value, 1, axis)


def tree(bits, entries):
    while len(entries) > 1:
        mask, bits = bits[0], bits[1:]
        entries = [jnp.where(mask, entries[i + 1], entries[i]) for i in range(0, len(entries), 2)]
    return entries[0]


def lookup(identity, entries):
    bits, width = [], 1
    while width < len(entries):
        bits.append((identity & width) != 0)
        width *= 2
    return tree(bits, entries)


def conduct(own, other):
    return 2.0 * own * other / jnp.maximum(own + other, 0.25)


CORNER, MIXED = 10.0 / 9.0, 4.0 / 9.0
Z, X, Y = 0, 1, 2
KEPT, SUM, DIFF = 0, 1, 2


def even(get, *which):
    return get(*which, 1) + get(*which, -1)


def odd(get, *which):
    return get(*which, 1) - get(*which, -1)


def stencil(get, comp):
    if comp == Z:
        e, p = get(Z, KEPT, 0), get(Z, SUM, 0)
        pe, pp, qq = even(get, Z, KEPT), even(get, Z, SUM), odd(get, Y, DIFF)
        return (
            2.0 * (p + pp) + 6.0 * pe + qq,
            2.0 * (e + pe) + p + CORNER * pp + MIXED * qq,
            odd(get, X, KEPT) + MIXED * odd(get, X, SUM),
        )
    if comp == X:
        shared = 2.0 * (get(X, SUM, 0) + even(get, X, KEPT))
        pp = even(get, X, SUM)
        return (
            shared + pp,
            6.0 * get(X, KEPT, 0) + shared + CORNER * pp,
            get(Y, DIFF, 0) + odd(get, Z, KEPT) + MIXED * (even(get, Y, DIFF) + odd(get, Z, SUM)),
        )
    p, pe, pp, qq = get(Y, SUM, 0), even(get, Y, KEPT), even(get, Y, SUM), odd(get, Z, DIFF)
    return (
        6.0 * p + 2.0 * (pe + pp) + qq,
        2.0 * (get(Y, KEPT, 0) + p) + pe + CORNER * pp + MIXED * qq,
        get(X, DIFF, 0) + MIXED * even(get, X, DIFF),
    )


def scalar_stencils(get):
    e, p, q = get(KEPT, 0), get(SUM, 0), get(DIFF, 0)
    pe, pp, qe, qp = even(get, KEPT), even(get, SUM), odd(get, KEPT), odd(get, SUM)
    pq, qq = even(get, DIFF), odd(get, DIFF)

    def evenly(c, a):
        return c + plus(a, 0) + minus(a, 0)

    def oddly(b):
        return plus(b, 0) - minus(b, 0)

    shared = 2.0 * (p + pe)
    yield evenly(2.0 * (p + pp) + 6.0 * pe, 2.0 * (e + pe) + p + CORNER * pp)
    yield evenly(shared + pp, 6.0 * e + shared + CORNER * pp)
    yield evenly(6.0 * p + 2.0 * (pe + pp), 2.0 * (e + p) + pe + CORNER * pp)
    yield oddly(qe + MIXED * qp)
    yield evenly(qq, MIXED * qq)
    yield oddly(q + MIXED * pq)


def gradient(get, comp):
    if comp == Z:
        qe, qp = odd(get, KEPT), odd(get, SUM)
        a = 2.0 * qe + 4.0 / 3.0 * qp
        return 4.0 * qe + 2.0 * qp + plus(a, 0) + minus(a, 0)
    if comp == X:
        b = 4.0 * get(KEPT, 0) + 2.0 * (get(SUM, 0) + even(get, KEPT)) + 4.0 / 3.0 * even(get, SUM)
        return plus(b, 0) - minus(b, 0)
    q, pq = get(DIFF, 0), even(get, DIFF)
    a = 2.0 * q + 4.0 / 3.0 * pq
    return 4.0 * q + 2.0 * pq + plus(a, 0) + minus(a, 0)


def poly_dot(first, second, moments):
    total = None
    for i, a in enumerate(first):
        for j, b in enumerate(second):
            term = a * b * moments[i + j]
            total = term if total is None else total + term
    return total


def shifted(poly):
    out = [TAU * c for c in poly] + [jnp.zeros_like(poly[0])]
    for k, c in enumerate(poly):
        out[k + 1] = out[k + 1] + c
    return out


def added(first, second):
    if len(first) < len(second):
        first, second = second, first
    return [a + second[i] if i < len(second) else a for i, a in enumerate(first)]


def iterate_coefficients(moments):
    one = jnp.ones_like(moments[0])
    residual, direction, solution = [one], [one], []
    norm = moments[0]
    for number in range(3):
        image = shifted(direction)
        alpha = norm / poly_dot(direction, image, moments)
        solution = added(solution, [alpha * c for c in direction])
        residual = added([-alpha * c for c in image], residual)
        if number < 2:
            following = poly_dot(residual, residual, moments)
            ratio = following / norm
            direction = added(residual, [ratio * c for c in direction])
            norm = following
    return solution, residual


def grouped(total, size, body, init):
    def trip(number, carry):
        for k in range(size):
            carry = body(number * size + k, carry)
        return carry

    return lax.fori_loop(0, total // size, trip, init)


def make_kernel(sizes):
    nx, ny = sizes["gx"], sizes["gy"]
    group_a, group_b = nx * 2, ny

    def kernel(
        kelvin_in, label_in, patch_in, traits, intensity,
        warmed_hbm, solution_hbm, residual_hbm,
        warmed_out, solution_out, residual_out,
        temp, label, patch, cond, rate, power, g_row, g_row_back, g_col, g_col_back, g_up, temp_one,
        packs, strips, packed_strain, strain_strips, label_strips,
        strain, e_label, e_strain, base, beside, field, lanes_even, lanes_odd, stiff,
        sums, sums_a, sums_b, total_a,
        local_sem, out_sem, send, recv,
    ):
        gx, gy, gz = lax.axis_index("gx"), lax.axis_index("gy"), lax.axis_index("gz")
        other = 1 - gz
        nexts = {-1: lax.rem(gx + nx - 1, nx), 0: gx, 1: lax.rem(gx + 1, nx)}
        gy_up, gy_down = lax.rem(gy + 1, ny), lax.rem(gy + ny - 1, ny)
        own_lanes = pl.ds(pl.multiple_of(gz * 128, 128), 128)

        loads = [
            pltpu.make_async_copy(kelvin_in, temp.at[:, 0:16, 0:128], local_sem.at[0]),
            pltpu.make_async_copy(label_in, label.at[:, 0:16, 0:128], local_sem.at[1]),
            pltpu.make_async_copy(patch_in, patch.at[:, 0:16, 0:128], local_sem.at[2]),
            pltpu.make_async_copy(
                label_in.at[pl.ds(4 * gz, 12)], e_label.at[:, 0:16, own_lanes], local_sem.at[3]
            ),
        ]
        for copy in loads:
            copy.start()
        temp[:, 16:24, 0:128] = jnp.zeros((16, 8, 128), F32)
        label[:, 16:24, 0:128] = jnp.zeros((16, 8, 128), jnp.int32)
        patch[:, 16:24, 0:128] = jnp.zeros((16, 8, 128), jnp.int32)
        for side in range(2):
            for d in (0, 2):
                strips[side, d] = jnp.zeros((2, 8, 128), F32)

        barrier = pltpu.get_barrier_semaphore()
        peers = [
            (nexts[dx], dy, dz)
            for dx in (-1, 0, 1)
            for dy in (gy, gy_up, gy_down)
            for dz in (gz, other)
            if not (dx == 0 and dy is gy and dz is gz)
        ]
        number_a = gx * 2 + gz
        ring_a = []
        for step in range(1, group_a):
            there = lax.rem(number_a + step, group_a)
            ring_a.append((there // 2, gy, lax.rem(there, 2)))
        ring_b = [(gx, lax.rem(gy + step, ny), gz) for step in range(1, group_b)]
        everyone = peers + ring_a[2:-2] + ring_b[1:-1] if nx > 2 and ny > 2 else peers + ring_a + ring_b
        for peer in everyone:
            pl.semaphore_signal(barrier, inc=1, device_id=peer, device_id_type=MESH)

        for copy in loads:
            copy.wait()

        lane = lax.broadcasted_iota(jnp.int32, (8, 128), 1)
        sub = lax.broadcasted_iota(jnp.int32, (8, 128), 0)

        def pack_inputs(layer, acc):
            acc = list(acc)
            for half in range(2):
                slot = layer * 2 + half
                rows = slice(8 * half, 8 * half + 8)
                place = lane - slot * 4
                ids = label[layer, rows, 0:128].astype(F32)
                kelvin = temp[layer, rows, 0:128]
                tile_ids = patch[layer, rows, 0:128].astype(F32)
                for side, (four, two) in enumerate(((0, 0), (124, 126))):
                    moved = pltpu.roll(ids, lax.rem(slot * 4 + 128 - four, 128), 1)
                    acc[2 * side] = jnp.where((lane >> 2) == slot, moved, acc[2 * side])
                    moved = pltpu.roll(kelvin, lax.rem(slot * 4 + 128 - two, 128), 1)
                    acc[2 * side + 1] = jnp.where((place >= 0) & (place < 2), moved, acc[2 * side + 1])
                    moved = pltpu.roll(tile_ids, lax.rem(slot * 4 + 130 - two, 128), 1)
                    acc[2 * side + 1] = jnp.where((place >= 2) & (place < 4), moved, acc[2 * side + 1])
            return tuple(acc)

        packed = grouped(16, 8, pack_inputs, tuple(jnp.zeros((8, 128), F32) for _ in range(4)))
        for k in range(4):
            packs[k // 2, k % 2] = packed[k]

        pl.semaphore_wait(barrier, len(everyone))

        count = [0]

        def remote(src, dst, peer):
            n = count[0]
            count[0] += 1
            copy = pltpu.make_async_remote_copy(
                src_ref=src, dst_ref=dst, send_sem=send.at[n], recv_sem=recv.at[n],
                device_id=peer, device_id_type=MESH,
            )
            copy.start()
            return copy

        heat = []
        for ref, deep in ((temp, 2), (label, 2), (patch, 1)):
            up, down = slice(16 - deep, 16), slice(24 - deep, 24)
            heat.append(remote(ref.at[:, 0:deep, 0:128], ref.at[:, 16 : 16 + deep, 0:128], (nexts[-1], gy, gz)))
            heat.append(remote(ref.at[:, up, 0:128], ref.at[:, down, 0:128], (nexts[1], gy, gz)))
        right_gy = jnp.where(gz == 0, gy, gy_up)
        left_gy = jnp.where(gz == 0, gy_down, gy)
        for dx in (0, -1, 1):
            rows = {0: slice(0, 8), -1: slice(0, 2), 1: slice(6, 8)}[dx]
            for side, there in ((0, left_gy), (1, right_gy)):
                heat.append(remote(packs.at[side, :, rows], strips.at[side, 1 - dx, :, rows], (nexts[dx], there, other)))

        side_gy = jnp.where(gz == 0, gy_down, gy_up)

        def elastic_sends(src, src_layers, dst, pack_src, pack_dst):
            out = [remote(src.at[pl.ds(src_layers(other), 12), 0:16, 0:128], dst.at[:, 0:16, own_lanes], (gx, gy, other))]
            for dz in (gz, other):
                layers = pl.ds(src_layers(dz), 12)
                out.append(remote(src.at[layers, 0:4, 0:128], dst.at[:, 16:20, own_lanes], (nexts[-1], gy, dz)))
                out.append(remote(src.at[layers, 12:16, 0:128], dst.at[:, 20:24, own_lanes], (nexts[1], gy, dz)))
                for dx in (0, -1, 1):
                    out.append(remote(pack_src, pack_dst.at[gz, 1 - dx], (nexts[dx], side_gy, dz)))
            return out

        labels = elastic_sends(label, lambda dz: 4 * dz, e_label, packs.at[gz, 0], label_strips)

        materials = range(4)
        conductivity = [traits[0, m] for m in materials]
        capacity = [traits[1, m] for m in materials]
        modulus = [traits[2, m] for m in materials]
        expansion = [traits[3, m] for m in materials]
        tiles = [intensity[t] for t in range(16)]

        cond[16] = g_up[0] = jnp.zeros((24, 256), F32)
        lanes = (lanes_even, lanes_odd)
        for n in range(4):
            beside[n, 0] = jnp.zeros((24, 384), F32)
        for ref in (base, field, *lanes):
            for n in range(ref.shape[0]):
                for m in range(ref.shape[1]):
                    ref[n, m, 0] = jnp.zeros((24, 384), F32)
        base[0, KEPT, 13] = base[1, KEPT, 13] = jnp.zeros((24, 384), F32)

        def own_fields(layer, carry):
            ids = label[layer, 0:16, 0:128]
            cond[layer, 0:16, 0:128] = lookup(ids, conductivity)
            rate[layer, 0:16, 0:128] = TIME_STEP / lookup(ids, capacity)
            power[layer, 0:16, 0:128] = lookup(patch[layer, 0:16, 0:128], tiles)
            return carry

        grouped(16, 8, own_fields, 0)

        for copy in heat:
            copy.wait_recv()

        def halo_blocks(blocks, inset=0, last=252):
            right = [blocks(0, d) for d in (-1, 0, 1)]
            left = [blocks(1, d) for d in (-1, 0, 1)]

            def corner(three):
                return jnp.where(sub < 4, three[2], pltpu.roll(three[0], 124, 1))

            right_corner, left_corner = corner(right), corner(left)

            def at(layer):
                def one(r, l, slot):
                    r = pltpu.roll(r, lax.rem(256 - inset - slot * 4, 128), 1)
                    l = pltpu.roll(l, lax.rem(last - inset - slot * 4, 128), 1)
                    return jnp.where(lane < 64, r, l)

                return jnp.concatenate([
                    one(right[1], left[1], layer * 2),
                    one(right[1], left[1], layer * 2 + 1),
                    one(right_corner, left_corner, layer * 2),
                ], axis=0)

            return at

        label_halo = halo_blocks(lambda side, d: strips[side, d + 1, 0])
        temp_halo = halo_blocks(lambda side, d: strips[side, d + 1, 1], 0, 254)
        patch_halo = halo_blocks(lambda side, d: strips[side, d + 1, 1], 2, 254)

        row = lax.broadcasted_iota(jnp.int32, (24, 128), 0)
        wide_lane = lax.broadcasted_iota(jnp.int32, (24, 128), 1)
        low_row = jnp.where(gx == nx - 1, 16, 24)
        high_row = jnp.where(gx == 0, 20, 32)
        rows_ok = ((row < 16) | ((row >= 16) & (row < 20) & (row < low_row)) | ((row >= 20) & (row < high_row) & (gx > 0)))
        first_tile, last_tile = (gy == 0) & (gz == 0), (gy == ny - 1) & (gz == 1)
        right_limit = jnp.where(last_tile, 0, 64)
        left_limit = jnp.where(first_tile, 128, 64)
        cols_ok = (wide_lane < right_limit) | (wide_lane >= left_limit)
        grid_ok = [rows_ok[16:24], rows_ok & cols_ok]
        e_right_limit = jnp.where(gy == ny - 1, 0, 64)
        e_left_limit = jnp.where(gy == 0, 128, 64)
        e_cols_ok = (wide_lane < e_right_limit) | (wide_lane >= e_left_limit)
        e_ok = [rows_ok, rows_ok, rows_ok & e_cols_ok]

        def heat_fields(layer, carry):
            temp[layer, :, 128:256] = temp_halo(layer)
            places = ((slice(16, 24), slice(0, 128)), (slice(0, 24), slice(128, 256)))
            ids = [label[layer, 16:24, 0:128], label_halo(layer).astype(jnp.int32)]
            tile_ids = [patch[layer, 16:24, 0:128], patch_halo(layer).astype(jnp.int32)]
            for (rows, columns), own, tile, inside in zip(places, ids, tile_ids, grid_ok):
                cond[layer, rows, columns] = jnp.where(inside, lookup(own, conductivity), 0.0)
                rate[layer, rows, columns] = TIME_STEP / lookup(own, capacity)
                power[layer, rows, columns] = lookup(tile, tiles)
            return carry

        grouped(16, 8, heat_fields, 0)

        def conductances(layer, carry):
            own = cond[layer]
            row_g, col_g = conduct(own, plus(own, 0)), conduct(own, plus(own, 1))
            g_row[layer], g_col[layer] = row_g, col_g
            g_row_back[layer], g_col_back[layer] = minus(row_g, 0), minus(col_g, 1)
            g_up[layer + 1] = conduct(own, cond[layer + 1])
            return carry

        grouped(16, 8, conductances, 0)

        def heat_step(source, layer):
            own = source[layer]
            above, below = source[jnp.minimum(layer + 1, 15)], source[jnp.maximum(layer - 1, 0)]
            flux = g_row[layer] * (plus(own, 0) - own) + g_row_back[layer] * (minus(own, 0) - own)
            flux = flux + g_col[layer] * (plus(own, 1) - own) + g_col_back[layer] * (minus(own, 1) - own)
            flux = flux + g_up[layer + 1] * (above - own) + g_up[layer] * (below - own)
            return own + rate[layer] * (flux + power[layer])

        def heat_one(layer, carry):
            temp_one[layer] = heat_step(temp, layer)
            return carry

        grouped(16, 8, heat_one, 0)

        start = jnp.where(gz == 0, 0, 124)

        def heat_two(layer, acc):
            warm = heat_step(temp_one, layer)[0:16, 0:128]
            warmed_out[layer] = warm
            value = lookup(label[layer, 0:16, 0:128], expansion) * warm
            strain[layer] = value
            for half in range(2):
                slot = layer * 2 + half
                moved = pltpu.roll(value[8 * half : 8 * half + 8], lax.rem(slot * 4 + 128 - start, 128), 1)
                acc = jnp.where((lane >> 2) == slot, moved, acc)
            return acc

        packed_strain[...] = grouped(16, 8, heat_two, jnp.zeros((8, 128), F32))
        stores = [pltpu.make_async_copy(warmed_out, warmed_hbm, out_sem.at[0])]
        stores[0].start()
        strains = elastic_sends(strain, lambda dz: 4 * dz, e_strain, packed_strain, strain_strips)

        def own_strain(layer, carry):
            e_strain[layer, 0:16, own_lanes] = strain[layer + 4 * gz]
            return carry

        lax.fori_loop(0, 12, own_strain, 0)

        largest = jnp.maximum(jnp.maximum(modulus[0], modulus[1]), jnp.maximum(modulus[2], modulus[3]))
        scale = SPAN * largest
        inverse = 0.125 / jnp.full((1, 128), scale, F32)
        scaled = [m * inverse for m in modulus]

        for copy in labels:
            copy.wait_recv()

        e_label_halo = halo_blocks(lambda side, d: label_strips[side, d + 1])

        def stacked(layer):
            return jnp.where(gz == 0, layer, 11 - layer)

        cuts = [slice(128 * n, 128 * n + 128) for n in range(3)]

        def modulus_fields(layer, carry):
            raw = stacked(layer)
            ids = [e_label[raw, :, cuts[0]], e_label[raw, :, cuts[1]], e_label_halo(raw + 4 * gz).astype(jnp.int32)]
            for n, cut in enumerate(cuts):
                base[0, KEPT, layer + 1, :, cut] = jnp.where(e_ok[n], lookup(ids[n], scaled), 0.0)
            return carry

        grouped(12, 4, modulus_fields, 0)

        def spread_modulus(layer):
            e = base[0, KEPT, layer + 1]
            beside[0, layer + 1], beside[1, layer + 1] = minus(e, 0), plus(e, 0)
            ahead, behind = plus(e, 1), minus(e, 1)
            beside[2, layer + 1], beside[3, layer + 1] = ahead, behind
            base[0, SUM, layer + 1], base[0, DIFF, layer + 1] = ahead + behind, ahead - behind

        def get_base(n, layer, cut):
            return lambda kind, dz: base[n, kind, layer + 1 + dz, :, cut]

        def stiffness(layer, carry):
            spread_modulus(layer + 2)
            for cut in cuts:
                e = base[0, KEPT, layer + 1, :, cut]
                for n, value in enumerate(scalar_stencils(get_base(0, layer, cut))):
                    stiff[n, layer, :, cut] = value + (8.0 * DIAGONAL * e - TAU) if n < 3 else value
            return carry

        spread_modulus(0)
        spread_modulus(1)
        lax.fori_loop(0, 10, stiffness, 0)

        for copy in strains:
            copy.wait_recv()

        e_strain_halo = halo_blocks(lambda side, d: strain_strips[side, d + 1])

        def strain_fields(layer, carry):
            raw = stacked(layer)
            hot = [e_strain[raw, :, cuts[0]], e_strain[raw, :, cuts[1]], e_strain_halo(raw + 4 * gz)]
            for n, cut in enumerate(cuts):
                base[1, KEPT, layer + 1, :, cut] = jnp.where(e_ok[n], hot[n], 0.0)
            return carry

        grouped(12, 4, strain_fields, 0)

        def put(step, layer, comps=range(3)):
            e = base[0, 0, layer + 1]
            to = lanes[step % 2]
            for comp in comps:
                value = field[step, comp, layer + 1]
                ahead, behind = plus(value, 1), minus(value, 1)
                to[0, comp, layer + 1] = ahead + behind
                to[1, comp, layer + 1] = ahead - behind
                ahead, behind = beside[2, layer + 1] * ahead, beside[3, layer + 1] * behind
                to[2, comp, layer + 1] = e * value
                to[3, comp, layer + 1] = ahead + behind
                to[4, comp, layer + 1] = ahead - behind

        def spread_strain(layer):
            s = base[1, KEPT, layer + 1]
            ahead, behind = plus(s, 1), minus(s, 1)
            base[2, KEPT, layer + 1] = base[0, KEPT, layer + 1] * s
            base[1, SUM, layer + 1], base[1, DIFF, layer + 1] = ahead + behind, ahead - behind
            ahead, behind = beside[2, layer + 1] * ahead, beside[3, layer + 1] * behind
            base[2, SUM, layer + 1], base[2, DIFF, layer + 1] = ahead + behind, ahead - behind

        def first_vector(layer, carry):
            spread_strain(layer + 2)
            put(0, layer - 1, [2])
            for comp in range(3):
                for cut in cuts:
                    of_e, of_s, of_es = [gradient(get_base(n, layer, cut), comp) for n in range(3)]
                    e, s = base[0, KEPT, layer + 1, :, cut], base[1, KEPT, layer + 1, :, cut]
                    load = e * of_s + s * of_e + of_es
                    field[0, comp, layer + 1, :, cut] = jnp.where(e > 0.0, -load, 0.0)
                if comp < 2:
                    put(0, layer, [comp])
            return carry

        spread_strain(0)
        spread_strain(1)
        lax.fori_loop(0, 11, first_vector, 0)
        put(0, 10, [2])

        places = ((0, 3, 4), (3, 1, 5), (4, 5, 2))

        def next_vector(step, layer):
            held = lanes[step % 2]
            if step < 2:
                put(step + 1, layer - 1, [2])
            for comp in range(3):
                for cut in cuts if step < 2 else cuts[:2]:
                    def plain(comp, kind, dz):
                        if kind == 0:
                            return field[step, comp, layer + 1 + dz, :, cut]
                        return held[kind - 1, comp, layer + 1 + dz, :, cut]

                    def weighted(comp, kind, dz):
                        return held[2 + kind, comp, layer + 1 + dz, :, cut]

                    c, a, b = stencil(plain, comp)
                    c_w, a_w, b_w = stencil(weighted, comp)
                    e = base[0, 0, layer + 1, :, cut]
                    value = -(e * c + c_w)
                    for n in range(3):
                        value = value + stiff[places[comp][n], layer, :, cut] * field[step, n, layer + 1, :, cut]
                    value = value - plus(beside[0, layer + 1, :, cut] * (a + b) + (a_w + b_w), 0)
                    value = value - minus(beside[1, layer + 1, :, cut] * (a - b) + (a_w - b_w), 0)
                    value = jnp.where(e > 0.0, value, 0.0)
                    if step < 2:
                        field[step + 1, comp, layer + 1, :, cut] = value
                    else:
                        field[step + 1, comp, layer + 1, 0:16, cut] = value[0:16]
                if step < 2 and comp < 2:
                    put(step + 1, layer, [comp])

        for step in range(3):
            def body(layer, carry, step=step):
                next_vector(step, layer)
                return carry

            lax.fori_loop(0, 10 - step, body, 0)
            if step < 2:
                put(step + 1, 9 - step, [2])

        def products(layer, acc):
            acc = list(acc)
            for comp in range(3):
                for half in range(2):
                    for n in range(2):
                        v = [
                            field[step, comp, layer + 1, 8 * half : 8 * half + 8, 128 * n : 128 * n + 128]
                            for step in range(4)
                        ]
                        for k in range(6):
                            acc[k] = acc[k] + v[k // 2] * v[k - k // 2]
            return tuple(acc)

        acc = lax.fori_loop(0, 8, products, tuple(jnp.zeros((8, 128), F32) for _ in range(6)))
        mine = jnp.zeros((8, 128), F32)
        for k in range(6):
            mine = jnp.where(sub == k, jnp.sum(acc[k], axis=0, keepdims=True), mine)
        mine = jnp.sum(mine, axis=1, keepdims=True)
        sums[...] = jnp.sum(jnp.where(lane == sub, mine, 0.0), axis=0, keepdims=True)

        def reduce_over(ring, src, dst):
            copies = [remote(src, dst.at[n], peer) for n, peer in enumerate(ring)]
            for copy in copies:
                copy.wait_recv()
            value = src[...]
            for n in range(len(ring)):
                value = value + dst[n]
            return copies, value

        first, value = reduce_over(ring_a, sums, sums_a)
        total_a[...] = value
        second, value = reduce_over(ring_b, total_a, sums_b)

        moments = [value[:, k : k + 1] for k in range(6)]
        x_of, r_of = iterate_coefficients(moments)
        x_of = [jnp.broadcast_to(c, (16, 256)) for c in x_of]
        r_of = [jnp.broadcast_to(c * scale, (16, 256)) for c in r_of]
        sign = jnp.where(gz == 0, 1.0, -1.0)

        def outputs(layer, carry):
            place = jnp.where(gz == 0, layer, 7 - layer)
            for comp in range(3):
                v = [field[step, comp, layer + 1, 0:16, 0:256] for step in range(4)]
                x = x_of[0] * v[0] + x_of[1] * v[1] + x_of[2] * v[2]
                r = r_of[0] * v[0] + r_of[1] * v[1] + r_of[2] * v[2] + r_of[3] * v[3]
                solution_out[comp, place] = x * sign if comp == 0 else x
                residual_out[comp, place] = r * sign if comp == 0 else r
            return carry

        lax.fori_loop(0, 8, outputs, 0)
        stores.append(pltpu.make_async_copy(solution_out, solution_hbm, out_sem.at[1]))
        stores.append(pltpu.make_async_copy(residual_out, residual_hbm, out_sem.at[2]))
        for copy in stores[1:]:
            copy.start()
        for copy in stores:
            copy.wait()

        for copy in heat + labels + strains + first + second:
            copy.wait_send()

    return kernel


def copy_out(*refs):
    sources, targets, held, (arrived, left) = refs[:3], refs[3:6], refs[6:9], refs[9:]
    pieces = [(n, n_piece) for n in (1, 2) for n_piece in range(3)] + [(0, slice(0, 16))]
    loads = [pltpu.make_async_copy(sources[n].at[k], held[n].at[k], arrived.at[i]) for i, (n, k) in enumerate(pieces)]
    stores = [pltpu.make_async_copy(held[n].at[k], targets[n].at[k], left.at[i]) for i, (n, k) in enumerate(pieces)]
    for copy in loads:
        copy.start()
    for load, store in zip(loads, stores):
        load.wait()
        store.start()
    for copy in stores:
        copy.wait()


def solution(mesh):
    sizes = dict(mesh.shape)
    hbm = pl.BlockSpec(memory_space=pltpu.HBM)
    smem = pl.BlockSpec(memory_space=pltpu.SMEM)
    copies = 12 + 11 + 11 + (2 * sizes["gx"] - 1) + (sizes["gy"] - 1)

    def per_device(kelvin, label, patch, traits, intensity):
        heat = lambda layers=16, kind=F32: pltpu.VMEM((layers, 24, 256), kind)
        block = lambda *lead: pltpu.VMEM((*lead, 8, 128), F32)
        wide = lambda *lead: pltpu.VMEM((*lead, 24, 384), F32)
        row = lambda *lead: pltpu.VMEM((*lead, 1, 128), F32)
        shapes = (
            jax.ShapeDtypeStruct((16, 16, 128), F32),
            jax.ShapeDtypeStruct((3, 8, 16, 256), F32),
            jax.ShapeDtypeStruct((3, 8, 16, 256), F32),
        )
        results = pl.pallas_call(
            make_kernel(sizes),
            out_shape=shapes,
            in_specs=[hbm, hbm, hbm, smem, smem],
            out_specs=(hbm, hbm, hbm),
            scratch_shapes=[
                *(pltpu.VMEM(shape.shape, F32) for shape in shapes),
                heat(), heat(kind=jnp.int32), heat(kind=jnp.int32),
                heat(17), heat(), heat(), heat(), heat(), heat(), heat(), heat(17), heat(),
                block(2, 2), block(2, 3, 2), block(), block(2, 3), block(2, 3),
                pltpu.VMEM((16, 16, 128), F32),
                pltpu.VMEM((12, 24, 384), jnp.int32), wide(12),
                wide(3, 3, 14), wide(4, 14), wide(4, 3, 13), wide(5, 3, 13), wide(5, 3, 13), wide(6, 11),
                row(), row(2 * sizes["gx"] - 1), row(sizes["gy"] - 1), row(),
                pltpu.SemaphoreType.DMA((4,)),
                pltpu.SemaphoreType.DMA((3,)),
                pltpu.SemaphoreType.DMA((copies,)),
                pltpu.SemaphoreType.DMA((copies,)),
            ],
            compiler_params=pltpu.CompilerParams(
                collective_id=0, has_side_effects=True, vmem_limit_bytes=60 * 1024 * 1024
            ),
        )(kelvin, label, patch, traits, intensity)
        return pl.pallas_call(
            copy_out,
            out_shape=shapes,
            in_specs=[hbm, hbm, hbm],
            out_specs=(hbm, hbm, hbm),
            scratch_shapes=[
                *(pltpu.VMEM(shape.shape, F32) for shape in shapes),
                pltpu.SemaphoreType.DMA((7,)),
                pltpu.SemaphoreType.DMA((7,)),
            ],
            compiler_params=pltpu.CompilerParams(vmem_limit_bytes=60 * 1024 * 1024),
        )(*results)

    columns = P(None, "gx", ("gy", "gz"))
    return jax.shard_map(
        per_device,
        mesh=mesh,
        in_specs=(columns, columns, columns, P(), P()),
        out_specs=(columns, P(None, "gz", "gx", "gy"), P(None, "gz", "gx", "gy")),
        check_vma=False,
    )
```

```python
import jax
import jax.numpy as jnp
from jax import lax
from jax.experimental import pallas as pl
from jax.experimental.pallas import tpu as pltpu
from jax.sharding import PartitionSpec as P

MESH = pl.DeviceIdType.MESH
F32 = jnp.float32
TIME_STEP = 0.03
TAU = 4.0 / 3.0
SPAN = 6.0
DIAGONAL = 0.5 + 2.5 + 2.5 + 10.0 / 9.0


def plus(value, axis):
    return pltpu.roll(value, value.shape[axis] - 1, axis)


def minus(value, axis):
    return pltpu.roll(value, 1, axis)


def tree(bits, entries):
    while len(entries) > 1:
        mask, bits = bits[0], bits[1:]
        entries = [jnp.where(mask, entries[i + 1], entries[i]) for i in range(0, len(entries), 2)]
    return entries[0]


def lookup(identity, entries):
    bits, width = [], 1
    while width < len(entries):
        bits.append((identity & width) != 0)
        width *= 2
    return tree(bits, entries)


def conduct(own, other):
    return 2.0 * own * other / jnp.maximum(own + other, 0.25)


CORNER, MIXED = 10.0 / 9.0, 4.0 / 9.0
Z, X, Y = 0, 1, 2
KEPT, SUM, DIFF = 0, 1, 2


def even(get, *which):
    return get(*which, 1) + get(*which, -1)


def odd(get, *which):
    return get(*which, 1) - get(*which, -1)


def stencil(get, comp):
    if comp == Z:
        e, p = get(Z, KEPT, 0), get(Z, SUM, 0)
        pe, pp, qq = even(get, Z, KEPT), even(get, Z, SUM), odd(get, Y, DIFF)
        return (
            2.0 * (p + pp) + 6.0 * pe + qq,
            2.0 * (e + pe) + p + CORNER * pp + MIXED * qq,
            odd(get, X, KEPT) + MIXED * odd(get, X, SUM),
        )
    if comp == X:
        shared = 2.0 * (get(X, SUM, 0) + even(get, X, KEPT))
        pp = even(get, X, SUM)
        return (
            shared + pp,
            6.0 * get(X, KEPT, 0) + shared + CORNER * pp,
            get(Y, DIFF, 0) + odd(get, Z, KEPT) + MIXED * (even(get, Y, DIFF) + odd(get, Z, SUM)),
        )
    p, pe, pp, qq = get(Y, SUM, 0), even(get, Y, KEPT), even(get, Y, SUM), odd(get, Z, DIFF)
    return (
        6.0 * p + 2.0 * (pe + pp) + qq,
        2.0 * (get(Y, KEPT, 0) + p) + pe + CORNER * pp + MIXED * qq,
        get(X, DIFF, 0) + MIXED * even(get, X, DIFF),
    )


def scalar_stencils(get):
    e, p, q = get(KEPT, 0), get(SUM, 0), get(DIFF, 0)
    pe, pp, qe, qp = even(get, KEPT), even(get, SUM), odd(get, KEPT), odd(get, SUM)
    pq, qq = even(get, DIFF), odd(get, DIFF)

    def evenly(c, a):
        return c + plus(a, 0) + minus(a, 0)

    def oddly(b):
        return plus(b, 0) - minus(b, 0)

    shared = 2.0 * (p + pe)
    yield evenly(2.0 * (p + pp) + 6.0 * pe, 2.0 * (e + pe) + p + CORNER * pp)
    yield evenly(shared + pp, 6.0 * e + shared + CORNER * pp)
    yield evenly(6.0 * p + 2.0 * (pe + pp), 2.0 * (e + p) + pe + CORNER * pp)
    yield oddly(qe + MIXED * qp)
    yield evenly(qq, MIXED * qq)
    yield oddly(q + MIXED * pq)


def gradient(get, comp):
    if comp == Z:
        qe, qp = odd(get, KEPT), odd(get, SUM)
        a = 2.0 * qe + 4.0 / 3.0 * qp
        return 4.0 * qe + 2.0 * qp + plus(a, 0) + minus(a, 0)
    if comp == X:
        b = 4.0 * get(KEPT, 0) + 2.0 * (get(SUM, 0) + even(get, KEPT)) + 4.0 / 3.0 * even(get, SUM)
        return plus(b, 0) - minus(b, 0)
    q, pq = get(DIFF, 0), even(get, DIFF)
    a = 2.0 * q + 4.0 / 3.0 * pq
    return 4.0 * q + 2.0 * pq + plus(a, 0) + minus(a, 0)


def poly_dot(first, second, moments):
    total = None
    for i, a in enumerate(first):
        for j, b in enumerate(second):
            term = a * b * moments[i + j]
            total = term if total is None else total + term
    return total


def shifted(poly):
    out = [TAU * c for c in poly] + [jnp.zeros_like(poly[0])]
    for k, c in enumerate(poly):
        out[k + 1] = out[k + 1] + c
    return out


def added(first, second):
    if len(first) < len(second):
        first, second = second, first
    return [a + second[i] if i < len(second) else a for i, a in enumerate(first)]


def iterate_coefficients(moments):
    one = jnp.ones_like(moments[0])
    residual, direction, solution = [one], [one], []
    norm = moments[0]
    for number in range(3):
        image = shifted(direction)
        alpha = norm / poly_dot(direction, image, moments)
        solution = added(solution, [alpha * c for c in direction])
        residual = added([-alpha * c for c in image], residual)
        if number < 2:
            following = poly_dot(residual, residual, moments)
            ratio = following / norm
            direction = added(residual, [ratio * c for c in direction])
            norm = following
    return solution, residual


def grouped(total, size, body, init):
    def trip(number, carry):
        for k in range(size):
            carry = body(number * size + k, carry)
        return carry

    return lax.fori_loop(0, total // size, trip, init)


def make_kernel(sizes):
    nx, ny = sizes["gx"], sizes["gy"]
    group_a, group_b = nx * 2, ny

    def kernel(
        kelvin_in, label_in, patch_in, traits, intensity,
        warmed_hbm, solution_hbm, residual_hbm,
        warmed_out, solution_out, residual_out,
        temp, label, patch, cond, rate, power, g_row, g_row_back, g_col, g_col_back, g_up, temp_one,
        packs, strips, packed_strain, strain_strips, label_strips,
        strain, e_label, e_strain, base, beside, field, lanes_even, lanes_odd, stiff,
        sums, sums_a, sums_b, total_a,
        local_sem, out_sem, send, recv,
    ):
        gx, gy, gz = lax.axis_index("gx"), lax.axis_index("gy"), lax.axis_index("gz")
        other = 1 - gz
        nexts = {-1: lax.rem(gx + nx - 1, nx), 0: gx, 1: lax.rem(gx + 1, nx)}
        gy_up, gy_down = lax.rem(gy + 1, ny), lax.rem(gy + ny - 1, ny)
        own_lanes = pl.ds(pl.multiple_of(gz * 128, 128), 128)

        loads = [
            pltpu.make_async_copy(kelvin_in, temp.at[:, 0:16, 0:128], local_sem.at[0]),
            pltpu.make_async_copy(label_in, label.at[:, 0:16, 0:128], local_sem.at[1]),
            pltpu.make_async_copy(patch_in, patch.at[:, 0:16, 0:128], local_sem.at[2]),
            pltpu.make_async_copy(
                label_in.at[pl.ds(4 * gz, 12)], e_label.at[:, 0:16, own_lanes], local_sem.at[3]
            ),
        ]
        for copy in loads:
            copy.start()
        temp[:, 16:24, 0:128] = jnp.zeros((16, 8, 128), F32)
        label[:, 16:24, 0:128] = jnp.zeros((16, 8, 128), jnp.int32)
        patch[:, 16:24, 0:128] = jnp.zeros((16, 8, 128), jnp.int32)
        for side in range(2):
            for d in (0, 2):
                strips[side, d] = jnp.zeros((2, 8, 128), F32)

        barrier = pltpu.get_barrier_semaphore()
        peers = [
            (nexts[dx], dy, dz)
            for dx in (-1, 0, 1)
            for dy in (gy, gy_up, gy_down)
            for dz in (gz, other)
            if not (dx == 0 and dy is gy and dz is gz)
        ]
        number_a = gx * 2 + gz


        def farthest_first(size):
            return sorted(range(1, size), key=lambda step: abs(size // 2 - step))

        ring_a, ring_b = {}, {}
        for step in farthest_first(group_a):
            there = lax.rem(number_a + step, group_a)
            ring_a[step] = (there // 2, gy, lax.rem(there, 2))
        for step in farthest_first(group_b):
            ring_b[step] = (gx, lax.rem(gy + step, ny), gz)
        everyone = peers + [ring_a[step] for step in range(3, group_a - 2)] + [ring_b[step] for step in range(2, group_b - 1)]
        for peer in everyone:
            pl.semaphore_signal(barrier, inc=1, device_id=peer, device_id_type=MESH)

        for copy in loads:
            copy.wait()

        lane = lax.broadcasted_iota(jnp.int32, (8, 128), 1)
        sub = lax.broadcasted_iota(jnp.int32, (8, 128), 0)

        def pack_inputs(layer, acc):
            acc = list(acc)
            for half in range(2):
                slot = layer * 2 + half
                rows = slice(8 * half, 8 * half + 8)
                place = lane - slot * 4
                ids = label[layer, rows, 0:128].astype(F32)
                kelvin = temp[layer, rows, 0:128]
                tile_ids = patch[layer, rows, 0:128].astype(F32)
                for side, (four, two) in enumerate(((0, 0), (124, 126))):
                    moved = pltpu.roll(ids, lax.rem(slot * 4 + 128 - four, 128), 1)
                    acc[2 * side] = jnp.where((lane >> 2) == slot, moved, acc[2 * side])
                    moved = pltpu.roll(kelvin, lax.rem(slot * 4 + 128 - two, 128), 1)
                    acc[2 * side + 1] = jnp.where((place >= 0) & (place < 2), moved, acc[2 * side + 1])
                    moved = pltpu.roll(tile_ids, lax.rem(slot * 4 + 130 - two, 128), 1)
                    acc[2 * side + 1] = jnp.where((place >= 2) & (place < 4), moved, acc[2 * side + 1])
            return tuple(acc)

        packed = grouped(16, 8, pack_inputs, tuple(jnp.zeros((8, 128), F32) for _ in range(4)))
        for k in range(4):
            packs[k // 2, k % 2] = packed[k]

        pl.semaphore_wait(barrier, len(everyone))

        count = [0]

        def remote(src, dst, peer):
            n = count[0]
            count[0] += 1
            copy = pltpu.make_async_remote_copy(
                src_ref=src, dst_ref=dst, send_sem=send.at[n], recv_sem=recv.at[n],
                device_id=peer, device_id_type=MESH,
            )
            copy.start()
            return copy

        heat = []
        right_gy = jnp.where(gz == 0, gy, gy_up)
        left_gy = jnp.where(gz == 0, gy_down, gy)
        for dx in (-1, 1, 0):
            rows = {0: slice(0, 8), -1: slice(0, 2), 1: slice(6, 8)}[dx]
            for side, there in ((0, left_gy), (1, right_gy)):
                heat.append(remote(packs.at[side, :, rows], strips.at[side, 1 - dx, :, rows], (nexts[dx], there, other)))
        for ref, deep in ((temp, 2), (label, 2), (patch, 1)):
            up, down = slice(16 - deep, 16), slice(24 - deep, 24)
            heat.append(remote(ref.at[:, 0:deep, 0:128], ref.at[:, 16 : 16 + deep, 0:128], (nexts[-1], gy, gz)))
            heat.append(remote(ref.at[:, up, 0:128], ref.at[:, down, 0:128], (nexts[1], gy, gz)))

        side_gy = jnp.where(gz == 0, gy_down, gy_up)

        def elastic_sends(src, src_layers, dst, pack_src, pack_dst):
            out = []
            for dx in (1, -1, 0):
                for dz in (other, gz):
                    out.append(remote(pack_src, pack_dst.at[gz, 1 - dx], (nexts[dx], side_gy, dz)))
            for dz in (other, gz):
                layers = pl.ds(src_layers(dz), 12)
                out.append(remote(src.at[layers, 0:4, 0:128], dst.at[:, 16:20, own_lanes], (nexts[-1], gy, dz)))
                out.append(remote(src.at[layers, 12:16, 0:128], dst.at[:, 20:24, own_lanes], (nexts[1], gy, dz)))
            out.append(remote(src.at[pl.ds(src_layers(other), 12), 0:16, 0:128], dst.at[:, 0:16, own_lanes], (gx, gy, other)))
            return out

        labels = elastic_sends(label, lambda dz: 4 * dz, e_label, packs.at[gz, 0], label_strips)

        materials = range(4)
        conductivity = [traits[0, m] for m in materials]
        capacity = [traits[1, m] for m in materials]
        modulus = [traits[2, m] for m in materials]
        expansion = [traits[3, m] for m in materials]
        tiles = [intensity[t] for t in range(16)]

        cond[16] = g_up[0] = jnp.zeros((24, 256), F32)
        lanes = (lanes_even, lanes_odd)
        for n in range(4):
            beside[n, 0] = jnp.zeros((24, 384), F32)
        for ref in (base, field, *lanes):
            for n in range(ref.shape[0]):
                for m in range(ref.shape[1]):
                    ref[n, m, 0] = jnp.zeros((24, 384), F32)
        base[0, KEPT, 13] = base[1, KEPT, 13] = jnp.zeros((24, 384), F32)

        def own_fields(layer, carry):
            ids = label[layer, 0:16, 0:128]
            cond[layer, 0:16, 0:128] = lookup(ids, conductivity)
            rate[layer, 0:16, 0:128] = TIME_STEP / lookup(ids, capacity)
            power[layer, 0:16, 0:128] = lookup(patch[layer, 0:16, 0:128], tiles)
            return carry

        grouped(16, 8, own_fields, 0)

        for copy in heat:
            copy.wait_recv()

        def halo_blocks(blocks, inset=0, last=252):
            right = [blocks(0, d) for d in (-1, 0, 1)]
            left = [blocks(1, d) for d in (-1, 0, 1)]

            def corner(three):
                return jnp.where(sub < 4, three[2], pltpu.roll(three[0], 124, 1))

            right_corner, left_corner = corner(right), corner(left)

            def at(layer):
                def one(r, l, slot):
                    r = pltpu.roll(r, lax.rem(256 - inset - slot * 4, 128), 1)
                    l = pltpu.roll(l, lax.rem(last - inset - slot * 4, 128), 1)
                    return jnp.where(lane < 64, r, l)

                return jnp.concatenate([
                    one(right[1], left[1], layer * 2),
                    one(right[1], left[1], layer * 2 + 1),
                    one(right_corner, left_corner, layer * 2),
                ], axis=0)

            return at

        label_halo = halo_blocks(lambda side, d: strips[side, d + 1, 0])
        temp_halo = halo_blocks(lambda side, d: strips[side, d + 1, 1], 0, 254)
        patch_halo = halo_blocks(lambda side, d: strips[side, d + 1, 1], 2, 254)

        row = lax.broadcasted_iota(jnp.int32, (24, 128), 0)
        wide_lane = lax.broadcasted_iota(jnp.int32, (24, 128), 1)
        low_row = jnp.where(gx == nx - 1, 16, 24)
        high_row = jnp.where(gx == 0, 20, 32)
        rows_ok = ((row < 16) | ((row >= 16) & (row < 20) & (row < low_row)) | ((row >= 20) & (row < high_row) & (gx > 0)))
        first_tile, last_tile = (gy == 0) & (gz == 0), (gy == ny - 1) & (gz == 1)
        right_limit = jnp.where(last_tile, 0, 64)
        left_limit = jnp.where(first_tile, 128, 64)
        cols_ok = (wide_lane < right_limit) | (wide_lane >= left_limit)
        grid_ok = [rows_ok[16:24], rows_ok & cols_ok]
        e_right_limit = jnp.where(gy == ny - 1, 0, 64)
        e_left_limit = jnp.where(gy == 0, 128, 64)
        e_cols_ok = (wide_lane < e_right_limit) | (wide_lane >= e_left_limit)
        e_ok = [rows_ok, rows_ok, rows_ok & e_cols_ok]

        def heat_fields(layer, carry):
            temp[layer, :, 128:256] = temp_halo(layer)
            places = ((slice(16, 24), slice(0, 128)), (slice(0, 24), slice(128, 256)))
            ids = [label[layer, 16:24, 0:128], label_halo(layer).astype(jnp.int32)]
            tile_ids = [patch[layer, 16:24, 0:128], patch_halo(layer).astype(jnp.int32)]
            for (rows, columns), own, tile, inside in zip(places, ids, tile_ids, grid_ok):
                cond[layer, rows, columns] = jnp.where(inside, lookup(own, conductivity), 0.0)
                rate[layer, rows, columns] = TIME_STEP / lookup(own, capacity)
                power[layer, rows, columns] = lookup(tile, tiles)
            return carry

        grouped(16, 8, heat_fields, 0)

        def conductances(layer, carry):
            own = cond[layer]
            row_g, col_g = conduct(own, plus(own, 0)), conduct(own, plus(own, 1))
            g_row[layer], g_col[layer] = row_g, col_g
            g_row_back[layer], g_col_back[layer] = minus(row_g, 0), minus(col_g, 1)
            g_up[layer + 1] = conduct(own, cond[layer + 1])
            return carry

        grouped(16, 8, conductances, 0)

        def heat_step(source, layer):
            own = source[layer]
            above, below = source[jnp.minimum(layer + 1, 15)], source[jnp.maximum(layer - 1, 0)]
            flux = g_row[layer] * (plus(own, 0) - own) + g_row_back[layer] * (minus(own, 0) - own)
            flux = flux + g_col[layer] * (plus(own, 1) - own) + g_col_back[layer] * (minus(own, 1) - own)
            flux = flux + g_up[layer + 1] * (above - own) + g_up[layer] * (below - own)
            return own + rate[layer] * (flux + power[layer])

        def heat_one(layer, carry):
            temp_one[layer] = heat_step(temp, layer)
            return carry

        grouped(16, 8, heat_one, 0)

        start = jnp.where(gz == 0, 0, 124)

        def heat_two(layer, acc):
            warm = heat_step(temp_one, layer)[0:16, 0:128]
            warmed_out[layer] = warm
            value = lookup(label[layer, 0:16, 0:128], expansion) * warm
            strain[layer] = value
            for half in range(2):
                slot = layer * 2 + half
                moved = pltpu.roll(value[8 * half : 8 * half + 8], lax.rem(slot * 4 + 128 - start, 128), 1)
                acc = jnp.where((lane >> 2) == slot, moved, acc)
            return acc

        packed_strain[...] = grouped(16, 8, heat_two, jnp.zeros((8, 128), F32))
        stores = [pltpu.make_async_copy(warmed_out, warmed_hbm, out_sem.at[0])]
        stores[0].start()
        strains = elastic_sends(strain, lambda dz: 4 * dz, e_strain, packed_strain, strain_strips)

        def own_strain(layer, carry):
            e_strain[layer, 0:16, own_lanes] = strain[layer + 4 * gz]
            return carry

        lax.fori_loop(0, 12, own_strain, 0)

        largest = jnp.maximum(jnp.maximum(modulus[0], modulus[1]), jnp.maximum(modulus[2], modulus[3]))
        scale = SPAN * largest
        inverse = 0.125 / jnp.full((1, 128), scale, F32)
        scaled = [m * inverse for m in modulus]

        for copy in labels:
            copy.wait_recv()

        e_label_halo = halo_blocks(lambda side, d: label_strips[side, d + 1])

        def stacked(layer):
            return jnp.where(gz == 0, layer, 11 - layer)

        cuts = [slice(128 * n, 128 * n + 128) for n in range(3)]

        def modulus_fields(layer, carry):
            raw = stacked(layer)
            ids = [e_label[raw, :, cuts[0]], e_label[raw, :, cuts[1]], e_label_halo(raw + 4 * gz).astype(jnp.int32)]
            for n, cut in enumerate(cuts):
                base[0, KEPT, layer + 1, :, cut] = jnp.where(e_ok[n], lookup(ids[n], scaled), 0.0)
            return carry

        grouped(12, 4, modulus_fields, 0)

        def spread_modulus(layer):
            e = base[0, KEPT, layer + 1]
            beside[0, layer + 1], beside[1, layer + 1] = minus(e, 0), plus(e, 0)
            ahead, behind = plus(e, 1), minus(e, 1)
            beside[2, layer + 1], beside[3, layer + 1] = ahead, behind
            base[0, SUM, layer + 1], base[0, DIFF, layer + 1] = ahead + behind, ahead - behind

        def get_base(n, layer, cut):
            return lambda kind, dz: base[n, kind, layer + 1 + dz, :, cut]

        def stiffness(layer, carry):
            spread_modulus(layer + 2)
            for cut in cuts:
                e = base[0, KEPT, layer + 1, :, cut]
                for n, value in enumerate(scalar_stencils(get_base(0, layer, cut))):
                    stiff[n, layer, :, cut] = value + (8.0 * DIAGONAL * e - TAU) if n < 3 else value
            return carry

        spread_modulus(0)
        spread_modulus(1)
        lax.fori_loop(0, 10, stiffness, 0)

        for copy in strains:
            copy.wait_recv()

        e_strain_halo = halo_blocks(lambda side, d: strain_strips[side, d + 1])

        def strain_fields(layer, carry):
            raw = stacked(layer)
            hot = [e_strain[raw, :, cuts[0]], e_strain[raw, :, cuts[1]], e_strain_halo(raw + 4 * gz)]
            for n, cut in enumerate(cuts):
                base[1, KEPT, layer + 1, :, cut] = jnp.where(e_ok[n], hot[n], 0.0)
            return carry

        grouped(12, 4, strain_fields, 0)

        def put(step, layer, comps=range(3)):
            e = base[0, 0, layer + 1]
            to = lanes[step % 2]
            for comp in comps:
                value = field[step, comp, layer + 1]
                ahead, behind = plus(value, 1), minus(value, 1)
                to[0, comp, layer + 1] = ahead + behind
                to[1, comp, layer + 1] = ahead - behind
                ahead, behind = beside[2, layer + 1] * ahead, beside[3, layer + 1] * behind
                to[2, comp, layer + 1] = e * value
                to[3, comp, layer + 1] = ahead + behind
                to[4, comp, layer + 1] = ahead - behind

        def spread_strain(layer):
            s = base[1, KEPT, layer + 1]
            ahead, behind = plus(s, 1), minus(s, 1)
            base[2, KEPT, layer + 1] = base[0, KEPT, layer + 1] * s
            base[1, SUM, layer + 1], base[1, DIFF, layer + 1] = ahead + behind, ahead - behind
            ahead, behind = beside[2, layer + 1] * ahead, beside[3, layer + 1] * behind
            base[2, SUM, layer + 1], base[2, DIFF, layer + 1] = ahead + behind, ahead - behind

        def first_vector(layer, carry):
            spread_strain(layer + 2)
            put(0, layer - 1, [2])
            for comp in range(3):
                for cut in cuts:
                    of_e, of_s, of_es = [gradient(get_base(n, layer, cut), comp) for n in range(3)]
                    e, s = base[0, KEPT, layer + 1, :, cut], base[1, KEPT, layer + 1, :, cut]
                    load = e * of_s + s * of_e + of_es
                    field[0, comp, layer + 1, :, cut] = jnp.where(e > 0.0, -load, 0.0)
                if comp < 2:
                    put(0, layer, [comp])
            return carry

        spread_strain(0)
        spread_strain(1)
        lax.fori_loop(0, 11, first_vector, 0)
        put(0, 10, [2])

        places = ((0, 3, 4), (3, 1, 5), (4, 5, 2))

        def next_vector(step, layer):
            held = lanes[step % 2]
            if step < 2:
                put(step + 1, layer - 1, [2])
            for comp in range(3):
                for cut in cuts if step < 2 else cuts[:2]:
                    def plain(comp, kind, dz):
                        if kind == 0:
                            return field[step, comp, layer + 1 + dz, :, cut]
                        return held[kind - 1, comp, layer + 1 + dz, :, cut]

                    def weighted(comp, kind, dz):
                        return held[2 + kind, comp, layer + 1 + dz, :, cut]

                    c, a, b = stencil(plain, comp)
                    c_w, a_w, b_w = stencil(weighted, comp)
                    e = base[0, 0, layer + 1, :, cut]
                    value = -(e * c + c_w)
                    for n in range(3):
                        value = value + stiff[places[comp][n], layer, :, cut] * field[step, n, layer + 1, :, cut]
                    value = value - plus(beside[0, layer + 1, :, cut] * (a + b) + (a_w + b_w), 0)
                    value = value - minus(beside[1, layer + 1, :, cut] * (a - b) + (a_w - b_w), 0)
                    value = jnp.where(e > 0.0, value, 0.0)
                    if step < 2:
                        field[step + 1, comp, layer + 1, :, cut] = value
                    else:
                        field[step + 1, comp, layer + 1, 0:16, cut] = value[0:16]
                if step < 2 and comp < 2:
                    put(step + 1, layer, [comp])

        for step in range(3):
            def body(layer, carry, step=step):
                next_vector(step, layer)
                return carry

            lax.fori_loop(0, 10 - step, body, 0)
            if step < 2:
                put(step + 1, 9 - step, [2])

        def products(layer, acc):
            acc = list(acc)
            for comp in range(3):
                for half in range(2):
                    for n in range(2):
                        v = [
                            field[step, comp, layer + 1, 8 * half : 8 * half + 8, 128 * n : 128 * n + 128]
                            for step in range(4)
                        ]
                        for k in range(6):
                            acc[k] = acc[k] + v[k // 2] * v[k - k // 2]
            return tuple(acc)

        acc = lax.fori_loop(0, 8, products, tuple(jnp.zeros((8, 128), F32) for _ in range(6)))
        mine = jnp.zeros((8, 128), F32)
        for k in range(6):
            mine = jnp.where(sub == k, jnp.sum(acc[k], axis=0, keepdims=True), mine)
        mine = jnp.sum(mine, axis=1, keepdims=True)
        sums[...] = jnp.sum(jnp.where(lane == sub, mine, 0.0), axis=0, keepdims=True)

        def reduce_over(ring, src, dst):
            copies = [remote(src, dst.at[n], peer) for n, peer in enumerate(ring.values())]
            for copy in copies:
                copy.wait_recv()
            value = src[...]
            for n in range(len(ring)):
                value = value + dst[n]
            return copies, value

        first, value = reduce_over(ring_a, sums, sums_a)
        total_a[...] = value
        second, value = reduce_over(ring_b, total_a, sums_b)

        moments = [value[:, k : k + 1] for k in range(6)]
        x_of, r_of = iterate_coefficients(moments)
        x_of = [jnp.broadcast_to(c, (16, 256)) for c in x_of]
        r_of = [jnp.broadcast_to(c * scale, (16, 256)) for c in r_of]
        sign = jnp.where(gz == 0, 1.0, -1.0)

        for comp in range(3):
            def outputs(layer, carry, comp=comp):
                place = jnp.where(gz == 0, layer, 7 - layer)
                v = [field[step, comp, layer + 1, 0:16, 0:256] for step in range(4)]
                x = x_of[0] * v[0] + x_of[1] * v[1] + x_of[2] * v[2]
                r = r_of[0] * v[0] + r_of[1] * v[1] + r_of[2] * v[2] + r_of[3] * v[3]
                solution_out[comp, place] = x * sign if comp == 0 else x
                residual_out[comp, place] = r * sign if comp == 0 else r
                return carry

            grouped(8, 2, outputs, 0)
            for n, (held, there) in enumerate(((solution_out, solution_hbm), (residual_out, residual_hbm))):
                stores.append(pltpu.make_async_copy(held.at[comp], there.at[comp], out_sem.at[1 + 2 * comp + n]))
                stores[-1].start()
        for copy in stores:
            copy.wait()

        for copy in heat + labels + strains + first + second:
            copy.wait_send()

    return kernel


def copy_out(*refs):
    sources, targets, held, (arrived, left) = refs[:3], refs[3:6], refs[6:9], refs[9:]
    pieces = [(n, n_piece) for n in (1, 2) for n_piece in range(3)] + [(0, slice(0, 16))]
    loads = [pltpu.make_async_copy(sources[n].at[k], held[n].at[k], arrived.at[i]) for i, (n, k) in enumerate(pieces)]
    stores = [pltpu.make_async_copy(held[n].at[k], targets[n].at[k], left.at[i]) for i, (n, k) in enumerate(pieces)]
    for copy in loads:
        copy.start()
    for load, store in zip(loads, stores):
        load.wait()
        store.start()
    for copy in stores:
        copy.wait()


def solution(mesh):
    sizes = dict(mesh.shape)
    hbm = pl.BlockSpec(memory_space=pltpu.HBM)
    smem = pl.BlockSpec(memory_space=pltpu.SMEM)
    copies = 12 + 11 + 11 + (2 * sizes["gx"] - 1) + (sizes["gy"] - 1)

    def per_device(kelvin, label, patch, traits, intensity):
        heat = lambda layers=16, kind=F32: pltpu.VMEM((layers, 24, 256), kind)
        block = lambda *lead: pltpu.VMEM((*lead, 8, 128), F32)
        wide = lambda *lead: pltpu.VMEM((*lead, 24, 384), F32)
        row = lambda *lead: pltpu.VMEM((*lead, 1, 128), F32)
        shapes = (
            jax.ShapeDtypeStruct((16, 16, 128), F32),
            jax.ShapeDtypeStruct((3, 8, 16, 256), F32),
            jax.ShapeDtypeStruct((3, 8, 16, 256), F32),
        )
        results = pl.pallas_call(
            make_kernel(sizes),
            out_shape=shapes,
            in_specs=[hbm, hbm, hbm, smem, smem],
            out_specs=(hbm, hbm, hbm),
            scratch_shapes=[
                *(pltpu.VMEM(shape.shape, F32) for shape in shapes),
                heat(), heat(kind=jnp.int32), heat(kind=jnp.int32),
                heat(17), heat(), heat(), heat(), heat(), heat(), heat(), heat(17), heat(),
                block(2, 2), block(2, 3, 2), block(), block(2, 3), block(2, 3),
                pltpu.VMEM((16, 16, 128), F32),
                pltpu.VMEM((12, 24, 384), jnp.int32), wide(12),
                wide(3, 3, 14), wide(4, 14), wide(4, 3, 13), wide(5, 3, 13), wide(5, 3, 13), wide(6, 11),
                row(), row(2 * sizes["gx"] - 1), row(sizes["gy"] - 1), row(),
                pltpu.SemaphoreType.DMA((4,)),
                pltpu.SemaphoreType.DMA((7,)),
                pltpu.SemaphoreType.DMA((copies,)),
                pltpu.SemaphoreType.DMA((copies,)),
            ],
            compiler_params=pltpu.CompilerParams(
                collective_id=0, has_side_effects=True, vmem_limit_bytes=60 * 1024 * 1024
            ),
        )(kelvin, label, patch, traits, intensity)
        return pl.pallas_call(
            copy_out,
            out_shape=shapes,
            in_specs=[hbm, hbm, hbm],
            out_specs=(hbm, hbm, hbm),
            scratch_shapes=[
                *(pltpu.VMEM(shape.shape, F32) for shape in shapes),
                pltpu.SemaphoreType.DMA((7,)),
                pltpu.SemaphoreType.DMA((7,)),
            ],
            compiler_params=pltpu.CompilerParams(vmem_limit_bytes=60 * 1024 * 1024),
        )(*results)

    columns = P(None, "gx", ("gy", "gz"))
    return jax.shard_map(
        per_device,
        mesh=mesh,
        in_specs=(columns, columns, columns, P(), P()),
        out_specs=(columns, P(None, "gz", "gx", "gy"), P(None, "gz", "gx", "gy")),
        check_vma=False,
    )
```

```python
import jax
import jax.numpy as jnp
from jax import lax
from jax.experimental import pallas as pl
from jax.experimental.pallas import tpu as pltpu
from jax.sharding import PartitionSpec as P

MESH = pl.DeviceIdType.MESH
F32 = jnp.float32
TIME_STEP = 0.03
TAU = 4.0 / 3.0
SPAN = 6.0
DIAGONAL = 0.5 + 2.5 + 2.5 + 10.0 / 9.0


def plus(value, axis):
    return pltpu.roll(value, value.shape[axis] - 1, axis)


def minus(value, axis):
    return pltpu.roll(value, 1, axis)


def tree(bits, entries):
    while len(entries) > 1:
        mask, bits = bits[0], bits[1:]
        entries = [jnp.where(mask, entries[i + 1], entries[i]) for i in range(0, len(entries), 2)]
    return entries[0]


def lookup(identity, entries):
    bits, width = [], 1
    while width < len(entries):
        bits.append((identity & width) != 0)
        width *= 2
    return tree(bits, entries)


def conduct(own, other):
    return 2.0 * own * other / jnp.maximum(own + other, 0.25)


CORNER, MIXED = 10.0 / 9.0, 4.0 / 9.0
Z, X, Y = 0, 1, 2
KEPT, SUM, DIFF = 0, 1, 2


def even(get, *which):
    return get(*which, 1) + get(*which, -1)


def odd(get, *which):
    return get(*which, 1) - get(*which, -1)


def stencil(get, comp):
    if comp == Z:
        e, p = get(Z, KEPT, 0), get(Z, SUM, 0)
        pe, pp, qq = even(get, Z, KEPT), even(get, Z, SUM), odd(get, Y, DIFF)
        return (
            2.0 * (p + pp) + 6.0 * pe + qq,
            2.0 * (e + pe) + p + CORNER * pp + MIXED * qq,
            odd(get, X, KEPT) + MIXED * odd(get, X, SUM),
        )
    if comp == X:
        shared = 2.0 * (get(X, SUM, 0) + even(get, X, KEPT))
        pp = even(get, X, SUM)
        return (
            shared + pp,
            6.0 * get(X, KEPT, 0) + shared + CORNER * pp,
            get(Y, DIFF, 0) + odd(get, Z, KEPT) + MIXED * (even(get, Y, DIFF) + odd(get, Z, SUM)),
        )
    p, pe, pp, qq = get(Y, SUM, 0), even(get, Y, KEPT), even(get, Y, SUM), odd(get, Z, DIFF)
    return (
        6.0 * p + 2.0 * (pe + pp) + qq,
        2.0 * (get(Y, KEPT, 0) + p) + pe + CORNER * pp + MIXED * qq,
        get(X, DIFF, 0) + MIXED * even(get, X, DIFF),
    )


def scalar_stencils(get):
    e, p, q = get(KEPT, 0), get(SUM, 0), get(DIFF, 0)
    pe, pp, qe, qp = even(get, KEPT), even(get, SUM), odd(get, KEPT), odd(get, SUM)
    pq, qq = even(get, DIFF), odd(get, DIFF)

    def evenly(c, a):
        return c + plus(a, 0) + minus(a, 0)

    def oddly(b):
        return plus(b, 0) - minus(b, 0)

    shared = 2.0 * (p + pe)
    yield evenly(2.0 * (p + pp) + 6.0 * pe, 2.0 * (e + pe) + p + CORNER * pp)
    yield evenly(shared + pp, 6.0 * e + shared + CORNER * pp)
    yield evenly(6.0 * p + 2.0 * (pe + pp), 2.0 * (e + p) + pe + CORNER * pp)
    yield oddly(qe + MIXED * qp)
    yield evenly(qq, MIXED * qq)
    yield oddly(q + MIXED * pq)


def gradient(get, comp):
    if comp == Z:
        qe, qp = odd(get, KEPT), odd(get, SUM)
        a = 2.0 * qe + 4.0 / 3.0 * qp
        return 4.0 * qe + 2.0 * qp + plus(a, 0) + minus(a, 0)
    if comp == X:
        b = 4.0 * get(KEPT, 0) + 2.0 * (get(SUM, 0) + even(get, KEPT)) + 4.0 / 3.0 * even(get, SUM)
        return plus(b, 0) - minus(b, 0)
    q, pq = get(DIFF, 0), even(get, DIFF)
    a = 2.0 * q + 4.0 / 3.0 * pq
    return 4.0 * q + 2.0 * pq + plus(a, 0) + minus(a, 0)


def poly_dot(first, second, moments):
    total = None
    for i, a in enumerate(first):
        for j, b in enumerate(second):
            term = a * b * moments[i + j]
            total = term if total is None else total + term
    return total


def shifted(poly):
    out = [TAU * c for c in poly] + [jnp.zeros_like(poly[0])]
    for k, c in enumerate(poly):
        out[k + 1] = out[k + 1] + c
    return out


def added(first, second):
    if len(first) < len(second):
        first, second = second, first
    return [a + second[i] if i < len(second) else a for i, a in enumerate(first)]


def iterate_coefficients(moments):
    one = jnp.ones_like(moments[0])
    residual, direction, solution = [one], [one], []
    norm = moments[0]
    for number in range(3):
        image = shifted(direction)
        alpha = norm / poly_dot(direction, image, moments)
        solution = added(solution, [alpha * c for c in direction])
        residual = added([-alpha * c for c in image], residual)
        if number < 2:
            following = poly_dot(residual, residual, moments)
            ratio = following / norm
            direction = added(residual, [ratio * c for c in direction])
            norm = following
    return solution, residual


def grouped(total, size, body, init):
    def trip(number, carry):
        for k in range(size):
            carry = body(number * size + k, carry)
        return carry

    return lax.fori_loop(0, total // size, trip, init)


def make_kernel(sizes):
    nx, ny = sizes["gx"], sizes["gy"]
    group_a, group_b = nx * 2, ny

    def kernel(
        kelvin_in, label_in, patch_in, traits_in, intensity_in,
        warmed_hbm, solution_hbm, residual_hbm,
        traits, intensity, warmed_out, solution_out, residual_out,
        temp, label, patch, cond, rate, power, g_row, g_row_back, g_col, g_col_back, g_up, temp_one,
        packs, strips, packed_strain, strain_strips, label_strips,
        strain, e_label, e_strain, base, beside, field, lanes_even, lanes_odd, stiff,
        sums, sums_a, sums_b, total_a,
        local_sem, out_sem, send, recv,
    ):
        gx, gy, gz = lax.axis_index("gx"), lax.axis_index("gy"), lax.axis_index("gz")
        other = 1 - gz
        nexts = {-1: lax.rem(gx + nx - 1, nx), 0: gx, 1: lax.rem(gx + 1, nx)}
        gy_up, gy_down = lax.rem(gy + 1, ny), lax.rem(gy + ny - 1, ny)
        own_lanes = pl.ds(pl.multiple_of(gz * 128, 128), 128)

        loads = [
            pltpu.make_async_copy(kelvin_in, temp.at[:, 0:16, 0:128], local_sem.at[0]),
            pltpu.make_async_copy(label_in, label.at[:, 0:16, 0:128], local_sem.at[1]),
            pltpu.make_async_copy(patch_in, patch.at[:, 0:16, 0:128], local_sem.at[2]),
            pltpu.make_async_copy(
                label_in.at[pl.ds(4 * gz, 12)], e_label.at[:, 0:16, own_lanes], local_sem.at[3]
            ),
            pltpu.make_async_copy(traits_in, traits, local_sem.at[4]),
            pltpu.make_async_copy(intensity_in, intensity, local_sem.at[5]),
        ]
        for copy in loads:
            copy.start()
        temp[:, 16:24, 0:128] = jnp.zeros((16, 8, 128), F32)
        label[:, 16:24, 0:128] = jnp.zeros((16, 8, 128), jnp.int32)
        patch[:, 16:24, 0:128] = jnp.zeros((16, 8, 128), jnp.int32)
        for side in range(2):
            for d in (0, 2):
                strips[side, d] = jnp.zeros((2, 8, 128), F32)

        barrier = pltpu.get_barrier_semaphore()
        peers = [
            (nexts[dx], dy, dz)
            for dx in (-1, 0, 1)
            for dy in (gy, gy_up, gy_down)
            for dz in (gz, other)
            if not (dx == 0 and dy is gy and dz is gz)
        ]
        number_a = gx * 2 + gz


        def farthest_first(size):
            return sorted(range(1, size), key=lambda step: abs(size // 2 - step))

        ring_a, ring_b = {}, {}
        for step in farthest_first(group_a):
            there = lax.rem(number_a + step, group_a)
            ring_a[step] = (there // 2, gy, lax.rem(there, 2))
        for step in farthest_first(group_b):
            ring_b[step] = (gx, lax.rem(gy + step, ny), gz)
        everyone = peers + [ring_a[step] for step in range(3, group_a - 2)] + [ring_b[step] for step in range(2, group_b - 1)]
        for peer in everyone:
            pl.semaphore_signal(barrier, inc=1, device_id=peer, device_id_type=MESH)

        for copy in loads:
            copy.wait()

        lane = lax.broadcasted_iota(jnp.int32, (8, 128), 1)
        sub = lax.broadcasted_iota(jnp.int32, (8, 128), 0)

        def pack_inputs(layer, acc):
            acc = list(acc)
            for half in range(2):
                slot = layer * 2 + half
                rows = slice(8 * half, 8 * half + 8)
                place = lane - slot * 4
                ids = label[layer, rows, 0:128].astype(F32)
                kelvin = temp[layer, rows, 0:128]
                tile_ids = patch[layer, rows, 0:128].astype(F32)
                for side, (four, two) in enumerate(((0, 0), (124, 126))):
                    moved = pltpu.roll(ids, lax.rem(slot * 4 + 128 - four, 128), 1)
                    acc[2 * side] = jnp.where((lane >> 2) == slot, moved, acc[2 * side])
                    moved = pltpu.roll(kelvin, lax.rem(slot * 4 + 128 - two, 128), 1)
                    acc[2 * side + 1] = jnp.where((place >= 0) & (place < 2), moved, acc[2 * side + 1])
                    moved = pltpu.roll(tile_ids, lax.rem(slot * 4 + 130 - two, 128), 1)
                    acc[2 * side + 1] = jnp.where((place >= 2) & (place < 4), moved, acc[2 * side + 1])
            return tuple(acc)

        packed = grouped(16, 8, pack_inputs, tuple(jnp.zeros((8, 128), F32) for _ in range(4)))
        for k in range(4):
            packs[k // 2, k % 2] = packed[k]

        pl.semaphore_wait(barrier, len(everyone))

        count = [0]

        def remote(src, dst, peer):
            n = count[0]
            count[0] += 1
            copy = pltpu.make_async_remote_copy(
                src_ref=src, dst_ref=dst, send_sem=send.at[n], recv_sem=recv.at[n],
                device_id=peer, device_id_type=MESH,
            )
            copy.start()
            return copy

        heat = []
        right_gy = jnp.where(gz == 0, gy, gy_up)
        left_gy = jnp.where(gz == 0, gy_down, gy)
        for dx in (-1, 1, 0):
            rows = {0: slice(0, 8), -1: slice(0, 2), 1: slice(6, 8)}[dx]
            for side, there in ((0, left_gy), (1, right_gy)):
                heat.append(remote(packs.at[side, :, rows], strips.at[side, 1 - dx, :, rows], (nexts[dx], there, other)))
        for ref, deep in ((temp, 2), (label, 2), (patch, 1)):
            up, down = slice(16 - deep, 16), slice(24 - deep, 24)
            heat.append(remote(ref.at[:, 0:deep, 0:128], ref.at[:, 16 : 16 + deep, 0:128], (nexts[-1], gy, gz)))
            heat.append(remote(ref.at[:, up, 0:128], ref.at[:, down, 0:128], (nexts[1], gy, gz)))

        side_gy = jnp.where(gz == 0, gy_down, gy_up)

        def elastic_sends(src, src_layers, dst, pack_src, pack_dst):
            out = []
            for dx in (1, -1, 0):
                for dz in (other, gz):
                    out.append(remote(pack_src, pack_dst.at[gz, 1 - dx], (nexts[dx], side_gy, dz)))
            for dz in (other, gz):
                layers = pl.ds(src_layers(dz), 12)
                out.append(remote(src.at[layers, 0:4, 0:128], dst.at[:, 16:20, own_lanes], (nexts[-1], gy, dz)))
                out.append(remote(src.at[layers, 12:16, 0:128], dst.at[:, 20:24, own_lanes], (nexts[1], gy, dz)))
            out.append(remote(src.at[pl.ds(src_layers(other), 12), 0:16, 0:128], dst.at[:, 0:16, own_lanes], (gx, gy, other)))
            return out

        labels = elastic_sends(label, lambda dz: 4 * dz, e_label, packs.at[gz, 0], label_strips)

        materials = range(4)
        conductivity = [traits[0, m] for m in materials]
        capacity = [traits[1, m] for m in materials]
        modulus = [traits[2, m] for m in materials]
        expansion = [-traits[3, m] for m in materials]
        tiles = [intensity[t] for t in range(16)]

        cond[16] = g_up[0] = jnp.zeros((24, 256), F32)
        lanes = (lanes_even, lanes_odd)
        for n in range(4):
            beside[n, 0] = jnp.zeros((24, 384), F32)
        for ref in (base, field, *lanes):
            for n in range(ref.shape[0]):
                for m in range(ref.shape[1]):
                    ref[n, m, 0] = jnp.zeros((24, 384), F32)
        base[0, KEPT, 13] = base[1, KEPT, 13] = jnp.zeros((24, 384), F32)

        def own_fields(layer, carry):
            ids = label[layer, 0:16, 0:128]
            cond[layer, 0:16, 0:128] = lookup(ids, conductivity)
            rate[layer, 0:16, 0:128] = TIME_STEP / lookup(ids, capacity)
            power[layer, 0:16, 0:128] = lookup(patch[layer, 0:16, 0:128], tiles)
            return carry

        grouped(16, 8, own_fields, 0)

        for copy in heat:
            copy.wait_recv()

        def halo_blocks(blocks, inset=0, last=252):
            right = [blocks(0, d) for d in (-1, 0, 1)]
            left = [blocks(1, d) for d in (-1, 0, 1)]

            def corner(three):
                return jnp.where(sub < 4, three[2], pltpu.roll(three[0], 124, 1))

            right_corner, left_corner = corner(right), corner(left)

            def at(layer):
                def one(r, l, slot):
                    r = pltpu.roll(r, lax.rem(256 - inset - slot * 4, 128), 1)
                    l = pltpu.roll(l, lax.rem(last - inset - slot * 4, 128), 1)
                    return jnp.where(lane < 64, r, l)

                return jnp.concatenate([
                    one(right[1], left[1], layer * 2),
                    one(right[1], left[1], layer * 2 + 1),
                    one(right_corner, left_corner, layer * 2),
                ], axis=0)

            return at

        label_halo = halo_blocks(lambda side, d: strips[side, d + 1, 0])
        temp_halo = halo_blocks(lambda side, d: strips[side, d + 1, 1], 0, 254)
        patch_halo = halo_blocks(lambda side, d: strips[side, d + 1, 1], 2, 254)

        row = lax.broadcasted_iota(jnp.int32, (24, 128), 0)
        wide_lane = lax.broadcasted_iota(jnp.int32, (24, 128), 1)
        low_row = jnp.where(gx == nx - 1, 16, 24)
        high_row = jnp.where(gx == 0, 20, 32)
        rows_ok = ((row < 16) | ((row >= 16) & (row < 20) & (row < low_row)) | ((row >= 20) & (row < high_row) & (gx > 0)))
        first_tile, last_tile = (gy == 0) & (gz == 0), (gy == ny - 1) & (gz == 1)
        right_limit = jnp.where(last_tile, 0, 64)
        left_limit = jnp.where(first_tile, 128, 64)
        cols_ok = (wide_lane < right_limit) | (wide_lane >= left_limit)
        grid_ok = [rows_ok[16:24], rows_ok & cols_ok]
        e_right_limit = jnp.where(gy == ny - 1, 0, 64)
        e_left_limit = jnp.where(gy == 0, 128, 64)
        e_cols_ok = (wide_lane < e_right_limit) | (wide_lane >= e_left_limit)
        e_ok = [rows_ok, rows_ok, rows_ok & e_cols_ok]

        def heat_fields(layer, carry):
            temp[layer, :, 128:256] = temp_halo(layer)
            places = ((slice(16, 24), slice(0, 128)), (slice(0, 24), slice(128, 256)))
            ids = [label[layer, 16:24, 0:128], label_halo(layer).astype(jnp.int32)]
            tile_ids = [patch[layer, 16:24, 0:128], patch_halo(layer).astype(jnp.int32)]
            for (rows, columns), own, tile, inside in zip(places, ids, tile_ids, grid_ok):
                cond[layer, rows, columns] = jnp.where(inside, lookup(own, conductivity), 0.0)
                rate[layer, rows, columns] = TIME_STEP / lookup(own, capacity)
                power[layer, rows, columns] = lookup(tile, tiles)
            return carry

        grouped(16, 8, heat_fields, 0)

        def conductances(layer, carry):
            own = cond[layer]
            row_g, col_g = conduct(own, plus(own, 0)), conduct(own, plus(own, 1))
            g_row[layer], g_col[layer] = row_g, col_g
            g_row_back[layer], g_col_back[layer] = minus(row_g, 0), minus(col_g, 1)
            g_up[layer + 1] = conduct(own, cond[layer + 1])
            return carry

        grouped(16, 8, conductances, 0)

        def heat_step(source, layer):
            own = source[layer]
            above, below = source[jnp.minimum(layer + 1, 15)], source[jnp.maximum(layer - 1, 0)]
            flux = g_row[layer] * (plus(own, 0) - own) + g_row_back[layer] * (minus(own, 0) - own)
            flux = flux + g_col[layer] * (plus(own, 1) - own) + g_col_back[layer] * (minus(own, 1) - own)
            flux = flux + g_up[layer + 1] * (above - own) + g_up[layer] * (below - own)
            return own + rate[layer] * (flux + power[layer])

        def heat_one(layer, carry):
            temp_one[layer] = heat_step(temp, layer)
            return carry

        grouped(16, 8, heat_one, 0)

        start = jnp.where(gz == 0, 0, 124)

        def heat_two(layer, acc):
            warm = heat_step(temp_one, layer)[0:16, 0:128]
            warmed_out[layer] = warm
            value = lookup(label[layer, 0:16, 0:128], expansion) * warm
            strain[layer] = value
            for half in range(2):
                slot = layer * 2 + half
                moved = pltpu.roll(value[8 * half : 8 * half + 8], lax.rem(slot * 4 + 128 - start, 128), 1)
                acc = jnp.where((lane >> 2) == slot, moved, acc)
            return acc

        packed_strain[...] = grouped(16, 8, heat_two, jnp.zeros((8, 128), F32))
        stores = [pltpu.make_async_copy(warmed_out, warmed_hbm, out_sem.at[0])]
        stores[0].start()
        strains = elastic_sends(strain, lambda dz: 4 * dz, e_strain, packed_strain, strain_strips)

        def own_strain(layer, carry):
            e_strain[layer, 0:16, own_lanes] = strain[layer + 4 * gz]
            return carry

        lax.fori_loop(0, 12, own_strain, 0)

        largest = jnp.maximum(jnp.maximum(modulus[0], modulus[1]), jnp.maximum(modulus[2], modulus[3]))
        scale = SPAN * largest
        inverse = 0.125 / jnp.full((1, 128), scale, F32)
        scaled = [m * inverse for m in modulus]

        for copy in labels:
            copy.wait_recv()

        e_label_halo = halo_blocks(lambda side, d: label_strips[side, d + 1])

        def stacked(layer):
            return jnp.where(gz == 0, layer, 11 - layer)

        cuts = [slice(128 * n, 128 * n + 128) for n in range(3)]

        def modulus_fields(layer, carry):
            raw = stacked(layer)
            ids = [e_label[raw, :, cuts[0]], e_label[raw, :, cuts[1]], e_label_halo(raw + 4 * gz).astype(jnp.int32)]
            for n, cut in enumerate(cuts):
                base[0, KEPT, layer + 1, :, cut] = jnp.where(e_ok[n], lookup(ids[n], scaled), 0.0)
            return carry

        grouped(12, 4, modulus_fields, 0)

        def spread_modulus(layer):
            e = base[0, KEPT, layer + 1]
            beside[0, layer + 1], beside[1, layer + 1] = minus(e, 0), plus(e, 0)
            ahead, behind = plus(e, 1), minus(e, 1)
            beside[2, layer + 1], beside[3, layer + 1] = ahead, behind
            base[0, SUM, layer + 1], base[0, DIFF, layer + 1] = ahead + behind, ahead - behind

        def get_base(n, layer, cut):
            return lambda kind, dz: base[n, kind, layer + 1 + dz, :, cut]

        def stiffness(layer, carry):
            spread_modulus(layer + 2)
            for cut in cuts:
                e = base[0, KEPT, layer + 1, :, cut]
                for n, value in enumerate(scalar_stencils(get_base(0, layer, cut))):
                    stiff[n, layer, :, cut] = value + (8.0 * DIAGONAL * e - TAU) if n < 3 else value
            return carry

        spread_modulus(0)
        spread_modulus(1)
        lax.fori_loop(0, 10, stiffness, 0)

        for copy in strains:
            copy.wait_recv()

        e_strain_halo = halo_blocks(lambda side, d: strain_strips[side, d + 1])

        def strain_fields(layer, carry):
            raw = stacked(layer)
            hot = [e_strain[raw, :, cuts[0]], e_strain[raw, :, cuts[1]], e_strain_halo(raw + 4 * gz)]
            for n, cut in enumerate(cuts):
                base[1, KEPT, layer + 1, :, cut] = jnp.where(e_ok[n], hot[n], 0.0)
            return carry

        grouped(12, 4, strain_fields, 0)

        def put(step, layer, comps=range(3)):
            e = base[0, 0, layer + 1]
            to = lanes[step % 2]
            for comp in comps:
                value = field[step, comp, layer + 1]
                ahead, behind = plus(value, 1), minus(value, 1)
                to[0, comp, layer + 1] = ahead + behind
                to[1, comp, layer + 1] = ahead - behind
                ahead, behind = beside[2, layer + 1] * ahead, beside[3, layer + 1] * behind
                to[2, comp, layer + 1] = e * value
                to[3, comp, layer + 1] = ahead + behind
                to[4, comp, layer + 1] = ahead - behind

        def spread_strain(layer):
            s = base[1, KEPT, layer + 1]
            ahead, behind = plus(s, 1), minus(s, 1)
            base[2, KEPT, layer + 1] = base[0, KEPT, layer + 1] * s
            base[1, SUM, layer + 1], base[1, DIFF, layer + 1] = ahead + behind, ahead - behind
            ahead, behind = beside[2, layer + 1] * ahead, beside[3, layer + 1] * behind
            base[2, SUM, layer + 1], base[2, DIFF, layer + 1] = ahead + behind, ahead - behind

        def first_vector(layer, carry):
            spread_strain(layer + 2)
            put(0, layer - 1, [2])
            for comp in range(3):
                for cut in cuts:
                    of_e, of_s, of_es = [gradient(get_base(n, layer, cut), comp) for n in range(3)]
                    e, s = base[0, KEPT, layer + 1, :, cut], base[1, KEPT, layer + 1, :, cut]
                    load = e * of_s + s * of_e + of_es
                    field[0, comp, layer + 1, :, cut] = jnp.where(e > 0.0, load, 0.0)
                if comp < 2:
                    put(0, layer, [comp])
            return carry

        spread_strain(0)
        spread_strain(1)
        lax.fori_loop(0, 11, first_vector, 0)
        put(0, 10, [2])

        places = ((0, 3, 4), (3, 1, 5), (4, 5, 2))

        def next_vector(step, layer):
            held = lanes[step % 2]
            if step < 2:
                put(step + 1, layer - 1, [2])
            for comp in range(3):
                for cut in cuts if step < 2 else cuts[:2]:
                    def plain(comp, kind, dz):
                        if kind == 0:
                            return field[step, comp, layer + 1 + dz, :, cut]
                        return held[kind - 1, comp, layer + 1 + dz, :, cut]

                    def weighted(comp, kind, dz):
                        return held[2 + kind, comp, layer + 1 + dz, :, cut]

                    c, a, b = stencil(plain, comp)
                    c_w, a_w, b_w = stencil(weighted, comp)
                    e = base[0, 0, layer + 1, :, cut]
                    terms = [stiff[places[comp][n], layer, :, cut] * field[step, n, layer + 1, :, cut] for n in range(3)]
                    value = terms[0] + terms[1] + terms[2] - (e * c + c_w)
                    value = value - plus(beside[0, layer + 1, :, cut] * (a + b) + (a_w + b_w), 0)
                    value = value - minus(beside[1, layer + 1, :, cut] * (a - b) + (a_w - b_w), 0)
                    value = jnp.where(e > 0.0, value, 0.0)
                    if step < 2:
                        field[step + 1, comp, layer + 1, :, cut] = value
                    else:
                        field[step + 1, comp, layer + 1, 0:16, cut] = value[0:16]
                if step < 2 and comp < 2:
                    put(step + 1, layer, [comp])

        for step in range(3):
            def body(layer, carry, step=step):
                next_vector(step, layer)
                return carry

            lax.fori_loop(0, 10 - step, body, 0)
            if step < 2:
                put(step + 1, 9 - step, [2])

        def products(layer, acc):
            acc = list(acc)
            for comp in range(3):
                for half in range(2):
                    for n in range(2):
                        v = [
                            field[step, comp, layer + 1, 8 * half : 8 * half + 8, 128 * n : 128 * n + 128]
                            for step in range(4)
                        ]
                        for k in range(6):
                            acc[k] = acc[k] + v[k // 2] * v[k - k // 2]
            return tuple(acc)

        acc = lax.fori_loop(0, 8, products, tuple(jnp.zeros((8, 128), F32) for _ in range(6)))
        mine = jnp.zeros((8, 128), F32)
        for k in range(6):
            mine = jnp.where(sub == k, jnp.sum(acc[k], axis=0, keepdims=True), mine)
        mine = jnp.sum(mine, axis=1, keepdims=True)
        sums[...] = jnp.sum(jnp.where(lane == sub, mine, 0.0), axis=0, keepdims=True)

        def reduce_over(ring, src, dst):
            copies = [remote(src, dst.at[n], peer) for n, peer in enumerate(ring.values())]
            for copy in copies:
                copy.wait_recv()
            value = src[...]
            for n in range(len(ring)):
                value = value + dst[n]
            return copies, value

        first, value = reduce_over(ring_a, sums, sums_a)
        total_a[...] = value
        second, value = reduce_over(ring_b, total_a, sums_b)

        moments = [value[:, k : k + 1] for k in range(6)]
        x_of, r_of = iterate_coefficients(moments)
        x_of = [jnp.broadcast_to(c, (16, 256)) for c in x_of]
        r_of = [jnp.broadcast_to(c * scale, (16, 256)) for c in r_of]
        sign = jnp.where(gz == 0, 1.0, -1.0)

        for comp in range(3):
            def outputs(layer, carry, comp=comp):
                place = jnp.where(gz == 0, layer, 7 - layer)
                v = [field[step, comp, layer + 1, 0:16, 0:256] for step in range(4)]
                x = x_of[0] * v[0] + x_of[1] * v[1] + x_of[2] * v[2]
                r = r_of[0] * v[0] + r_of[1] * v[1] + r_of[2] * v[2] + r_of[3] * v[3]
                solution_out[comp, place] = x * sign if comp == 0 else x
                residual_out[comp, place] = r * sign if comp == 0 else r
                return carry

            grouped(8, 2, outputs, 0)
            for n, (held, there) in enumerate(((solution_out, solution_hbm), (residual_out, residual_hbm))):
                stores.append(pltpu.make_async_copy(held.at[comp], there.at[comp], out_sem.at[1 + 2 * comp + n]))
                stores[-1].start()
        for copy in stores:
            copy.wait()

        for copy in heat + labels + strains + first + second:
            copy.wait_send()

    return kernel


def copy_out(*refs):
    sources, targets, held, (arrived, left) = refs[:3], refs[3:6], refs[6:9], refs[9:]
    pieces = [(n, n_piece) for n in (1, 2) for n_piece in range(3)] + [(0, slice(0, 16))]
    loads = [pltpu.make_async_copy(sources[n].at[k], held[n].at[k], arrived.at[i]) for i, (n, k) in enumerate(pieces)]
    stores = [pltpu.make_async_copy(held[n].at[k], targets[n].at[k], left.at[i]) for i, (n, k) in enumerate(pieces)]
    for copy in loads:
        copy.start()
    for load, store in zip(loads, stores):
        load.wait()
        store.start()
    for copy in stores:
        copy.wait()


def solution(mesh):
    sizes = dict(mesh.shape)
    hbm = pl.BlockSpec(memory_space=pltpu.HBM)
    copies = 12 + 11 + 11 + (2 * sizes["gx"] - 1) + (sizes["gy"] - 1)

    def per_device(kelvin, label, patch, traits, intensity):
        heat = lambda layers=16, kind=F32: pltpu.VMEM((layers, 24, 256), kind)
        block = lambda *lead: pltpu.VMEM((*lead, 8, 128), F32)
        wide = lambda *lead: pltpu.VMEM((*lead, 24, 384), F32)
        row = lambda *lead: pltpu.VMEM((*lead, 1, 128), F32)
        shapes = (
            jax.ShapeDtypeStruct((16, 16, 128), F32),
            jax.ShapeDtypeStruct((3, 8, 16, 256), F32),
            jax.ShapeDtypeStruct((3, 8, 16, 256), F32),
        )
        results = pl.pallas_call(
            make_kernel(sizes),
            out_shape=shapes,
            in_specs=[hbm] * 5,
            out_specs=(hbm, hbm, hbm),
            scratch_shapes=[
                pltpu.SMEM(traits.shape, F32), pltpu.SMEM(intensity.shape, F32),
                *(pltpu.VMEM(shape.shape, F32) for shape in shapes),
                heat(), heat(kind=jnp.int32), heat(kind=jnp.int32),
                heat(17), heat(), heat(), heat(), heat(), heat(), heat(), heat(17), heat(),
                block(2, 2), block(2, 3, 2), block(), block(2, 3), block(2, 3),
                pltpu.VMEM((16, 16, 128), F32),
                pltpu.VMEM((12, 24, 384), jnp.int32), wide(12),
                wide(3, 3, 14), wide(4, 14), wide(4, 3, 13), wide(5, 3, 13), wide(5, 3, 13), wide(6, 11),
                row(), row(2 * sizes["gx"] - 1), row(sizes["gy"] - 1), row(),
                pltpu.SemaphoreType.DMA((6,)),
                pltpu.SemaphoreType.DMA((7,)),
                pltpu.SemaphoreType.DMA((copies,)),
                pltpu.SemaphoreType.DMA((copies,)),
            ],
            compiler_params=pltpu.CompilerParams(
                collective_id=0, has_side_effects=True, vmem_limit_bytes=60 * 1024 * 1024
            ),
        )(kelvin, label, patch, traits, intensity)
        return pl.pallas_call(
            copy_out,
            out_shape=shapes,
            in_specs=[hbm, hbm, hbm],
            out_specs=(hbm, hbm, hbm),
            scratch_shapes=[
                *(pltpu.VMEM(shape.shape, F32) for shape in shapes),
                pltpu.SemaphoreType.DMA((7,)),
                pltpu.SemaphoreType.DMA((7,)),
            ],
            compiler_params=pltpu.CompilerParams(vmem_limit_bytes=60 * 1024 * 1024),
        )(*results)

    columns = P(None, "gx", ("gy", "gz"))
    return jax.shard_map(
        per_device,
        mesh=mesh,
        in_specs=(columns, columns, columns, P(), P()),
        out_specs=(columns, P(None, "gz", "gx", "gy"), P(None, "gz", "gx", "gy")),
        check_vma=False,
    )
```

```python
import jax
import jax.numpy as jnp
from jax import lax
from jax.experimental import pallas as pl
from jax.experimental.pallas import tpu as pltpu
from jax.sharding import PartitionSpec as P

MESH = pl.DeviceIdType.MESH
F32 = jnp.float32
TIME_STEP = 0.03
TAU = 4.0 / 3.0
SPAN = 6.0
DIAGONAL = 0.5 + 2.5 + 2.5 + 10.0 / 9.0


def plus(value, axis):
    return pltpu.roll(value, value.shape[axis] - 1, axis)


def minus(value, axis):
    return pltpu.roll(value, 1, axis)


def tree(bits, entries):
    while len(entries) > 1:
        mask, bits = bits[0], bits[1:]
        entries = [jnp.where(mask, entries[i + 1], entries[i]) for i in range(0, len(entries), 2)]
    return entries[0]


def lookup(identity, entries):
    bits, width = [], 1
    while width < len(entries):
        bits.append((identity & width) != 0)
        width *= 2
    return tree(bits, entries)


def conduct(own, other):
    return 2.0 * own * other / jnp.maximum(own + other, 0.25)


CORNER, MIXED = 10.0 / 9.0, 4.0 / 9.0
Z, X, Y = 0, 1, 2
KEPT, SUM, DIFF = 0, 1, 2


def even(get, *which):
    return get(*which, 1) + get(*which, -1)


def odd(get, *which):
    return get(*which, 1) - get(*which, -1)


def stencil(get, comp):
    if comp == Z:
        e, p = get(Z, KEPT, 0), get(Z, SUM, 0)
        pe, pp, qq = even(get, Z, KEPT), even(get, Z, SUM), odd(get, Y, DIFF)
        return (
            2.0 * (p + pp) + 6.0 * pe + qq,
            2.0 * (e + pe) + p + CORNER * pp + MIXED * qq,
            odd(get, X, KEPT) + MIXED * odd(get, X, SUM),
        )
    if comp == X:
        shared = 2.0 * (get(X, SUM, 0) + even(get, X, KEPT))
        pp = even(get, X, SUM)
        return (
            shared + pp,
            6.0 * get(X, KEPT, 0) + shared + CORNER * pp,
            get(Y, DIFF, 0) + odd(get, Z, KEPT) + MIXED * (even(get, Y, DIFF) + odd(get, Z, SUM)),
        )
    p, pe, pp, qq = get(Y, SUM, 0), even(get, Y, KEPT), even(get, Y, SUM), odd(get, Z, DIFF)
    return (
        6.0 * p + 2.0 * (pe + pp) + qq,
        2.0 * (get(Y, KEPT, 0) + p) + pe + CORNER * pp + MIXED * qq,
        get(X, DIFF, 0) + MIXED * even(get, X, DIFF),
    )


def scalar_stencils(get):
    e, p, q = get(KEPT, 0), get(SUM, 0), get(DIFF, 0)
    pe, pp, qe, qp = even(get, KEPT), even(get, SUM), odd(get, KEPT), odd(get, SUM)
    pq, qq = even(get, DIFF), odd(get, DIFF)

    def evenly(c, a):
        return c + plus(a, 0) + minus(a, 0)

    def oddly(b):
        return plus(b, 0) - minus(b, 0)

    shared = 2.0 * (p + pe)
    yield evenly(2.0 * (p + pp) + 6.0 * pe, 2.0 * (e + pe) + p + CORNER * pp)
    yield evenly(shared + pp, 6.0 * e + shared + CORNER * pp)
    yield evenly(6.0 * p + 2.0 * (pe + pp), 2.0 * (e + p) + pe + CORNER * pp)
    yield oddly(qe + MIXED * qp)
    yield evenly(qq, MIXED * qq)
    yield oddly(q + MIXED * pq)


def gradient(get, comp):
    if comp == Z:
        qe, qp = odd(get, KEPT), odd(get, SUM)
        a = 2.0 * qe + 4.0 / 3.0 * qp
        return 4.0 * qe + 2.0 * qp + plus(a, 0) + minus(a, 0)
    if comp == X:
        b = 4.0 * get(KEPT, 0) + 2.0 * (get(SUM, 0) + even(get, KEPT)) + 4.0 / 3.0 * even(get, SUM)
        return plus(b, 0) - minus(b, 0)
    q, pq = get(DIFF, 0), even(get, DIFF)
    a = 2.0 * q + 4.0 / 3.0 * pq
    return 4.0 * q + 2.0 * pq + plus(a, 0) + minus(a, 0)


def poly_dot(first, second, moments):
    total = None
    for i, a in enumerate(first):
        for j, b in enumerate(second):
            term = a * b * moments[i + j]
            total = term if total is None else total + term
    return total


def shifted(poly):
    out = [TAU * c for c in poly] + [jnp.zeros_like(poly[0])]
    for k, c in enumerate(poly):
        out[k + 1] = out[k + 1] + c
    return out


def added(first, second):
    if len(first) < len(second):
        first, second = second, first
    return [a + second[i] if i < len(second) else a for i, a in enumerate(first)]


def iterate_coefficients(moments):
    one = jnp.ones_like(moments[0])
    residual, direction, solution = [one], [one], []
    norm = moments[0]
    for number in range(3):
        image = shifted(direction)
        alpha = norm / poly_dot(direction, image, moments)
        solution = added(solution, [alpha * c for c in direction])
        residual = added([-alpha * c for c in image], residual)
        if number < 2:
            following = poly_dot(residual, residual, moments)
            ratio = following / norm
            direction = added(residual, [ratio * c for c in direction])
            norm = following
    return solution, residual


def grouped(total, size, body, init):
    def trip(number, carry):
        for k in range(size):
            carry = body(number * size + k, carry)
        return carry

    return lax.fori_loop(0, total // size, trip, init)


def make_kernel(sizes):
    nx, ny = sizes["gx"], sizes["gy"]
    group_a, group_b = nx * 2, ny

    def kernel(
        kelvin_in, label_in, patch_in, traits_in, intensity_in,
        warmed_hbm, solution_hbm, residual_hbm,
        traits, intensity, warmed_out, solution_out, residual_out,
        temp, label, patch, cond, rate, power, g_row, g_row_back, g_col, g_col_back, g_up, temp_one,
        packs, strips, packed_strain, strain_strips, label_strips,
        strain, e_label, e_strain, base, beside, field, lanes_even, lanes_odd, stiff,
        sums, sums_a, sums_b, total_a,
        local_sem, out_sem, send, recv,
    ):
        gx, gy, gz = lax.axis_index("gx"), lax.axis_index("gy"), lax.axis_index("gz")
        other = 1 - gz
        nexts = {-1: lax.rem(gx + nx - 1, nx), 0: gx, 1: lax.rem(gx + 1, nx)}
        gy_up, gy_down = lax.rem(gy + 1, ny), lax.rem(gy + ny - 1, ny)
        own_lanes = pl.ds(pl.multiple_of(gz * 128, 128), 128)

        loads = [
            pltpu.make_async_copy(kelvin_in, temp.at[:, 0:16, 0:128], local_sem.at[0]),
            pltpu.make_async_copy(label_in, label.at[:, 0:16, 0:128], local_sem.at[1]),
            pltpu.make_async_copy(patch_in, patch.at[:, 0:16, 0:128], local_sem.at[2]),
            pltpu.make_async_copy(
                label_in.at[pl.ds(4 * gz, 12)], e_label.at[:, 0:16, own_lanes], local_sem.at[3]
            ),
            pltpu.make_async_copy(traits_in, traits, local_sem.at[4]),
            pltpu.make_async_copy(intensity_in, intensity, local_sem.at[5]),
        ]
        for copy in loads:
            copy.start()
        temp[:, 16:24, 0:128] = jnp.zeros((16, 8, 128), F32)
        label[:, 16:24, 0:128] = jnp.zeros((16, 8, 128), jnp.int32)
        patch[:, 16:24, 0:128] = jnp.zeros((16, 8, 128), jnp.int32)
        for side in range(2):
            for d in (0, 2):
                strips[side, d] = jnp.zeros((2, 8, 128), F32)

        barrier = pltpu.get_barrier_semaphore()
        peers = [
            (nexts[dx], dy, dz)
            for dx in (-1, 0, 1)
            for dy in (gy, gy_up, gy_down)
            for dz in (gz, other)
            if not (dx == 0 and dy is gy and dz is gz)
        ]
        number_a = gx * 2 + gz


        def farthest_first(size):
            return sorted(range(1, size), key=lambda step: abs(size // 2 - step))

        ring_a, ring_b = {}, {}
        for step in farthest_first(group_a):
            there = lax.rem(number_a + step, group_a)
            ring_a[step] = (there // 2, gy, lax.rem(there, 2))
        for step in farthest_first(group_b):
            ring_b[step] = (gx, lax.rem(gy + step, ny), gz)
        everyone = peers + [ring_a[step] for step in range(3, group_a - 2)] + [ring_b[step] for step in range(2, group_b - 1)]
        for peer in everyone:
            pl.semaphore_signal(barrier, inc=1, device_id=peer, device_id_type=MESH)

        for copy in loads[:3]:
            copy.wait()

        lane = lax.broadcasted_iota(jnp.int32, (8, 128), 1)
        sub = lax.broadcasted_iota(jnp.int32, (8, 128), 0)

        def pack_inputs(layer, acc):
            acc = list(acc)
            for half in range(2):
                slot = layer * 2 + half
                rows = slice(8 * half, 8 * half + 8)
                place = lane - slot * 4
                ids = label[layer, rows, 0:128].astype(F32)
                kelvin = temp[layer, rows, 0:128]
                tile_ids = patch[layer, rows, 0:128].astype(F32)
                for side, (four, two) in enumerate(((0, 0), (124, 126))):
                    moved = pltpu.roll(ids, lax.rem(slot * 4 + 128 - four, 128), 1)
                    acc[2 * side] = jnp.where((lane >> 2) == slot, moved, acc[2 * side])
                    moved = pltpu.roll(kelvin, lax.rem(slot * 4 + 128 - two, 128), 1)
                    acc[2 * side + 1] = jnp.where((place >= 0) & (place < 2), moved, acc[2 * side + 1])
                    moved = pltpu.roll(tile_ids, lax.rem(slot * 4 + 130 - two, 128), 1)
                    acc[2 * side + 1] = jnp.where((place >= 2) & (place < 4), moved, acc[2 * side + 1])
            return tuple(acc)

        packed = grouped(16, 16, pack_inputs, tuple(jnp.zeros((8, 128), F32) for _ in range(4)))
        for k in range(4):
            packs[k // 2, k % 2] = packed[k]

        pl.semaphore_wait(barrier, len(everyone))

        count = [0]

        def remote(src, dst, peer):
            n = count[0]
            count[0] += 1
            copy = pltpu.make_async_remote_copy(
                src_ref=src, dst_ref=dst, send_sem=send.at[n], recv_sem=recv.at[n],
                device_id=peer, device_id_type=MESH,
            )
            copy.start()
            return copy

        heat = []
        right_gy = jnp.where(gz == 0, gy, gy_up)
        left_gy = jnp.where(gz == 0, gy_down, gy)
        for dx in (-1, 1, 0):
            rows = {0: slice(0, 8), -1: slice(0, 2), 1: slice(6, 8)}[dx]
            for side, there in ((0, left_gy), (1, right_gy)):
                heat.append(remote(packs.at[side, :, rows], strips.at[side, 1 - dx, :, rows], (nexts[dx], there, other)))
        for ref, deep in ((temp, 2), (label, 2), (patch, 1)):
            up, down = slice(16 - deep, 16), slice(24 - deep, 24)
            heat.append(remote(ref.at[:, 0:deep, 0:128], ref.at[:, 16 : 16 + deep, 0:128], (nexts[-1], gy, gz)))
            heat.append(remote(ref.at[:, up, 0:128], ref.at[:, down, 0:128], (nexts[1], gy, gz)))

        side_gy = jnp.where(gz == 0, gy_down, gy_up)

        def elastic_sends(src, src_layers, dst, pack_src, pack_dst):
            out = []
            for dx in (1, -1, 0):
                for dz in (other, gz):
                    out.append(remote(pack_src, pack_dst.at[gz, 1 - dx], (nexts[dx], side_gy, dz)))
            for dz in (other, gz):
                layers = pl.ds(src_layers(dz), 12)
                out.append(remote(src.at[layers, 0:4, 0:128], dst.at[:, 16:20, own_lanes], (nexts[-1], gy, dz)))
                out.append(remote(src.at[layers, 12:16, 0:128], dst.at[:, 20:24, own_lanes], (nexts[1], gy, dz)))
            out.append(remote(src.at[pl.ds(src_layers(other), 12), 0:16, 0:128], dst.at[:, 0:16, own_lanes], (gx, gy, other)))
            return out

        labels = elastic_sends(label, lambda dz: 4 * dz, e_label, packs.at[gz, 0], label_strips)

        for copy in loads[3:]:
            copy.wait()

        materials = range(4)
        conductivity = [traits[0, m] for m in materials]
        capacity = [traits[1, m] for m in materials]
        modulus = [traits[2, m] for m in materials]
        expansion = [-traits[3, m] for m in materials]
        tiles = [intensity[t] for t in range(16)]

        cond[16] = g_up[0] = jnp.zeros((24, 256), F32)
        lanes = (lanes_even, lanes_odd)
        for n in range(4):
            beside[n, 0] = jnp.zeros((24, 384), F32)
        for ref in (base, field, *lanes):
            for n in range(ref.shape[0]):
                for m in range(ref.shape[1]):
                    ref[n, m, 0] = jnp.zeros((24, 384), F32)
        base[0, KEPT, 13] = base[1, KEPT, 13] = jnp.zeros((24, 384), F32)

        def own_fields(layer, carry):
            ids = label[layer, 0:16, 0:128]
            cond[layer, 0:16, 0:128] = lookup(ids, conductivity)
            rate[layer, 0:16, 0:128] = TIME_STEP / lookup(ids, capacity)
            power[layer, 0:16, 0:128] = lookup(patch[layer, 0:16, 0:128], tiles)
            return carry

        grouped(16, 8, own_fields, 0)

        for copy in heat:
            copy.wait_recv()

        def halo_blocks(blocks, inset=0, last=252):
            right = [blocks(0, d) for d in (-1, 0, 1)]
            left = [blocks(1, d) for d in (-1, 0, 1)]

            def corner(three):
                return jnp.where(sub < 4, three[2], pltpu.roll(three[0], 124, 1))

            right_corner, left_corner = corner(right), corner(left)

            def at(layer):
                def one(r, l, slot):
                    r = pltpu.roll(r, lax.rem(256 - inset - slot * 4, 128), 1)
                    l = pltpu.roll(l, lax.rem(last - inset - slot * 4, 128), 1)
                    return jnp.where(lane < 64, r, l)

                return jnp.concatenate([
                    one(right[1], left[1], layer * 2),
                    one(right[1], left[1], layer * 2 + 1),
                    one(right_corner, left_corner, layer * 2),
                ], axis=0)

            return at

        label_halo = halo_blocks(lambda side, d: strips[side, d + 1, 0])
        temp_halo = halo_blocks(lambda side, d: strips[side, d + 1, 1], 0, 254)
        patch_halo = halo_blocks(lambda side, d: strips[side, d + 1, 1], 2, 254)

        row = lax.broadcasted_iota(jnp.int32, (24, 128), 0)
        wide_lane = lax.broadcasted_iota(jnp.int32, (24, 128), 1)
        low_row = jnp.where(gx == nx - 1, 16, 24)
        high_row = jnp.where(gx == 0, 20, 32)
        rows_ok = ((row < 16) | ((row >= 16) & (row < 20) & (row < low_row)) | ((row >= 20) & (row < high_row) & (gx > 0)))
        first_tile, last_tile = (gy == 0) & (gz == 0), (gy == ny - 1) & (gz == 1)
        right_limit = jnp.where(last_tile, 0, 64)
        left_limit = jnp.where(first_tile, 128, 64)
        cols_ok = (wide_lane < right_limit) | (wide_lane >= left_limit)
        grid_ok = [rows_ok[16:24], rows_ok & cols_ok]
        e_right_limit = jnp.where(gy == ny - 1, 0, 64)
        e_left_limit = jnp.where(gy == 0, 128, 64)
        e_cols_ok = (wide_lane < e_right_limit) | (wide_lane >= e_left_limit)
        e_ok = [rows_ok, rows_ok, rows_ok & e_cols_ok]

        def heat_fields(layer, carry):
            temp[layer, :, 128:256] = temp_halo(layer)
            places = ((slice(16, 24), slice(0, 128)), (slice(0, 24), slice(128, 256)))
            ids = [label[layer, 16:24, 0:128], label_halo(layer).astype(jnp.int32)]
            tile_ids = [patch[layer, 16:24, 0:128], patch_halo(layer).astype(jnp.int32)]
            for (rows, columns), own, tile, inside in zip(places, ids, tile_ids, grid_ok):
                cond[layer, rows, columns] = jnp.where(inside, lookup(own, conductivity), 0.0)
                rate[layer, rows, columns] = TIME_STEP / lookup(own, capacity)
                power[layer, rows, columns] = lookup(tile, tiles)
            return carry

        grouped(16, 8, heat_fields, 0)

        def conductances(layer, carry):
            own = cond[layer]
            row_g, col_g = conduct(own, plus(own, 0)), conduct(own, plus(own, 1))
            g_row[layer], g_col[layer] = row_g, col_g
            g_row_back[layer], g_col_back[layer] = minus(row_g, 0), minus(col_g, 1)
            g_up[layer + 1] = conduct(own, cond[layer + 1])
            return carry

        grouped(16, 8, conductances, 0)

        def heat_step(source, layer):
            own = source[layer]
            above, below = source[jnp.minimum(layer + 1, 15)], source[jnp.maximum(layer - 1, 0)]
            flux = g_row[layer] * (plus(own, 0) - own) + g_row_back[layer] * (minus(own, 0) - own)
            flux = flux + g_col[layer] * (plus(own, 1) - own) + g_col_back[layer] * (minus(own, 1) - own)
            flux = flux + g_up[layer + 1] * (above - own) + g_up[layer] * (below - own)
            return own + rate[layer] * (flux + power[layer])

        def heat_one(layer, carry):
            temp_one[layer] = heat_step(temp, layer)
            return carry

        grouped(16, 8, heat_one, 0)

        start = jnp.where(gz == 0, 0, 124)

        def heat_two(layer, acc):
            warm = heat_step(temp_one, layer)[0:16, 0:128]
            warmed_out[layer] = warm
            value = lookup(label[layer, 0:16, 0:128], expansion) * warm
            strain[layer] = value
            for half in range(2):
                slot = layer * 2 + half
                moved = pltpu.roll(value[8 * half : 8 * half + 8], lax.rem(slot * 4 + 128 - start, 128), 1)
                acc = jnp.where((lane >> 2) == slot, moved, acc)
            return acc

        packed_strain[...] = grouped(16, 8, heat_two, jnp.zeros((8, 128), F32))
        stores = [pltpu.make_async_copy(warmed_out, warmed_hbm, out_sem.at[0])]
        stores[0].start()
        strains = elastic_sends(strain, lambda dz: 4 * dz, e_strain, packed_strain, strain_strips)

        def own_strain(layer, carry):
            e_strain[layer, 0:16, own_lanes] = strain[layer + 4 * gz]
            return carry

        lax.fori_loop(0, 12, own_strain, 0)

        largest = jnp.maximum(jnp.maximum(modulus[0], modulus[1]), jnp.maximum(modulus[2], modulus[3]))
        scale = SPAN * largest
        inverse = 0.125 / jnp.full((1, 128), scale, F32)
        scaled = [m * inverse for m in modulus]

        for copy in labels:
            copy.wait_recv()

        e_label_halo = halo_blocks(lambda side, d: label_strips[side, d + 1])

        def stacked(layer):
            return jnp.where(gz == 0, layer, 11 - layer)

        cuts = [slice(128 * n, 128 * n + 128) for n in range(3)]

        def modulus_fields(layer, carry):
            raw = stacked(layer)
            ids = [e_label[raw, :, cuts[0]], e_label[raw, :, cuts[1]], e_label_halo(raw + 4 * gz).astype(jnp.int32)]
            for n, cut in enumerate(cuts):
                base[0, KEPT, layer + 1, :, cut] = jnp.where(e_ok[n], lookup(ids[n], scaled), 0.0)
            return carry

        grouped(12, 4, modulus_fields, 0)

        def spread_modulus(layer):
            e = base[0, KEPT, layer + 1]
            beside[0, layer + 1], beside[1, layer + 1] = minus(e, 0), plus(e, 0)
            ahead, behind = plus(e, 1), minus(e, 1)
            beside[2, layer + 1], beside[3, layer + 1] = ahead, behind
            base[0, SUM, layer + 1], base[0, DIFF, layer + 1] = ahead + behind, ahead - behind

        def get_base(n, layer, cut):
            return lambda kind, dz: base[n, kind, layer + 1 + dz, :, cut]

        def stiffness(layer, carry):
            spread_modulus(layer + 2)
            for cut in cuts:
                e = base[0, KEPT, layer + 1, :, cut]
                for n, value in enumerate(scalar_stencils(get_base(0, layer, cut))):
                    stiff[n, layer, :, cut] = value + (8.0 * DIAGONAL * e - TAU) if n < 3 else value
            return carry

        spread_modulus(0)
        spread_modulus(1)
        lax.fori_loop(0, 10, stiffness, 0)

        for copy in strains:
            copy.wait_recv()

        e_strain_halo = halo_blocks(lambda side, d: strain_strips[side, d + 1])

        def strain_fields(layer, carry):
            raw = stacked(layer)
            hot = [e_strain[raw, :, cuts[0]], e_strain[raw, :, cuts[1]], e_strain_halo(raw + 4 * gz)]
            for n, cut in enumerate(cuts):
                base[1, KEPT, layer + 1, :, cut] = jnp.where(e_ok[n], hot[n], 0.0)
            return carry

        grouped(12, 4, strain_fields, 0)

        def put(step, layer, comps=range(3)):
            e = base[0, 0, layer + 1]
            to = lanes[step % 2]
            for comp in comps:
                value = field[step, comp, layer + 1]
                ahead, behind = plus(value, 1), minus(value, 1)
                to[0, comp, layer + 1] = ahead + behind
                to[1, comp, layer + 1] = ahead - behind
                ahead, behind = beside[2, layer + 1] * ahead, beside[3, layer + 1] * behind
                to[2, comp, layer + 1] = e * value
                to[3, comp, layer + 1] = ahead + behind
                to[4, comp, layer + 1] = ahead - behind

        def spread_strain(layer):
            s = base[1, KEPT, layer + 1]
            ahead, behind = plus(s, 1), minus(s, 1)
            base[2, KEPT, layer + 1] = base[0, KEPT, layer + 1] * s
            base[1, SUM, layer + 1], base[1, DIFF, layer + 1] = ahead + behind, ahead - behind
            ahead, behind = beside[2, layer + 1] * ahead, beside[3, layer + 1] * behind
            base[2, SUM, layer + 1], base[2, DIFF, layer + 1] = ahead + behind, ahead - behind

        def first_vector(layer, carry):
            spread_strain(layer + 2)
            put(0, layer - 1, [2])
            for comp in range(3):
                for cut in cuts:
                    of_e, of_s, of_es = [gradient(get_base(n, layer, cut), comp) for n in range(3)]
                    e, s = base[0, KEPT, layer + 1, :, cut], base[1, KEPT, layer + 1, :, cut]
                    load = e * of_s + s * of_e + of_es
                    field[0, comp, layer + 1, :, cut] = jnp.where(e > 0.0, load, 0.0)
                if comp < 2:
                    put(0, layer, [comp])
            return carry

        spread_strain(0)
        spread_strain(1)
        lax.fori_loop(0, 11, first_vector, 0)
        put(0, 10, [2])

        places = ((0, 3, 4), (3, 1, 5), (4, 5, 2))

        def next_vector(step, layer):
            held = lanes[step % 2]
            if step < 2:
                put(step + 1, layer - 1, [2])
            for comp in range(3):
                for cut in cuts if step < 2 else cuts[:2]:
                    def plain(comp, kind, dz):
                        if kind == 0:
                            return field[step, comp, layer + 1 + dz, :, cut]
                        return held[kind - 1, comp, layer + 1 + dz, :, cut]

                    def weighted(comp, kind, dz):
                        return held[2 + kind, comp, layer + 1 + dz, :, cut]

                    c, a, b = stencil(plain, comp)
                    c_w, a_w, b_w = stencil(weighted, comp)
                    e = base[0, 0, layer + 1, :, cut]
                    terms = [stiff[places[comp][n], layer, :, cut] * field[step, n, layer + 1, :, cut] for n in range(3)]
                    value = terms[0] + terms[1] + terms[2] - (e * c + c_w)
                    value = value - plus(beside[0, layer + 1, :, cut] * (a + b) + (a_w + b_w), 0)
                    value = value - minus(beside[1, layer + 1, :, cut] * (a - b) + (a_w - b_w), 0)
                    value = jnp.where(e > 0.0, value, 0.0)
                    if step < 2:
                        field[step + 1, comp, layer + 1, :, cut] = value
                    else:
                        field[step + 1, comp, layer + 1, 0:16, cut] = value[0:16]
                if step < 2 and comp < 2:
                    put(step + 1, layer, [comp])

        for step in range(3):
            def body(layer, carry, step=step):
                next_vector(step, layer)
                return carry

            lax.fori_loop(0, 10 - step, body, 0)
            if step < 2:
                put(step + 1, 9 - step, [2])

        def products(layer, acc):
            acc = list(acc)
            for comp in range(3):
                for half in range(2):
                    for n in range(2):
                        v = [
                            field[step, comp, layer + 1, 8 * half : 8 * half + 8, 128 * n : 128 * n + 128]
                            for step in range(4)
                        ]
                        for k in range(6):
                            acc[k] = acc[k] + v[k // 2] * v[k - k // 2]
            return tuple(acc)

        acc = lax.fori_loop(0, 8, products, tuple(jnp.zeros((8, 128), F32) for _ in range(6)))
        mine = jnp.zeros((8, 128), F32)
        for k in range(6):
            mine = jnp.where(sub == k, jnp.sum(acc[k], axis=0, keepdims=True), mine)
        mine = jnp.sum(mine, axis=1, keepdims=True)
        sums[...] = jnp.sum(jnp.where(lane == sub, mine, 0.0), axis=0, keepdims=True)

        def reduce_over(ring, src, dst):
            copies = [remote(src, dst.at[n], peer) for n, peer in enumerate(ring.values())]
            for copy in copies:
                copy.wait_recv()
            value = src[...]
            for n in range(len(ring)):
                value = value + dst[n]
            return copies, value

        first, value = reduce_over(ring_a, sums, sums_a)
        total_a[...] = value
        second, value = reduce_over(ring_b, total_a, sums_b)

        moments = [value[:, k : k + 1] for k in range(6)]
        x_of, r_of = iterate_coefficients(moments)
        x_of = [jnp.broadcast_to(c, (16, 256)) for c in x_of]
        r_of = [jnp.broadcast_to(c * scale, (16, 256)) for c in r_of]
        sign = jnp.where(gz == 0, 1.0, -1.0)

        for comp in range(3):
            def outputs(layer, carry, comp=comp):
                place = jnp.where(gz == 0, layer, 7 - layer)
                v = [field[step, comp, layer + 1, 0:16, 0:256] for step in range(4)]
                x = x_of[0] * v[0] + x_of[1] * v[1] + x_of[2] * v[2]
                r = r_of[0] * v[0] + r_of[1] * v[1] + r_of[2] * v[2] + r_of[3] * v[3]
                solution_out[comp, place] = x * sign if comp == 0 else x
                residual_out[comp, place] = r * sign if comp == 0 else r
                return carry

            grouped(8, 2, outputs, 0)
            for n, (held, there) in enumerate(((solution_out, solution_hbm), (residual_out, residual_hbm))):
                stores.append(pltpu.make_async_copy(held.at[comp], there.at[comp], out_sem.at[1 + 2 * comp + n]))
                stores[-1].start()
        for copy in stores:
            copy.wait()

        for copy in heat + labels + strains + first + second:
            copy.wait_send()

    return kernel


def copy_out(*refs):
    sources, targets, held, (arrived, left) = refs[:3], refs[3:6], refs[6:9], refs[9:]
    pieces = [(n, n_piece) for n in (1, 2) for n_piece in range(3)] + [(0, slice(0, 16))]
    loads = [pltpu.make_async_copy(sources[n].at[k], held[n].at[k], arrived.at[i]) for i, (n, k) in enumerate(pieces)]
    stores = [pltpu.make_async_copy(held[n].at[k], targets[n].at[k], left.at[i]) for i, (n, k) in enumerate(pieces)]
    for copy in loads:
        copy.start()
    for load, store in zip(loads, stores):
        load.wait()
        store.start()
    for copy in stores:
        copy.wait()


def solution(mesh):
    sizes = dict(mesh.shape)
    hbm = pl.BlockSpec(memory_space=pltpu.HBM)
    copies = 12 + 11 + 11 + (2 * sizes["gx"] - 1) + (sizes["gy"] - 1)

    def per_device(kelvin, label, patch, traits, intensity):
        heat = lambda layers=16, kind=F32: pltpu.VMEM((layers, 24, 256), kind)
        block = lambda *lead: pltpu.VMEM((*lead, 8, 128), F32)
        wide = lambda *lead: pltpu.VMEM((*lead, 24, 384), F32)
        row = lambda *lead: pltpu.VMEM((*lead, 1, 128), F32)
        shapes = (
            jax.ShapeDtypeStruct((16, 16, 128), F32),
            jax.ShapeDtypeStruct((3, 8, 16, 256), F32),
            jax.ShapeDtypeStruct((3, 8, 16, 256), F32),
        )
        results = pl.pallas_call(
            make_kernel(sizes),
            out_shape=shapes,
            in_specs=[hbm] * 5,
            out_specs=(hbm, hbm, hbm),
            scratch_shapes=[
                pltpu.SMEM(traits.shape, F32), pltpu.SMEM(intensity.shape, F32),
                *(pltpu.VMEM(shape.shape, F32) for shape in shapes),
                heat(), heat(kind=jnp.int32), heat(kind=jnp.int32),
                heat(17), heat(), heat(), heat(), heat(), heat(), heat(), heat(17), heat(),
                block(2, 2), block(2, 3, 2), block(), block(2, 3), block(2, 3),
                pltpu.VMEM((16, 16, 128), F32),
                pltpu.VMEM((12, 24, 384), jnp.int32), wide(12),
                wide(3, 3, 14), wide(4, 14), wide(4, 3, 13), wide(5, 3, 13), wide(5, 3, 13), wide(6, 11),
                row(), row(2 * sizes["gx"] - 1), row(sizes["gy"] - 1), row(),
                pltpu.SemaphoreType.DMA((6,)),
                pltpu.SemaphoreType.DMA((7,)),
                pltpu.SemaphoreType.DMA((copies,)),
                pltpu.SemaphoreType.DMA((copies,)),
            ],
            compiler_params=pltpu.CompilerParams(
                collective_id=0, has_side_effects=True, vmem_limit_bytes=60 * 1024 * 1024
            ),
        )(kelvin, label, patch, traits, intensity)
        return pl.pallas_call(
            copy_out,
            out_shape=shapes,
            in_specs=[hbm, hbm, hbm],
            out_specs=(hbm, hbm, hbm),
            scratch_shapes=[
                *(pltpu.VMEM(shape.shape, F32) for shape in shapes),
                pltpu.SemaphoreType.DMA((7,)),
                pltpu.SemaphoreType.DMA((7,)),
            ],
            compiler_params=pltpu.CompilerParams(vmem_limit_bytes=60 * 1024 * 1024),
        )(*results)

    columns = P(None, "gx", ("gy", "gz"))
    return jax.shard_map(
        per_device,
        mesh=mesh,
        in_specs=(columns, columns, columns, P(), P()),
        out_specs=(columns, P(None, "gz", "gx", "gy"), P(None, "gz", "gx", "gy")),
        check_vma=False,
    )
```
